8 devices in a mesh: terms: 8 (over z, y, x, core).
Axes of the slice: x: 2, y: 2, z: 1, core: 2. Of those that a mesh axis runs over, the one named last changes fastest.
Arguments:
- psi: float32 [2, 128, 4, 4, 128], replicated
- left_env: bfloat16 [128, 128, 128], P('terms')
- phys_op: bfloat16 [128, 16, 16], P('terms')
- right_env: bfloat16 [128, 128, 128], P('terms')
Outputs:
- output 1: float32 [2, 7, 128, 4, 4, 128], P(None, None, 'terms')
- output 2: float32 [2, 6], replicated
- output 3: float32 [2, 6], replicated
All inputs are finite; a program needn't handle non-finite values.
Results may differ from the reference program's by a relative error of at most 0.0107488.
Values are sent between devices in bfloat16 or wider.
A program may use at most 1 GiB of HBM per device.

```python
import jax
import jax.numpy as jnp
from jax import lax

BOND_DIM = 128
PHYS_DIM = 4
ROOT_COUNT = 2
TERM_COUNT = 128
LANCZOS_STEPS = 6
PAIRS = PHYS_DIM * PHYS_DIM
N_ELEMS = BOND_DIM * PAIRS * BOND_DIM


def symmetric_terms(key, count, width):
    noise_key, shift_key = jax.random.split(key)
    raw = jax.random.normal(noise_key, (count, width, width), jnp.float32)
    noise = (raw + jnp.swapaxes(raw, 1, 2)) * (2.0 * width) ** -0.5
    shift = jax.random.normal(shift_key, (count,), jnp.float32)
    return noise + shift[:, None, None] * jnp.eye(width, dtype=jnp.float32)


def setup_inputs(seed: int = 0) -> dict:
    keys = jax.random.split(jax.random.key(seed), 4)
    psi = jax.random.normal(keys[0], (ROOT_COUNT, BOND_DIM, PHYS_DIM, PHYS_DIM, BOND_DIM), jnp.float32)
    left_env = symmetric_terms(keys[1], TERM_COUNT, BOND_DIM).astype(jnp.bfloat16)
    phys_op = (symmetric_terms(keys[2], TERM_COUNT, PAIRS) * TERM_COUNT ** -0.5).astype(jnp.bfloat16)
    right_env = symmetric_terms(keys[3], TERM_COUNT, BOND_DIM).astype(jnp.bfloat16)
    return {'psi': psi, 'left_env': left_env, 'phys_op': phys_op, 'right_env': right_env}


def reference(psi, left_env, phys_op, right_env):
    psi_mat = psi.reshape(ROOT_COUNT, BOND_DIM, PAIRS, BOND_DIM)
    norms = jnp.sqrt(jnp.sum(psi_mat * psi_mat, axis=(1, 2, 3)) / N_ELEMS)
    v_start = psi_mat / norms[:, None, None, None]

    def matvec(v_cur):
        flat_in = v_cur.astype(jnp.bfloat16).reshape(ROOT_COUNT * BOND_DIM * PAIRS, BOND_DIM)

        def add_term(acc, term):
            left_k, phys_k, right_k = term
            right_part = jnp.dot(flat_in, right_k.T, preferred_element_type=jnp.float32).astype(jnp.bfloat16)
            right_part = right_part.reshape(ROOT_COUNT, BOND_DIM, PAIRS, BOND_DIM)
            mid_part = jnp.einsum('qu,rcub->rcqb', phys_k.astype(jnp.float32), right_part.astype(jnp.float32)).astype(jnp.bfloat16)
            left_part = jnp.einsum('ac,rcqb->raqb', left_k.astype(jnp.float32), mid_part.astype(jnp.float32))
            return acc + left_part, None

        zero_acc = jnp.zeros((ROOT_COUNT, BOND_DIM, PAIRS, BOND_DIM), jnp.float32)
        total, _ = lax.scan(add_term, zero_acc, (left_env, phys_op, right_env))
        return total

    def lanczos_step(carry, unused):
        v_prev, v_cur, beta_prev = carry
        sigma = matvec(v_cur)
        alpha = jnp.sum(sigma * v_cur, axis=(1, 2, 3)) / N_ELEMS
        residual = sigma - alpha[:, None, None, None] * v_cur - beta_prev[:, None, None, None] * v_prev
        beta = jnp.sqrt(jnp.sum(residual * residual, axis=(1, 2, 3)) / N_ELEMS)
        v_next = residual / beta[:, None, None, None]
        return (v_cur, v_next, beta), (v_next, alpha, beta)

    start_carry = (jnp.zeros_like(v_start), v_start, jnp.zeros((ROOT_COUNT,), jnp.float32))
    _, (later, alphas, betas) = lax.scan(lanczos_step, start_carry, None, length=LANCZOS_STEPS)
    vectors = jnp.concatenate([v_start[None], later], axis=0)
    vectors = jnp.transpose(vectors, (1, 0, 2, 3, 4)).reshape(ROOT_COUNT, LANCZOS_STEPS + 1, BOND_DIM, PHYS_DIM, PHYS_DIM, BOND_DIM)
    return (vectors, alphas.T, betas.T)
```

```python
import functools

import jax
import jax.numpy as jnp
from jax import lax
from jax.experimental import pallas as pl
from jax.experimental.pallas import tpu as pltpu
from jax.sharding import PartitionSpec as P

STEPS = 6
DEVS = 8
TERMS = 16
PAIRS = 16
BOND = 128
ROWS = 16
N_ELEMS = float(BOND * PAIRS * BOND)
MESH = pl.DeviceIdType.MESH
F32 = jnp.float32
BF16 = jnp.bfloat16


def flip(dev, bits):
    out = dev
    if bits & 1:
        out = out + 1 - 2 * lax.rem(dev, 2)
    if bits & 2:
        out = out + 2 - 4 * lax.rem(dev // 2, 2)
    if bits & 4:
        out = out + 4 - 8 * lax.rem(dev // 4, 2)
    return out


def total(x):
    return jnp.sum(jnp.sum(x, axis=0, keepdims=True), axis=1, keepdims=True)


def kernel(
    v0_ref, vfull_ref, left_ref, right_ref, phys_ref, out_ref, alpha_ref, beta_ref,
    left, right, phys, wide, v_in, y_buf, z_buf, acc, sig, v_cur, v_prev, beta_old, stats, mine, turned, got,
    r_send, r_recv, w_send, w_recv, l_send, l_recv, s_send, s_recv, g_send, g_recv, o_send, o_recv,
):
    me = lax.axis_index("terms")
    peers = {e: flip(me, e) for e in range(1, DEVS)}

    barrier = pltpu.get_barrier_semaphore()
    for e in range(1, DEVS):
        pl.semaphore_signal(barrier, inc=1, device_id=(peers[e],), device_id_type=MESH)
    pl.semaphore_wait(barrier, DEVS - 1)

    def copy(src, dst, send, recv, e):
        return pltpu.make_async_remote_copy(
            src_ref=src, dst_ref=dst, send_sem=send, recv_sem=recv, device_id=(peers[e],), device_id_type=MESH
        )

    def r_copy(e):
        rows = pl.ds(pl.multiple_of(peers[e] * ROWS, ROWS), ROWS)
        return copy(right_ref.at[:, rows, :], right.at[e], r_send.at[e], r_recv.at[e], e)

    def w_copy(e):
        return copy(phys_ref, phys.at[e], w_send.at[e], w_recv.at[e], e)

    def l_copy(e):
        return copy(left_ref, left.at[e], l_send.at[e], l_recv.at[e], e)

    def l_pass(e):
        return copy(left.at[e], left.at[e + 1], l_send.at[e + 1], l_recv.at[e + 1], 1)

    def s_copy(r, e):
        return copy(mine.at[r], stats.at[r, me], s_send.at[r, e], s_recv.at[r, e], e)

    def g_copy(r, e):
        return copy(v_in.at[r, me], v_in.at[r, me], g_send.at[r, e], g_recv.at[r, e], e)

    def g_pass(r, e):
        slot = v_in.at[r, peers[e]]
        return copy(slot, slot, g_send.at[r, e + 1], g_recv.at[r, e + 1], 1)

    def o_copy(r, e):
        rows = pl.ds(pl.multiple_of(peers[e] * ROWS, ROWS), ROWS)
        return copy(turned.at[r, :, rows, :], got.at[r, me], o_send.at[r, e], o_recv.at[r, e], e)

    for e in range(1, DEVS):
        r_copy(e).start()
        w_copy(e).start()
    for e in (1, 2, 4, 6):
        l_copy(e).start()
    own = pl.ds(pl.multiple_of(me * ROWS, ROWS), ROWS)
    right[0] = right_ref[:, own, :]
    phys[0] = phys_ref[...]
    left[0] = left_ref[...]
    v_in[...] = vfull_ref[...]
    v_cur[...] = v0_ref[...]
    v_prev[...] = jnp.zeros_like(v_prev)
    beta_old[...] = jnp.zeros_like(beta_old)
    for e in range(1, DEVS):
        r_copy(e).wait()
        w_copy(e).wait()

    sub = lax.broadcasted_iota(jnp.int32, (8, BOND), 0)
    lane = lax.broadcasted_iota(jnp.int32, (8, BOND), 1)
    eye = jnp.where(lax.rem(lane, 8) == sub, 1.0, 0.0).astype(F32)
    pick_row = lax.broadcasted_iota(jnp.int32, (PAIRS * PAIRS, BOND), 0)
    pick_col = lax.broadcasted_iota(jnp.int32, (PAIRS * PAIRS, BOND), 1) // 8

    @pl.loop(0, DEVS)
    def _(d):
        w_d = phys[d]
        spread = []
        for q in range(PAIRS):
            pick = jnp.where(pick_row == pick_col + q * PAIRS, 1.0, 0.0).astype(BF16)
            spread.append(jnp.dot(w_d, pick, preferred_element_type=F32))
        for k in range(TERMS):
            for q in range(0, PAIRS, 2):
                two = [jnp.broadcast_to(spread[q + i][k : k + 1, :], (8, BOND)) * eye for i in range(2)]
                wide[d, k, q * 8 : q * 8 + 16, :] = jnp.concatenate(two, axis=0).astype(BF16)

    for e in (2, 4, 6):
        l_copy(e).wait()
        l_pass(e).start()
    l_copy(1).wait()
    for e in (2, 4, 6):
        l_pass(e).wait()

    def chunk(r, d):
        r_d = right[d].reshape(TERMS * ROWS, BOND)
        for u in range(0, PAIRS, 2):
            v_u = jnp.concatenate([v_in[r, :, u + i].reshape(BOND, BOND) for i in range(2)], axis=1)
            y = jnp.dot(r_d, v_u, preferred_element_type=F32).reshape(TERMS, 2, 8, 2 * BOND)
            y = jnp.concatenate([y[..., :BOND], y[..., BOND:]], axis=2)
            y_buf[:, :, u * 8 : u * 8 + 16, :] = y.astype(BF16)
        for k in range(TERMS):
            y_k = jnp.concatenate([y_buf[k, 0], y_buf[k, 1]], axis=1)
            z = jnp.dot(wide[d, k], y_k, preferred_element_type=F32).astype(BF16)
            for h in range(2):
                z_buf[h * BOND : (h + 1) * BOND, k * BOND : (k + 1) * BOND] = z[:, h * BOND : (h + 1) * BOND]
        part = jnp.dot(z_buf[...], left[d].reshape(TERMS * BOND, BOND), preferred_element_type=F32)

        @pl.when(d == 0)
        def _():
            acc[...] = part

        @pl.when(d > 0)
        def _():
            acc[...] += part

    def share(r):
        s, v, vp = acc[...], v_cur[r], v_prev[r]
        d_p, n_p = total(s * v), total(v * v)
        guess = jnp.where(n_p > 0.0, d_p / jnp.where(n_p > 0.0, n_p, 1.0), 0.0)
        s = s - guess * v - beta_old[r, 0:1, :] * vp
        sig[r] = s
        rows = [d_p, n_p, guess, total(s * s), total(s * v)]
        tile = jnp.zeros((8, BOND), F32)
        for i, row in enumerate(rows):
            tile = jnp.where(sub == i, row, tile)
        mine[r] = tile
        stats[r, me] = tile
        for e in range(1, DEVS):
            s_copy(r, e).start()

    def advance(r, j, last):
        for e in range(1, DEVS):
            s_copy(r, e).wait()
        alpha = jnp.zeros((1, BOND), F32)
        for p in range(DEVS):
            alpha = alpha + stats[r, p, 0:1, :]
        alpha = alpha / N_ELEMS
        square = jnp.zeros((1, BOND), F32)
        for p in range(DEVS):
            d_p = alpha - stats[r, p, 2:3, :]
            square = square + (stats[r, p, 3:4, :] - 2.0 * d_p * stats[r, p, 4:5, :] + d_p * d_p * stats[r, p, 1:2, :])
        beta = jnp.sqrt(jnp.maximum(square, 0.0) / N_ELEMS)
        shift = alpha - mine[r, 2:3, :]
        v = v_cur[r]
        nxt = (sig[r] - shift * v) / beta
        v_prev[r] = v
        v_cur[r] = nxt
        beta_old[r] = jnp.broadcast_to(beta, (8, BOND))
        alpha_ref[r, j] = jnp.broadcast_to(alpha, (8, BOND))
        beta_ref[r, j] = jnp.broadcast_to(beta, (8, BOND))
        halves = nxt.reshape(2, PAIRS, 8, BOND)
        joined = jnp.concatenate([halves[0], halves[1]], axis=1)
        if last:
            pass
        else:
            v_in[r, me] = joined.astype(BF16)
            for e in (1, 2, 4, 6):
                g_copy(r, e).start()
        for g in range(2):
            turned[r, g] = joined[g * 8 : (g + 1) * 8].reshape(BOND, BOND).T
        for e in range(1, DEVS):
            o_copy(r, e).start()
        got[r, me] = turned[r, :, own, :]

    def relay(r):
        for e in (2, 4, 6):
            g_copy(r, e).wait()
            g_pass(r, e).start()

    def arrive(r):
        g_copy(r, 1).wait()
        for e in (2, 4, 6):
            g_pass(r, e).wait()

    def collect(r, j):
        for e in range(1, DEVS):
            o_copy(r, e).wait()
        chunk_of = lax.broadcasted_iota(jnp.int32, (ROWS, BOND), 1) // 16
        for g in range(2):
            x = [got[r, p, g] for p in range(DEVS)]
            for bit in (1, 2, 4):
                odd = lax.rem(chunk_of // bit, 2) == 1
                for p in range(DEVS):
                    if p & bit:
                        continue
                    low, high = x[p], x[p + bit]
                    x[p] = jnp.where(odd, pltpu.roll(high, 16 * bit, 1), low)
                    x[p + bit] = jnp.where(odd, high, pltpu.roll(low, BOND - 16 * bit, 1))
            for q in range(8):
                out_ref[r, j, g * 8 + q] = x[q]

    @pl.loop(0, 2 * STEPS)
    def _(t):
        r, j = lax.rem(t, 2), t // 2
        pr, pj = 1 - r, (t - 1) // 2

        @pl.when(t >= 2)
        def _():
            arrive(r)

        @pl.loop(0, DEVS)
        def _(d):
            chunk(r, d)

            @pl.when(jnp.logical_and(d == 0, jnp.logical_and(t >= 1, t < 2 * STEPS - 1)))
            def _():
                advance(pr, pj, False)

            @pl.when(jnp.logical_and(d == 0, t == 2 * STEPS - 1))
            def _():
                advance(pr, pj, True)

            @pl.when(jnp.logical_and(d == 3, t >= 2))
            def _():
                collect(r, j - 1)

            @pl.when(jnp.logical_and(d == 5, jnp.logical_and(t >= 1, t < 2 * STEPS - 1)))
            def _():
                relay(pr)

        share(r)

    advance(1, STEPS - 1, True)
    collect(0, STEPS - 1)
    collect(1, STEPS - 1)


def solution(mesh):
    def device_fn(psi, left_loc, phys_loc, right_loc):
        roots = psi.shape[0]
        me = lax.axis_index("terms")
        psi_mat = psi.reshape(roots, BOND, PAIRS, BOND)
        norms = jnp.sqrt(jnp.sum(psi_mat * psi_mat, axis=(1, 2, 3)) / N_ELEMS)
        v_full = psi_mat / norms[:, None, None, None]
        first = lax.dynamic_slice_in_dim(v_full, me * ROWS, ROWS, axis=1)
        across = jnp.transpose(v_full, (0, 2, 3, 1))
        v_bf = across.astype(BF16).reshape(roots, PAIRS, DEVS, ROWS, BOND).transpose(0, 2, 1, 3, 4)
        v_own = lax.dynamic_slice_in_dim(across, me * ROWS, ROWS, axis=2)
        v_own = v_own.reshape(roots, PAIRS, 2, 8, BOND).transpose(0, 2, 1, 3, 4).reshape(roots, 2 * BOND, BOND)
        vm = pl.BlockSpec(memory_space=pltpu.VMEM)
        dma = pltpu.SemaphoreType.DMA
        rest, alpha, beta = pl.pallas_call(
            kernel,
            out_shape=(
                jax.ShapeDtypeStruct((roots, STEPS, PAIRS, ROWS, BOND), F32),
                jax.ShapeDtypeStruct((roots, STEPS, 8, BOND), F32),
                jax.ShapeDtypeStruct((roots, STEPS, 8, BOND), F32),
            ),
            in_specs=[vm] * 5,
            out_specs=(vm, vm, vm),
            scratch_shapes=[
                pltpu.VMEM((DEVS, TERMS, BOND, BOND), BF16),
                pltpu.VMEM((DEVS, TERMS, ROWS, BOND), BF16),
                pltpu.VMEM((DEVS, TERMS, PAIRS * PAIRS), BF16),
                pltpu.VMEM((DEVS, TERMS, BOND, BOND), BF16),
                pltpu.VMEM((roots, DEVS, PAIRS, ROWS, BOND), BF16),
                pltpu.VMEM((TERMS, 2, BOND, BOND), BF16),
                pltpu.VMEM((2 * BOND, TERMS * BOND), BF16),
                pltpu.VMEM((2 * BOND, BOND), F32),
                pltpu.VMEM((roots, 2 * BOND, BOND), F32),
                pltpu.VMEM((roots, 2 * BOND, BOND), F32),
                pltpu.VMEM((roots, 2 * BOND, BOND), F32),
                pltpu.VMEM((roots, 8, BOND), F32),
                pltpu.VMEM((roots, DEVS, 8, BOND), F32),
                pltpu.VMEM((roots, 8, BOND), F32),
                pltpu.VMEM((roots, 2, BOND, BOND), F32),
                pltpu.VMEM((roots, DEVS, 2, ROWS, BOND), F32),
                dma((DEVS,)), dma((DEVS,)), dma((DEVS,)), dma((DEVS,)), dma((DEVS,)), dma((DEVS,)),
                dma((roots, DEVS)), dma((roots, DEVS)), dma((roots, DEVS)), dma((roots, DEVS)),
                dma((roots, DEVS)), dma((roots, DEVS)),
            ],
            compiler_params=pltpu.CompilerParams(
                collective_id=0, has_side_effects=True, vmem_limit_bytes=56 * 1024 * 1024
            ),
        )(v_own, v_bf, left_loc, right_loc, phys_loc.reshape(TERMS, PAIRS * PAIRS))
        rest = jnp.transpose(rest, (0, 1, 3, 2, 4))
        vecs = jnp.concatenate([first[:, None], rest], axis=1)
        vecs = vecs.reshape(roots, STEPS + 1, ROWS, psi.shape[2], psi.shape[3], BOND)
        return vecs, alpha[:, :, 0, 0], beta[:, :, 0, 0]

    return jax.shard_map(
        device_fn, mesh=mesh, in_specs=(P(), P("terms"), P("terms"), P("terms")),
        out_specs=(P(None, None, "terms"), P(), P()), check_vma=False,
    )
```

```python
import functools

import jax
import jax.numpy as jnp
from jax import lax
from jax.experimental import pallas as pl
from jax.experimental.pallas import tpu as pltpu
from jax.sharding import PartitionSpec as P

STEPS = 6
DEVS = 8
TERMS = 16
PAIRS = 16
BOND = 128
ROWS = 16
N_ELEMS = float(BOND * PAIRS * BOND)
MESH = pl.DeviceIdType.MESH
F32 = jnp.float32
BF16 = jnp.bfloat16


def flip(dev, bits):
    out = dev
    if bits & 1:
        out = out + 1 - 2 * lax.rem(dev, 2)
    if bits & 2:
        out = out + 2 - 4 * lax.rem(dev // 2, 2)
    if bits & 4:
        out = out + 4 - 8 * lax.rem(dev // 4, 2)
    return out


def total(x):
    return jnp.sum(jnp.sum(x, axis=0, keepdims=True), axis=1, keepdims=True)


def kernel(
    v0_ref, vfull_ref, left_ref, right_ref, phys_ref, out_ref, alpha_ref, beta_ref,
    left, right, phys, wide, v_in, y_buf, z_buf, acc, sig, v_cur, v_prev, beta_old, stats, mine, turned, got,
    r_send, r_recv, w_send, w_recv, l_send, l_recv, s_send, s_recv, g_send, g_recv, o_send, o_recv,
):
    me = lax.axis_index("terms")
    peers = {e: flip(me, e) for e in range(1, DEVS)}

    barrier = pltpu.get_barrier_semaphore()
    for e in range(1, DEVS):
        pl.semaphore_signal(barrier, inc=1, device_id=(peers[e],), device_id_type=MESH)
    pl.semaphore_wait(barrier, DEVS - 1)

    def copy(src, dst, send, recv, e):
        return pltpu.make_async_remote_copy(
            src_ref=src, dst_ref=dst, send_sem=send, recv_sem=recv, device_id=(peers[e],), device_id_type=MESH
        )

    def r_copy(e):
        rows = pl.ds(pl.multiple_of(peers[e] * ROWS, ROWS), ROWS)
        return copy(right_ref.at[:, rows, :], right.at[e], r_send.at[e], r_recv.at[e], e)

    def w_copy(e):
        return copy(phys_ref, phys.at[e], w_send.at[e], w_recv.at[e], e)

    def l_copy(e):
        return copy(left_ref, left.at[e], l_send.at[e], l_recv.at[e], e)

    def l_pass(e):
        return copy(left.at[e], left.at[e + 1], l_send.at[e + 1], l_recv.at[e + 1], 1)

    def s_copy(r, e):
        return copy(mine.at[r], stats.at[r, me], s_send.at[r, e], s_recv.at[r, e], e)

    def g_copy(r, e):
        return copy(v_in.at[r, me], v_in.at[r, me], g_send.at[r, e], g_recv.at[r, e], e)

    def g_pass(r, e):
        slot = v_in.at[r, peers[e]]
        return copy(slot, slot, g_send.at[r, e + 1], g_recv.at[r, e + 1], 1)

    def o_copy(r, e):
        rows = pl.ds(pl.multiple_of(peers[e] * ROWS, ROWS), ROWS)
        return copy(turned.at[r, :, rows, :], got.at[r, me], o_send.at[r, e], o_recv.at[r, e], e)

    for e in range(1, DEVS):
        r_copy(e).start()
        w_copy(e).start()
    for e in (1, 2, 4, 6):
        l_copy(e).start()
    own = pl.ds(pl.multiple_of(me * ROWS, ROWS), ROWS)
    right[0] = right_ref[:, own, :]
    phys[0] = phys_ref[...]
    left[0] = left_ref[...]
    v_in[...] = vfull_ref[...]
    v_cur[...] = v0_ref[...]
    v_prev[...] = jnp.zeros_like(v_prev)
    beta_old[...] = jnp.zeros_like(beta_old)
    for e in range(1, DEVS):
        r_copy(e).wait()
        w_copy(e).wait()

    sub = lax.broadcasted_iota(jnp.int32, (8, BOND), 0)
    lane = lax.broadcasted_iota(jnp.int32, (8, BOND), 1)
    eye = jnp.where(lax.rem(lane, 8) == sub, 1.0, 0.0).astype(F32)
    pick_row = lax.broadcasted_iota(jnp.int32, (PAIRS * PAIRS, BOND), 0)
    pick_col = lax.broadcasted_iota(jnp.int32, (PAIRS * PAIRS, BOND), 1) // 8

    @pl.loop(0, DEVS)
    def _(d):
        w_d = phys[d]
        spread = []
        for q in range(PAIRS):
            pick = jnp.where(pick_row == pick_col + q * PAIRS, 1.0, 0.0).astype(BF16)
            spread.append(jnp.dot(w_d, pick, preferred_element_type=F32))
        for k in range(TERMS):
            for q in range(0, PAIRS, 2):
                two = [jnp.broadcast_to(spread[q + i][k : k + 1, :], (8, BOND)) * eye for i in range(2)]
                wide[d, k, q * 8 : q * 8 + 16, :] = jnp.concatenate(two, axis=0).astype(BF16)

    for e in (2, 4, 6):
        l_copy(e).wait()
        l_pass(e).start()
    l_copy(1).wait()
    for e in (2, 4, 6):
        l_pass(e).wait()

    def chunk(r, d):
        r_d = right[d].reshape(TERMS * ROWS, BOND)
        for u in range(0, PAIRS, 2):
            v_u = jnp.concatenate([v_in[r, :, u + i].reshape(BOND, BOND) for i in range(2)], axis=1)
            y = jnp.dot(r_d, v_u, preferred_element_type=F32).reshape(TERMS, 2, 8, 2 * BOND)
            y = jnp.concatenate([y[..., :BOND], y[..., BOND:]], axis=2)
            y_buf[:, :, u * 8 : u * 8 + 16, :] = y.astype(BF16)
        for k in range(TERMS):
            y_k = jnp.concatenate([y_buf[k, 0], y_buf[k, 1]], axis=1)
            z = jnp.dot(wide[d, k], y_k, preferred_element_type=F32).astype(BF16)
            for h in range(2):
                z_buf[h * BOND : (h + 1) * BOND, k * BOND : (k + 1) * BOND] = z[:, h * BOND : (h + 1) * BOND]
        part = jnp.dot(z_buf[...], left[d].reshape(TERMS * BOND, BOND), preferred_element_type=F32)

        @pl.when(d == 0)
        def _():
            acc[...] = part

        @pl.when(d > 0)
        def _():
            acc[...] += part

    def share(r):
        s, v, vp = acc[...], v_cur[r], v_prev[r]
        d_p, n_p = total(s * v), total(v * v)
        guess = jnp.where(n_p > 0.0, d_p / jnp.where(n_p > 0.0, n_p, 1.0), 0.0)
        s = s - guess * v - beta_old[r, 0:1, :] * vp
        sig[r] = s
        rows = [d_p, n_p, guess, total(s * s), total(s * v)]
        tile = jnp.zeros((8, BOND), F32)
        for i, row in enumerate(rows):
            tile = jnp.where(sub == i, row, tile)
        mine[r] = tile
        stats[r, me] = tile
        for e in range(1, DEVS):
            s_copy(r, e).start()

    def advance(r, j, last):
        for e in range(1, DEVS):
            s_copy(r, e).wait()
        alpha = jnp.zeros((1, BOND), F32)
        for p in range(DEVS):
            alpha = alpha + stats[r, p, 0:1, :]
        alpha = alpha / N_ELEMS
        square = jnp.zeros((1, BOND), F32)
        for p in range(DEVS):
            d_p = alpha - stats[r, p, 2:3, :]
            square = square + (stats[r, p, 3:4, :] - 2.0 * d_p * stats[r, p, 4:5, :] + d_p * d_p * stats[r, p, 1:2, :])
        beta = jnp.sqrt(jnp.maximum(square, 0.0) / N_ELEMS)
        shift = alpha - mine[r, 2:3, :]
        v = v_cur[r]
        nxt = (sig[r] - shift * v) / beta
        v_prev[r] = v
        v_cur[r] = nxt
        beta_old[r] = jnp.broadcast_to(beta, (8, BOND))
        alpha_ref[r, j] = jnp.broadcast_to(alpha, (8, BOND))
        beta_ref[r, j] = jnp.broadcast_to(beta, (8, BOND))
        halves = nxt.reshape(2, PAIRS, 8, BOND)
        joined = jnp.concatenate([halves[0], halves[1]], axis=1)
        if last:
            pass
        else:
            v_in[r, me] = joined.astype(BF16)
            for e in (1, 2, 4, 6):
                g_copy(r, e).start()
        for g in range(2):
            turned[r, g] = joined[g * 8 : (g + 1) * 8].reshape(BOND, BOND).T
        for e in range(1, DEVS):
            o_copy(r, e).start()
        got[r, me] = turned[r, :, own, :]

    def relay(r):
        for e in (2, 4, 6):
            g_copy(r, e).wait()
            g_pass(r, e).start()

    def arrive(r):
        g_copy(r, 1).wait()
        for e in (2, 4, 6):
            g_pass(r, e).wait()

    def collect(r, j):
        for e in range(1, DEVS):
            o_copy(r, e).wait()
        chunk_of = lax.broadcasted_iota(jnp.int32, (ROWS, BOND), 1) // 16
        for g in range(2):
            x = [got[r, p, g] for p in range(DEVS)]
            for bit in (1, 2, 4):
                odd = lax.rem(chunk_of // bit, 2) == 1
                for p in range(DEVS):
                    if p & bit:
                        continue
                    low, high = x[p], x[p + bit]
                    x[p] = jnp.where(odd, pltpu.roll(high, 16 * bit, 1), low)
                    x[p + bit] = jnp.where(odd, high, pltpu.roll(low, BOND - 16 * bit, 1))
            for q in range(8):
                out_ref[r, j, g * 8 + q] = x[q]

    @pl.loop(0, 2 * STEPS)
    def _(t):
        r, j = lax.rem(t, 2), t // 2
        pr, pj = 1 - r, (t - 1) // 2

        @pl.when(t >= 2)
        def _():
            arrive(r)

        @pl.loop(0, DEVS)
        def _(d):
            chunk(r, d)

            @pl.when(jnp.logical_and(d == 2, jnp.logical_and(t >= 1, t < 2 * STEPS - 1)))
            def _():
                advance(pr, pj, False)

            @pl.when(jnp.logical_and(d == 2, t == 2 * STEPS - 1))
            def _():
                advance(pr, pj, True)

            @pl.when(jnp.logical_and(d == 3, t >= 2))
            def _():
                collect(r, j - 1)

            @pl.when(jnp.logical_and(d == 6, jnp.logical_and(t >= 1, t < 2 * STEPS - 1)))
            def _():
                relay(pr)

        share(r)

    advance(1, STEPS - 1, True)
    collect(0, STEPS - 1)
    collect(1, STEPS - 1)


def solution(mesh):
    def device_fn(psi, left_loc, phys_loc, right_loc):
        roots = psi.shape[0]
        me = lax.axis_index("terms")
        psi_mat = psi.reshape(roots, BOND, PAIRS, BOND)
        norms = jnp.sqrt(jnp.sum(psi_mat * psi_mat, axis=(1, 2, 3)) / N_ELEMS)
        v_full = psi_mat / norms[:, None, None, None]
        first = lax.dynamic_slice_in_dim(v_full, me * ROWS, ROWS, axis=1)
        across = jnp.transpose(v_full, (0, 2, 3, 1))
        v_bf = across.astype(BF16).reshape(roots, PAIRS, DEVS, ROWS, BOND).transpose(0, 2, 1, 3, 4)
        v_own = lax.dynamic_slice_in_dim(across, me * ROWS, ROWS, axis=2)
        v_own = v_own.reshape(roots, PAIRS, 2, 8, BOND).transpose(0, 2, 1, 3, 4).reshape(roots, 2 * BOND, BOND)
        vm = pl.BlockSpec(memory_space=pltpu.VMEM)
        dma = pltpu.SemaphoreType.DMA
        rest, alpha, beta = pl.pallas_call(
            kernel,
            out_shape=(
                jax.ShapeDtypeStruct((roots, STEPS, PAIRS, ROWS, BOND), F32),
                jax.ShapeDtypeStruct((roots, STEPS, 8, BOND), F32),
                jax.ShapeDtypeStruct((roots, STEPS, 8, BOND), F32),
            ),
            in_specs=[vm] * 5,
            out_specs=(vm, vm, vm),
            scratch_shapes=[
                pltpu.VMEM((DEVS, TERMS, BOND, BOND), BF16),
                pltpu.VMEM((DEVS, TERMS, ROWS, BOND), BF16),
                pltpu.VMEM((DEVS, TERMS, PAIRS * PAIRS), BF16),
                pltpu.VMEM((DEVS, TERMS, BOND, BOND), BF16),
                pltpu.VMEM((roots, DEVS, PAIRS, ROWS, BOND), BF16),
                pltpu.VMEM((TERMS, 2, BOND, BOND), BF16),
                pltpu.VMEM((2 * BOND, TERMS * BOND), BF16),
                pltpu.VMEM((2 * BOND, BOND), F32),
                pltpu.VMEM((roots, 2 * BOND, BOND), F32),
                pltpu.VMEM((roots, 2 * BOND, BOND), F32),
                pltpu.VMEM((roots, 2 * BOND, BOND), F32),
                pltpu.VMEM((roots, 8, BOND), F32),
                pltpu.VMEM((roots, DEVS, 8, BOND), F32),
                pltpu.VMEM((roots, 8, BOND), F32),
                pltpu.VMEM((roots, 2, BOND, BOND), F32),
                pltpu.VMEM((roots, DEVS, 2, ROWS, BOND), F32),
                dma((DEVS,)), dma((DEVS,)), dma((DEVS,)), dma((DEVS,)), dma((DEVS,)), dma((DEVS,)),
                dma((roots, DEVS)), dma((roots, DEVS)), dma((roots, DEVS)), dma((roots, DEVS)),
                dma((roots, DEVS)), dma((roots, DEVS)),
            ],
            compiler_params=pltpu.CompilerParams(
                collective_id=0, has_side_effects=True, vmem_limit_bytes=56 * 1024 * 1024
            ),
        )(v_own, v_bf, left_loc, right_loc, phys_loc.reshape(TERMS, PAIRS * PAIRS))
        rest = jnp.transpose(rest, (0, 1, 3, 2, 4))
        vecs = jnp.concatenate([first[:, None], rest], axis=1)
        vecs = vecs.reshape(roots, STEPS + 1, ROWS, psi.shape[2], psi.shape[3], BOND)
        return vecs, alpha[:, :, 0, 0], beta[:, :, 0, 0]

    return jax.shard_map(
        device_fn, mesh=mesh, in_specs=(P(), P("terms"), P("terms"), P("terms")),
        out_specs=(P(None, None, "terms"), P(), P()), check_vma=False,
    )
```

```python
import functools

import jax
import jax.numpy as jnp
from jax import lax
from jax.experimental import pallas as pl
from jax.experimental.pallas import tpu as pltpu
from jax.sharding import PartitionSpec as P

STEPS = 6
DEVS = 8
TERMS = 16
PAIRS = 16
BOND = 128
ROWS = 16
N_ELEMS = float(BOND * PAIRS * BOND)
FORM_AFTER = 2
RELAY_AFTER = 6
MESH = pl.DeviceIdType.MESH
F32 = jnp.float32
BF16 = jnp.bfloat16


def flip(dev, bits):
    out = dev
    if bits & 1:
        out = out + 1 - 2 * lax.rem(dev, 2)
    if bits & 2:
        out = out + 2 - 4 * lax.rem(dev // 2, 2)
    if bits & 4:
        out = out + 4 - 8 * lax.rem(dev // 4, 2)
    return out


def total(x):
    return jnp.sum(jnp.sum(x, axis=0, keepdims=True), axis=1, keepdims=True)


def kernel(
    psi_ref, left_ref, right_ref, phys_ref, out_ref, alpha_ref, beta_ref,
    left, right, phys, wide, v_in, y_buf0, y_buf1, z_buf0, z_buf1, acc, sig, v_cur, v_prev, beta_old, stats, mine,
    turned, got, across, numbers,
    r_send, r_recv, w_send, w_recv, l_send, l_recv, s_send, s_recv, g_send, g_recv, o_send, o_recv,
):
    me = lax.axis_index("terms")
    peers = {e: flip(me, e) for e in range(1, DEVS)}

    barrier = pltpu.get_barrier_semaphore()
    for e in range(1, DEVS):
        pl.semaphore_signal(barrier, inc=1, device_id=(peers[e],), device_id_type=MESH)
    pl.semaphore_wait(barrier, DEVS - 1)

    def copy(src, dst, send, recv, e):
        return pltpu.make_async_remote_copy(
            src_ref=src, dst_ref=dst, send_sem=send, recv_sem=recv, device_id=(peers[e],), device_id_type=MESH
        )

    def r_copy(e):
        rows = pl.ds(pl.multiple_of(peers[e] * ROWS, ROWS), ROWS)
        return copy(right_ref.at[:, rows, :], right.at[e], r_send.at[e], r_recv.at[e], e)

    def w_copy(e):
        return copy(phys_ref, phys.at[e], w_send.at[e], w_recv.at[e], e)

    def l_copy(e):
        return copy(left_ref, left.at[e], l_send.at[e], l_recv.at[e], e)

    def l_pass(e):
        return copy(left.at[e], left.at[e + 1], l_send.at[e + 1], l_recv.at[e + 1], 1)

    def s_copy(r, e):
        return copy(mine.at[r], stats.at[r, me], s_send.at[r, e], s_recv.at[r, e], e)

    def g_copy(r, e):
        return copy(v_in.at[r, me], v_in.at[r, me], g_send.at[r, e], g_recv.at[r, e], e)

    def g_pass(r, e):
        slot = v_in.at[r, peers[e]]
        return copy(slot, slot, g_send.at[r, e + 1], g_recv.at[r, e + 1], 1)

    def o_copy(r, e):
        rows = pl.ds(pl.multiple_of(peers[e] * ROWS, ROWS), ROWS)
        return copy(turned.at[r, :, rows, :], got.at[r, me], o_send.at[r, e], o_recv.at[r, e], e)

    for e in range(1, DEVS):
        r_copy(e).start()
        w_copy(e).start()
    for e in (1, 2, 4, 6):
        l_copy(e).start()
    own = pl.ds(pl.multiple_of(me * ROWS, ROWS), ROWS)
    right[0] = right_ref[:, own, :]
    phys[0] = phys_ref[...]
    left[0] = left_ref[...]
    v_prev[...] = jnp.zeros_like(v_prev)
    beta_old[...] = jnp.zeros_like(beta_old)
    numbers[...] = jnp.zeros_like(numbers)

    @pl.loop(0, 2)
    def _(r):
        acc[0:BOND, :] = jnp.zeros((BOND, BOND), F32)

        @pl.loop(0, 4)
        def _(s):
            for t in range(4):
                x = psi_ref[r, :, s, t, :]
                acc[0:BOND, :] += x * x
                across[s * 4 + t] = x.T

        norm = jnp.sqrt(total(acc[0:BOND, :]) / N_ELEMS)

        @pl.loop(0, PAIRS)
        def _(u):
            v_in[r, :, u] = (across[u] / norm).astype(BF16).reshape(DEVS, ROWS, BOND)
            two = across[u, own, :] / norm
            row = pl.multiple_of(u * 8, 8)
            v_cur[r, pl.ds(row, 8), :] = two[0:8]
            v_cur[r, pl.ds(row + BOND, 8), :] = two[8:16]

        out_ref[r, 0] = psi_ref[r, own] / norm.reshape(1, 1, 1, 1)

    for e in range(1, DEVS):
        r_copy(e).wait()
        w_copy(e).wait()

    sub = lax.broadcasted_iota(jnp.int32, (8, BOND), 0)
    lane = lax.broadcasted_iota(jnp.int32, (8, BOND), 1)
    eye = jnp.where(lax.rem(lane, 8) == sub, 1.0, 0.0).astype(F32)
    pick_row = lax.broadcasted_iota(jnp.int32, (PAIRS * PAIRS, BOND), 0)
    pick_col = lax.broadcasted_iota(jnp.int32, (PAIRS * PAIRS, BOND), 1) // 8

    @pl.loop(0, DEVS)
    def _(d):
        w_d = phys[d]
        spread = []
        for q in range(PAIRS):
            pick = jnp.where(pick_row == pick_col + q * PAIRS, 1.0, 0.0).astype(BF16)
            spread.append(jnp.dot(w_d, pick, preferred_element_type=F32))
        for k in range(TERMS):
            for q in range(0, PAIRS, 2):
                two = [jnp.broadcast_to(spread[q + i][k : k + 1, :], (8, BOND)) * eye for i in range(2)]
                wide[d, k, q * 8 : q * 8 + 16, :] = jnp.concatenate(two, axis=0).astype(BF16)

    for e in (2, 4, 6):
        l_copy(e).wait()
        l_pass(e).start()
    l_copy(1).wait()
    for e in (2, 4, 6):
        l_pass(e).wait()

    def chunk(r, d):
        y_buf, z_buf = ((y_buf0, z_buf0), (y_buf1, z_buf1))[d % 2]
        r_d = right[d].reshape(TERMS * ROWS, BOND)
        for u in range(0, PAIRS, 2):
            v_u = jnp.concatenate([v_in[r, :, u + i].reshape(BOND, BOND) for i in range(2)], axis=1)
            y = jnp.dot(r_d, v_u, preferred_element_type=F32).reshape(TERMS, 2, 8, 2 * BOND)
            y = jnp.concatenate([y[..., :BOND], y[..., BOND:]], axis=2)
            y_buf[:, :, u * 8 : u * 8 + 16, :] = y.astype(BF16)
        for k in range(TERMS):
            y_k = jnp.concatenate([y_buf[k, 0], y_buf[k, 1]], axis=1)
            z = jnp.dot(wide[d, k], y_k, preferred_element_type=F32).astype(BF16)
            for h in range(2):
                z_buf[h * BOND : (h + 1) * BOND, k * BOND : (k + 1) * BOND] = z[:, h * BOND : (h + 1) * BOND]
        part = jnp.dot(z_buf[...], left[d].reshape(TERMS * BOND, BOND), preferred_element_type=F32)
        if d == 0:
            acc[...] = part
        else:
            acc[...] += part

    def share(r):
        s, v, vp = acc[...], v_cur[r], v_prev[r]
        d_p, n_p = total(s * v), total(v * v)
        guess = jnp.where(n_p > 0.0, d_p / jnp.where(n_p > 0.0, n_p, 1.0), 0.0)
        s = s - guess * v - beta_old[r, 0:1, :] * vp
        sig[r] = s
        rows = [d_p, n_p, guess, total(s * s), total(s * v)]
        tile = jnp.zeros((8, BOND), F32)
        for i, row in enumerate(rows):
            tile = jnp.where(sub == i, row, tile)
        mine[r] = tile
        stats[r, me] = tile
        for e in range(1, DEVS):
            s_copy(r, e).start()

    def advance(r, j, last):
        for e in range(1, DEVS):
            s_copy(r, e).wait()
        alpha = jnp.zeros((1, BOND), F32)
        for p in range(DEVS):
            alpha = alpha + stats[r, p, 0:1, :]
        alpha = alpha / N_ELEMS
        square = jnp.zeros((1, BOND), F32)
        for p in range(DEVS):
            d_p = alpha - stats[r, p, 2:3, :]
            square = square + (stats[r, p, 3:4, :] - 2.0 * d_p * stats[r, p, 4:5, :] + d_p * d_p * stats[r, p, 1:2, :])
        beta = jnp.sqrt(jnp.maximum(square, 0.0) / N_ELEMS)
        shift = alpha - mine[r, 2:3, :]
        v = v_cur[r]
        nxt = (sig[r] - shift * v) / beta
        v_prev[r] = v
        v_cur[r] = nxt
        beta_old[r] = jnp.broadcast_to(beta, (8, BOND))
        here = jnp.logical_and(sub == r, lane == j)
        numbers[0] = jnp.where(here, alpha, numbers[0])
        numbers[1] = jnp.where(here, beta, numbers[1])
        halves = nxt.reshape(2, PAIRS, 8, BOND)
        joined = jnp.concatenate([halves[0], halves[1]], axis=1)
        if last:
            pass
        else:
            v_in[r, me] = joined.astype(BF16)
            for e in (1, 2, 4, 6):
                g_copy(r, e).start()
        for g in range(2):
            turned[r, g] = joined[g * 8 : (g + 1) * 8].reshape(BOND, BOND).T
        for e in range(1, DEVS):
            o_copy(r, e).start()
        got[r, me] = turned[r, :, own, :]

    def relay(r):
        for e in (2, 4, 6):
            g_copy(r, e).wait()
            g_pass(r, e).start()

    def arrive(r):
        g_copy(r, 1).wait()
        for e in (2, 4, 6):
            g_pass(r, e).wait()

    def collect(r, j):
        for e in range(1, DEVS):
            o_copy(r, e).wait()
        chunk_of = lax.broadcasted_iota(jnp.int32, (ROWS, BOND), 1) // 16
        for g in range(2):
            x = [got[r, p, g] for p in range(DEVS)]
            for bit in (1, 2, 4):
                odd = lax.rem(chunk_of // bit, 2) == 1
                for p in range(DEVS):
                    if p & bit:
                        continue
                    low, high = x[p], x[p + bit]
                    x[p] = jnp.where(odd, pltpu.roll(high, 16 * bit, 1), low)
                    x[p + bit] = jnp.where(odd, high, pltpu.roll(low, BOND - 16 * bit, 1))
            for q in range(8):
                pair = g * 8 + q
                out_ref[r, j + 1, :, pair // 4, pair % 4, :] = x[q]

    @pl.loop(0, 2 * STEPS)
    def _(t):
        r, j = lax.rem(t, 2), t // 2
        pr, pj = 1 - r, (t - 1) // 2

        @pl.when(t >= 2)
        def _():
            arrive(r)

        for d in range(DEVS):
            chunk(r, d)
            if d == FORM_AFTER:

                @pl.when(jnp.logical_and(t >= 1, t < 2 * STEPS - 1))
                def _():
                    advance(pr, pj, False)

                @pl.when(t == 2 * STEPS - 1)
                def _():
                    advance(pr, pj, True)

                @pl.when(t >= 2)
                def _():
                    collect(r, j - 1)

            if d == RELAY_AFTER:

                @pl.when(jnp.logical_and(t >= 1, t < 2 * STEPS - 1))
                def _():
                    relay(pr)

        share(r)

    advance(1, STEPS - 1, True)
    collect(0, STEPS - 1)
    collect(1, STEPS - 1)
    alpha_ref[...] = numbers[0, 0:2, 0:STEPS]
    beta_ref[...] = numbers[1, 0:2, 0:STEPS]


def solution(mesh):
    def device_fn(psi, left_loc, phys_loc, right_loc):
        roots = psi.shape[0]
        vm = pl.BlockSpec(memory_space=pltpu.VMEM)
        dma = pltpu.SemaphoreType.DMA
        return pl.pallas_call(
            kernel,
            out_shape=(
                jax.ShapeDtypeStruct((roots, STEPS + 1, ROWS) + psi.shape[2:], F32),
                jax.ShapeDtypeStruct((roots, STEPS), F32),
                jax.ShapeDtypeStruct((roots, STEPS), F32),
            ),
            in_specs=[vm] * 4,
            out_specs=(vm, vm, vm),
            scratch_shapes=[
                pltpu.VMEM((DEVS, TERMS, BOND, BOND), BF16),
                pltpu.VMEM((DEVS, TERMS, ROWS, BOND), BF16),
                pltpu.VMEM((DEVS, TERMS, PAIRS * PAIRS), BF16),
                pltpu.VMEM((DEVS, TERMS, BOND, BOND), BF16),
                pltpu.VMEM((roots, DEVS, PAIRS, ROWS, BOND), BF16),
                pltpu.VMEM((TERMS, 2, BOND, BOND), BF16),
                pltpu.VMEM((TERMS, 2, BOND, BOND), BF16),
                pltpu.VMEM((2 * BOND, TERMS * BOND), BF16),
                pltpu.VMEM((2 * BOND, TERMS * BOND), BF16),
                pltpu.VMEM((2 * BOND, BOND), F32),
                pltpu.VMEM((roots, 2 * BOND, BOND), F32),
                pltpu.VMEM((roots, 2 * BOND, BOND), F32),
                pltpu.VMEM((roots, 2 * BOND, BOND), F32),
                pltpu.VMEM((roots, 8, BOND), F32),
                pltpu.VMEM((roots, DEVS, 8, BOND), F32),
                pltpu.VMEM((roots, 8, BOND), F32),
                pltpu.VMEM((roots, 2, BOND, BOND), F32),
                pltpu.VMEM((roots, DEVS, 2, ROWS, BOND), F32),
                pltpu.VMEM((PAIRS, BOND, BOND), F32),
                pltpu.VMEM((2, 8, BOND), F32),
                dma((DEVS,)), dma((DEVS,)), dma((DEVS,)), dma((DEVS,)), dma((DEVS,)), dma((DEVS,)),
                dma((roots, DEVS)), dma((roots, DEVS)), dma((roots, DEVS)), dma((roots, DEVS)),
                dma((roots, DEVS)), dma((roots, DEVS)),
            ],
            compiler_params=pltpu.CompilerParams(
                collective_id=0, has_side_effects=True, vmem_limit_bytes=56 * 1024 * 1024
            ),
        )(psi, left_loc, right_loc, phys_loc.reshape(TERMS, PAIRS * PAIRS))

    return jax.shard_map(
        device_fn, mesh=mesh, in_specs=(P(), P("terms"), P("terms"), P("terms")),
        out_specs=(P(None, None, "terms"), P(), P()), check_vma=False,
    )
```

```python
import functools

import jax
import jax.numpy as jnp
from jax import lax
from jax.experimental import pallas as pl
from jax.experimental.pallas import tpu as pltpu
from jax.sharding import PartitionSpec as P

STEPS = 6
DEVS = 8
TERMS = 16
PAIRS = 16
BOND = 128
ROWS = 16
N_ELEMS = float(BOND * PAIRS * BOND)
FORM_AFTER = 1
COLLECT_AFTER = 5
MESH = pl.DeviceIdType.MESH
F32 = jnp.float32
BF16 = jnp.bfloat16


def flip(dev, bits):
    out = dev
    if bits & 1:
        out = out + 1 - 2 * lax.rem(dev, 2)
    if bits & 2:
        out = out + 2 - 4 * lax.rem(dev // 2, 2)
    if bits & 4:
        out = out + 4 - 8 * lax.rem(dev // 4, 2)
    return out


def total(x):
    return jnp.sum(jnp.sum(x, axis=0, keepdims=True), axis=1, keepdims=True)


def kernel(
    psi_ref, left_ref, right_ref, phys_ref, out_ref, alpha_ref, beta_ref,
    left, right, phys, wide, v_in, y_buf0, y_buf1, z_buf0, z_buf1, acc, sig, v_cur, v_prev, beta_old, stats, mine,
    turned, got, across, numbers,
    r_send, r_recv, w_send, w_recv, l_send, l_recv, s_send, s_recv, g_send, g_recv, o_send, o_recv,
):
    me = lax.axis_index("terms")
    peers = {e: flip(me, e) for e in range(1, DEVS)}

    barrier = pltpu.get_barrier_semaphore()
    for e in range(1, DEVS):
        pl.semaphore_signal(barrier, inc=1, device_id=(peers[e],), device_id_type=MESH)
    pl.semaphore_wait(barrier, DEVS - 1)

    def copy(src, dst, send, recv, e):
        return pltpu.make_async_remote_copy(
            src_ref=src, dst_ref=dst, send_sem=send, recv_sem=recv, device_id=(peers[e],), device_id_type=MESH
        )

    def r_copy(e):
        rows = pl.ds(pl.multiple_of(peers[e] * ROWS, ROWS), ROWS)
        return copy(right_ref.at[:, rows, :], right.at[e], r_send.at[e], r_recv.at[e], e)

    def w_copy(e):
        return copy(phys_ref, phys.at[e], w_send.at[e], w_recv.at[e], e)

    def l_copy(e):
        return copy(left_ref, left.at[e], l_send.at[e], l_recv.at[e], e)

    def l_pass(e):
        return copy(left.at[e], left.at[e + 1], l_send.at[e + 1], l_recv.at[e + 1], 1)

    def s_copy(r, e):
        return copy(mine.at[r], stats.at[r, me], s_send.at[r, e], s_recv.at[r, e], e)

    def g_copy(r, e):
        return copy(v_in.at[r, me], v_in.at[r, me], g_send.at[r, e], g_recv.at[r, e], e)

    def g_pass(r, e):
        slot = v_in.at[r, peers[e]]
        return copy(slot, slot, g_send.at[r, e + 1], g_recv.at[r, e + 1], 1)

    def o_copy(r, e):
        rows = pl.ds(pl.multiple_of(peers[e] * ROWS, ROWS), ROWS)
        return copy(turned.at[r, :, rows, :], got.at[r, me], o_send.at[r, e], o_recv.at[r, e], e)

    for both in ((1,), (2, 3), (4, 5), (6, 7)):
        for e in both:
            r_copy(e).start()
            w_copy(e).start()
        l_copy(2 * (both[0] // 2) if both[0] > 1 else 1).start()
    own = pl.ds(pl.multiple_of(me * ROWS, ROWS), ROWS)
    right[0] = right_ref[:, own, :]
    phys[0] = phys_ref[...]
    left[0] = left_ref[...]
    v_prev[...] = jnp.zeros_like(v_prev)
    beta_old[...] = jnp.zeros_like(beta_old)
    numbers[...] = jnp.zeros_like(numbers)

    @pl.loop(0, 2)
    def _(r):
        acc[0:BOND, :] = jnp.zeros((BOND, BOND), F32)

        @pl.loop(0, 4)
        def _(s):
            for t in range(4):
                x = psi_ref[r, :, s, t, :]
                acc[0:BOND, :] += x * x
                across[s * 4 + t] = x.T

        norm = jnp.sqrt(total(acc[0:BOND, :]) / N_ELEMS)

        @pl.loop(0, PAIRS)
        def _(u):
            v_in[r, :, u] = (across[u] / norm).astype(BF16).reshape(DEVS, ROWS, BOND)
            two = across[u, own, :] / norm
            row = pl.multiple_of(u * 8, 8)
            v_cur[r, pl.ds(row, 8), :] = two[0:8]
            v_cur[r, pl.ds(row + BOND, 8), :] = two[8:16]

        out_ref[r, 0] = psi_ref[r, own] / norm.reshape(1, 1, 1, 1)

    sub = lax.broadcasted_iota(jnp.int32, (8, BOND), 0)
    lane = lax.broadcasted_iota(jnp.int32, (8, BOND), 1)
    eye = jnp.where(lax.rem(lane, 8) == sub, 1.0, 0.0).astype(F32)
    pick_row = lax.broadcasted_iota(jnp.int32, (PAIRS * PAIRS, BOND), 0)
    pick_col = lax.broadcasted_iota(jnp.int32, (PAIRS * PAIRS, BOND), 1) // 8

    def widen(d):
        w_d = phys[d]
        spread = []
        for q in range(PAIRS):
            pick = jnp.where(pick_row == pick_col + q * PAIRS, 1.0, 0.0).astype(BF16)
            spread.append(jnp.dot(w_d, pick, preferred_element_type=F32))
        for k in range(TERMS):
            for q in range(0, PAIRS, 2):
                two = [jnp.broadcast_to(spread[q + i][k : k + 1, :], (8, BOND)) * eye for i in range(2)]
                wide[d, k, q * 8 : q * 8 + 16, :] = jnp.concatenate(two, axis=0).astype(BF16)

    def chunk(r, d, y_buf, z_buf, first):
        r_d = right[d].reshape(TERMS * ROWS, BOND)
        for u in range(0, PAIRS, 2):
            v_u = jnp.concatenate([v_in[r, :, u + i].reshape(BOND, BOND) for i in range(2)], axis=1)
            y = jnp.dot(r_d, v_u, preferred_element_type=F32).reshape(TERMS, 2, 8, 2 * BOND)
            y = jnp.concatenate([y[..., :BOND], y[..., BOND:]], axis=2)
            y_buf[:, :, u * 8 : u * 8 + 16, :] = y.astype(BF16)
        for k in range(TERMS):
            y_k = jnp.concatenate([y_buf[k, 0], y_buf[k, 1]], axis=1)
            z = jnp.dot(wide[d, k], y_k, preferred_element_type=F32).astype(BF16)
            for h in range(2):
                z_buf[h * BOND : (h + 1) * BOND, k * BOND : (k + 1) * BOND] = z[:, h * BOND : (h + 1) * BOND]
        part = jnp.dot(z_buf[...], left[d].reshape(TERMS * BOND, BOND), preferred_element_type=F32)
        if first:
            acc[...] = part
        else:
            acc[...] += part

    def share(r):
        s, v, vp = acc[...], v_cur[r], v_prev[r]
        d_p, n_p = total(s * v), total(v * v)
        guess = jnp.where(n_p > 0.0, d_p / jnp.where(n_p > 0.0, n_p, 1.0), 0.0)
        s = s - guess * v - beta_old[r, 0:1, :] * vp
        sig[r] = s
        rows = [d_p, n_p, guess, total(s * s), total(s * v)]
        tile = jnp.zeros((8, BOND), F32)
        for i, row in enumerate(rows):
            tile = jnp.where(sub == i, row, tile)
        mine[r] = tile
        stats[r, me] = tile
        for e in (6, 7, 2, 3, 4, 5, 1):
            s_copy(r, e).start()

    def advance(r, j, last):
        for e in range(1, DEVS):
            s_copy(r, e).wait()
        alpha = jnp.zeros((1, BOND), F32)
        for p in range(DEVS):
            alpha = alpha + stats[r, p, 0:1, :]
        alpha = alpha / N_ELEMS
        square = jnp.zeros((1, BOND), F32)
        for p in range(DEVS):
            d_p = alpha - stats[r, p, 2:3, :]
            square = square + (stats[r, p, 3:4, :] - 2.0 * d_p * stats[r, p, 4:5, :] + d_p * d_p * stats[r, p, 1:2, :])
        beta = jnp.sqrt(jnp.maximum(square, 0.0) / N_ELEMS)
        shift = alpha - mine[r, 2:3, :]
        v = v_cur[r]
        nxt = (sig[r] - shift * v) / beta
        v_prev[r] = v
        v_cur[r] = nxt
        beta_old[r] = jnp.broadcast_to(beta, (8, BOND))
        here = jnp.logical_and(sub == r, lane == j)
        numbers[0] = jnp.where(here, alpha, numbers[0])
        numbers[1] = jnp.where(here, beta, numbers[1])
        halves = nxt.reshape(2, PAIRS, 8, BOND)
        joined = jnp.concatenate([halves[0], halves[1]], axis=1)
        if last:
            pass
        else:
            v_in[r, me] = joined.astype(BF16)
            for e in (6, 2, 4, 1):
                g_copy(r, e).start()
        for g in range(2):
            turned[r, g] = joined[g * 8 : (g + 1) * 8].reshape(BOND, BOND).T

    def post(r):
        for e in (6, 7, 2, 3, 4, 5, 1):
            o_copy(r, e).start()
        got[r, me] = turned[r, :, own, :]

    def relay(r):
        for e in (4, 6, 2):
            g_copy(r, e).wait()
            g_pass(r, e).start()

    def arrive(r):
        g_copy(r, 1).wait()
        for e in (2, 4, 6):
            g_pass(r, e).wait()

    def collect(r, j):
        for e in range(1, DEVS):
            o_copy(r, e).wait()
        chunk_of = lax.broadcasted_iota(jnp.int32, (ROWS, BOND), 1) // 16
        for g in range(2):
            x = [got[r, p, g] for p in range(DEVS)]
            for bit in (1, 2, 4):
                odd = lax.rem(chunk_of // bit, 2) == 1
                for p in range(DEVS):
                    if p & bit:
                        continue
                    low, high = x[p], x[p + bit]
                    x[p] = jnp.where(odd, pltpu.roll(high, 16 * bit, 1), low)
                    x[p + bit] = jnp.where(odd, high, pltpu.roll(low, BOND - 16 * bit, 1))
            for q in range(8):
                pair = g * 8 + q
                out_ref[r, j + 1, :, pair // 4, pair % 4, :] = x[q]

    acc[...] = jnp.zeros_like(acc)

    @pl.loop(0, DEVS)
    def _(d):
        for e in range(1, DEVS):

            @pl.when(d == e)
            def _():
                r_copy(e).wait()
                w_copy(e).wait()

        widen(d)
        for e in range(1, DEVS):

            @pl.when(d == e)
            def _():
                if e in (1, 2, 4, 6):
                    l_copy(e).wait()
                    if e > 1:
                        l_pass(e).start()
                else:
                    l_pass(e - 1).wait()

        chunk(0, d, y_buf0, z_buf0, False)

    share(0)

    @pl.loop(1, 2 * STEPS)
    def _(t):
        r, j = lax.rem(t, 2), t // 2
        pr, pj = 1 - r, (t - 1) // 2

        @pl.when(t >= 2)
        def _():
            arrive(r)

        for d in range(DEVS):
            chunk(r, d, (y_buf0, y_buf1)[d % 2], (z_buf0, z_buf1)[d % 2], d == 0)
            if d == FORM_AFTER:

                @pl.when(t < 2 * STEPS - 1)
                def _():
                    advance(pr, pj, False)

                @pl.when(t == 2 * STEPS - 1)
                def _():
                    advance(pr, pj, True)

            if d == COLLECT_AFTER:

                @pl.when(t >= 2)
                def _():
                    collect(r, j - 1)

        share(r)

        @pl.when(t < 2 * STEPS - 1)
        def _():
            relay(pr)

        post(pr)

    advance(1, STEPS - 1, True)
    post(1)
    collect(0, STEPS - 1)
    collect(1, STEPS - 1)
    alpha_ref[...] = numbers[0, 0:2, 0:STEPS]
    beta_ref[...] = numbers[1, 0:2, 0:STEPS]


def solution(mesh):
    def device_fn(psi, left_loc, phys_loc, right_loc):
        roots = psi.shape[0]
        vm = pl.BlockSpec(memory_space=pltpu.VMEM)
        dma = pltpu.SemaphoreType.DMA
        return pl.pallas_call(
            kernel,
            out_shape=(
                jax.ShapeDtypeStruct((roots, STEPS + 1, ROWS) + psi.shape[2:], F32),
                jax.ShapeDtypeStruct((roots, STEPS), F32),
                jax.ShapeDtypeStruct((roots, STEPS), F32),
            ),
            in_specs=[vm] * 4,
            out_specs=(vm, vm, vm),
            scratch_shapes=[
                pltpu.VMEM((DEVS, TERMS, BOND, BOND), BF16),
                pltpu.VMEM((DEVS, TERMS, ROWS, BOND), BF16),
                pltpu.VMEM((DEVS, TERMS, PAIRS * PAIRS), BF16),
                pltpu.VMEM((DEVS, TERMS, BOND, BOND), BF16),
                pltpu.VMEM((roots, DEVS, PAIRS, ROWS, BOND), BF16),
                pltpu.VMEM((TERMS, 2, BOND, BOND), BF16),
                pltpu.VMEM((TERMS, 2, BOND, BOND), BF16),
                pltpu.VMEM((2 * BOND, TERMS * BOND), BF16),
                pltpu.VMEM((2 * BOND, TERMS * BOND), BF16),
                pltpu.VMEM((2 * BOND, BOND), F32),
                pltpu.VMEM((roots, 2 * BOND, BOND), F32),
                pltpu.VMEM((roots, 2 * BOND, BOND), F32),
                pltpu.VMEM((roots, 2 * BOND, BOND), F32),
                pltpu.VMEM((roots, 8, BOND), F32),
                pltpu.VMEM((roots, DEVS, 8, BOND), F32),
                pltpu.VMEM((roots, 8, BOND), F32),
                pltpu.VMEM((roots, 2, BOND, BOND), F32),
                pltpu.VMEM((roots, DEVS, 2, ROWS, BOND), F32),
                pltpu.VMEM((PAIRS, BOND, BOND), F32),
                pltpu.VMEM((2, 8, BOND), F32),
                dma((DEVS,)), dma((DEVS,)), dma((DEVS,)), dma((DEVS,)), dma((DEVS,)), dma((DEVS,)),
                dma((roots, DEVS)), dma((roots, DEVS)), dma((roots, DEVS)), dma((roots, DEVS)),
                dma((roots, DEVS)), dma((roots, DEVS)),
            ],
            compiler_params=pltpu.CompilerParams(
                collective_id=0, has_side_effects=True, vmem_limit_bytes=56 * 1024 * 1024
            ),
        )(psi, left_loc, right_loc, phys_loc.reshape(TERMS, PAIRS * PAIRS))

    return jax.shard_map(
        device_fn, mesh=mesh, in_specs=(P(), P("terms"), P("terms"), P("terms")),
        out_specs=(P(None, None, "terms"), P(), P()), check_vma=False,
    )
```

```python
import functools

import jax
import jax.numpy as jnp
from jax import lax
from jax.experimental import pallas as pl
from jax.experimental.pallas import tpu as pltpu
from jax.sharding import PartitionSpec as P

STEPS = 6
DEVS = 8
TERMS = 16
PAIRS = 16
BOND = 128
ROWS = 16
N_ELEMS = float(BOND * PAIRS * BOND)
FORM_BEFORE = 0
COLLECT_BEFORE = 4
MESH = pl.DeviceIdType.MESH
F32 = jnp.float32
BF16 = jnp.bfloat16


def flip(dev, bits):
    out = dev
    if bits & 1:
        out = out + 1 - 2 * lax.rem(dev, 2)
    if bits & 2:
        out = out + 2 - 4 * lax.rem(dev // 2, 2)
    if bits & 4:
        out = out + 4 - 8 * lax.rem(dev // 4, 2)
    return out


def total(x):
    return jnp.sum(jnp.sum(x, axis=0, keepdims=True), axis=1, keepdims=True)


def kernel(
    psi_ref, left_ref, right_ref, phys_ref, out_ref, alpha_ref, beta_ref,
    left, right, phys, wide, v_in, y_buf, z_buf0, z_buf1, acc, sig, v_cur, v_prev, beta_old, stats, mine,
    turned, got, across, numbers, dense,
    r_send, r_recv, w_send, w_recv, l_send, l_recv, s_send, s_recv, g_send, g_recv, o_send, o_recv,
):
    me = lax.axis_index("terms")
    peers = {e: flip(me, e) for e in range(1, DEVS)}

    barrier = pltpu.get_barrier_semaphore()
    for e in range(1, DEVS):
        pl.semaphore_signal(barrier, inc=1, device_id=(peers[e],), device_id_type=MESH)
    pl.semaphore_wait(barrier, DEVS - 1)

    def copy(src, dst, send, recv, e):
        return pltpu.make_async_remote_copy(
            src_ref=src, dst_ref=dst, send_sem=send, recv_sem=recv, device_id=(peers[e],), device_id_type=MESH
        )

    def r_copy(e):
        rows = pl.ds(pl.multiple_of(peers[e] * ROWS, ROWS), ROWS)
        return copy(right_ref.at[:, rows, :], right.at[e], r_send.at[e], r_recv.at[e], e)

    def w_copy(e):
        return copy(dense, phys.at[e], w_send.at[e], w_recv.at[e], e)

    def l_copy(e):
        return copy(left_ref, left.at[e], l_send.at[e], l_recv.at[e], e)

    def l_pass(e):
        return copy(left.at[e], left.at[e + 1], l_send.at[e + 1], l_recv.at[e + 1], 1)

    def s_copy(r, e):
        return copy(mine.at[r], stats.at[r, me], s_send.at[r, e], s_recv.at[r, e], e)

    def g_copy(r, g, e):
        slot = v_in.at[r, me, g * 8 : (g + 1) * 8]
        return copy(slot, slot, g_send.at[r, g, e], g_recv.at[r, g, e], e)

    def g_pass(r, g, e):
        slot = v_in.at[r, peers[e], g * 8 : (g + 1) * 8]
        return copy(slot, slot, g_send.at[r, g, e + 1], g_recv.at[r, g, e + 1], 1)

    def o_copy(r, e):
        rows = pl.ds(pl.multiple_of(peers[e] * ROWS, ROWS), ROWS)
        return copy(turned.at[r, :, rows, :], got.at[r, me], o_send.at[r, e], o_recv.at[r, e], e)

    w_own = phys_ref[...].astype(F32)
    row_u = lax.broadcasted_iota(jnp.int32, (PAIRS, PAIRS * PAIRS), 0)
    col_qu = lax.broadcasted_iota(jnp.int32, (PAIRS, PAIRS * PAIRS), 1)
    flat = jnp.zeros((TERMS, PAIRS * PAIRS), F32)
    for q in range(PAIRS):
        put = jnp.where(col_qu == row_u + q * PAIRS, 1.0, 0.0).astype(BF16)
        flat += jnp.dot(w_own[:, q, :].astype(BF16), put, preferred_element_type=F32)
    dense[...] = flat.astype(BF16)
    for both in ((1,), (2, 3), (4, 5), (6, 7)):
        for e in both:
            r_copy(e).start()
            w_copy(e).start()
        l_copy(2 * (both[0] // 2) if both[0] > 1 else 1).start()
    own = pl.ds(pl.multiple_of(me * ROWS, ROWS), ROWS)
    right[0] = right_ref[:, own, :]
    phys[0] = dense[...]
    left[0] = left_ref[...]
    v_prev[...] = jnp.zeros_like(v_prev)
    beta_old[...] = jnp.zeros_like(beta_old)
    numbers[...] = jnp.zeros_like(numbers)

    @pl.loop(0, 2)
    def _(r):
        acc[0:BOND, :] = jnp.zeros((BOND, BOND), F32)

        @pl.loop(0, 4)
        def _(s):
            for t in range(4):
                x = psi_ref[r, :, s, t, :]
                acc[0:BOND, :] += x * x
                across[s * 4 + t] = x.T

        norm = jnp.sqrt(total(acc[0:BOND, :]) / N_ELEMS)

        @pl.loop(0, PAIRS)
        def _(u):
            v_in[r, :, u] = (across[u] / norm).astype(BF16).reshape(DEVS, ROWS, BOND)
            two = across[u, own, :] / norm
            row = pl.multiple_of(u * 8, 8)
            v_cur[r, pl.ds(row, 8), :] = two[0:8]
            v_cur[r, pl.ds(row + BOND, 8), :] = two[8:16]

        out_ref[r, 0] = psi_ref[r, own] / norm.reshape(1, 1, 1, 1)

    sub = lax.broadcasted_iota(jnp.int32, (8, BOND), 0)
    lane = lax.broadcasted_iota(jnp.int32, (8, BOND), 1)
    eye = jnp.where(lax.rem(lane, 8) == sub, 1.0, 0.0).astype(F32)
    pick_row = lax.broadcasted_iota(jnp.int32, (PAIRS * PAIRS, BOND), 0)
    pick_col = lax.broadcasted_iota(jnp.int32, (PAIRS * PAIRS, BOND), 1) // 8

    def widen(d):
        w_d = phys[d]
        spread = []
        for q in range(PAIRS):
            pick = jnp.where(pick_row == pick_col + q * PAIRS, 1.0, 0.0).astype(BF16)
            spread.append(jnp.dot(w_d, pick, preferred_element_type=F32))
        for k in range(TERMS):
            for q in range(0, PAIRS, 2):
                two = [jnp.broadcast_to(spread[q + i][k : k + 1, :], (8, BOND)) * eye for i in range(2)]
                wide[d, k, q * 8 : q * 8 + 16, :] = jnp.concatenate(two, axis=0).astype(BF16)

    def form_y(r, d, pairs):
        r_d = right[d].reshape(TERMS * ROWS, BOND)
        for u in pairs:
            v_u = jnp.concatenate([v_in[r, :, u + i].reshape(BOND, BOND) for i in range(2)], axis=1)
            y = jnp.dot(r_d, v_u, preferred_element_type=F32).reshape(TERMS, 2, 8, 2 * BOND)
            y = jnp.concatenate([y[..., :BOND], y[..., BOND:]], axis=2)
            y_buf[d, :, :, u * 8 : u * 8 + 16, :] = y.astype(BF16)

    def form_out(d, z_buf, first):
        for k in range(TERMS):
            y_k = jnp.concatenate([y_buf[d, k, 0], y_buf[d, k, 1]], axis=1)
            z = jnp.dot(wide[d, k], y_k, preferred_element_type=F32).astype(BF16)
            for h in range(2):
                z_buf[h * BOND : (h + 1) * BOND, k * BOND : (k + 1) * BOND] = z[:, h * BOND : (h + 1) * BOND]
        part = jnp.dot(z_buf[...], left[d].reshape(TERMS * BOND, BOND), preferred_element_type=F32)
        if first:
            acc[...] = part
        else:
            acc[...] += part

    def share(r):
        s, v, vp = acc[...], v_cur[r], v_prev[r]
        d_p, n_p = total(s * v), total(v * v)
        guess = jnp.where(n_p > 0.0, d_p / jnp.where(n_p > 0.0, n_p, 1.0), 0.0)
        s = s - guess * v - beta_old[r, 0:1, :] * vp
        sig[r] = s
        rows = [d_p, n_p, guess, total(s * s), total(s * v)]
        tile = jnp.zeros((8, BOND), F32)
        for i, row in enumerate(rows):
            tile = jnp.where(sub == i, row, tile)
        mine[r] = tile
        stats[r, me] = tile
        for e in (6, 7, 2, 3, 4, 5, 1):
            s_copy(r, e).start()

    def advance(r, j, last):
        for e in range(1, DEVS):
            s_copy(r, e).wait()
        alpha = jnp.zeros((1, BOND), F32)
        for p in range(DEVS):
            alpha = alpha + stats[r, p, 0:1, :]
        alpha = alpha / N_ELEMS
        square = jnp.zeros((1, BOND), F32)
        for p in range(DEVS):
            d_p = alpha - stats[r, p, 2:3, :]
            square = square + (stats[r, p, 3:4, :] - 2.0 * d_p * stats[r, p, 4:5, :] + d_p * d_p * stats[r, p, 1:2, :])
        beta = jnp.sqrt(jnp.maximum(square, 0.0) / N_ELEMS)
        shift = alpha - mine[r, 2:3, :]
        v = v_cur[r]
        nxt = (sig[r] - shift * v) / beta
        v_prev[r] = v
        v_cur[r] = nxt
        beta_old[r] = jnp.broadcast_to(beta, (8, BOND))
        here = jnp.logical_and(sub == r, lane == j)
        numbers[0] = jnp.where(here, alpha, numbers[0])
        numbers[1] = jnp.where(here, beta, numbers[1])
        halves = nxt.reshape(2, PAIRS, 8, BOND)
        joined = jnp.concatenate([halves[0], halves[1]], axis=1)

        @pl.when(jnp.logical_not(last))
        def _():
            v_in[r, me] = joined.astype(BF16)
            for g in range(2):
                for e in (6, 2, 4, 1):
                    g_copy(r, g, e).start()

        for g in range(2):
            turned[r, g] = joined[g * 8 : (g + 1) * 8].reshape(BOND, BOND).T

    def post(r):
        for e in (6, 7, 2, 3, 4, 5, 1):
            o_copy(r, e).start()
        got[r, me] = turned[r, :, own, :]

    def relay(r):
        for g in range(2):
            for e in (4, 6, 2):
                g_copy(r, g, e).wait()
                g_pass(r, g, e).start()

    def arrive(r, g):
        g_copy(r, g, 1).wait()
        for e in (4, 6, 2):
            g_pass(r, g, e).wait()

    def collect(r, j):
        for e in range(1, DEVS):
            o_copy(r, e).wait()
        chunk_of = lax.broadcasted_iota(jnp.int32, (ROWS, BOND), 1) // 16
        for g in range(2):
            x = [got[r, p, g] for p in range(DEVS)]
            for bit in (1, 2, 4):
                odd = lax.rem(chunk_of // bit, 2) == 1
                for p in range(DEVS):
                    if p & bit:
                        continue
                    low, high = x[p], x[p + bit]
                    x[p] = jnp.where(odd, pltpu.roll(high, 16 * bit, 1), low)
                    x[p + bit] = jnp.where(odd, high, pltpu.roll(low, BOND - 16 * bit, 1))
            for q in range(8):
                pair = g * 8 + q
                out_ref[r, j + 1, :, pair // 4, pair % 4, :] = x[q]

    acc[...] = jnp.zeros_like(acc)

    @pl.loop(0, DEVS)
    def _(d):
        for e in range(1, DEVS):

            @pl.when(d == e)
            def _():
                r_copy(e).wait()
                w_copy(e).wait()

        widen(d)
        for e in range(1, DEVS):

            @pl.when(d == e)
            def _():
                if e in (1, 2, 4, 6):
                    l_copy(e).wait()
                    if e > 1:
                        l_pass(e).start()
                else:
                    l_pass(e - 1).wait()

        form_y(0, d, range(0, PAIRS, 2))
        form_out(d, z_buf0, False)

    share(0)

    @pl.loop(1, 2 * STEPS)
    def _(t):
        r, j = lax.rem(t, 2), t // 2
        pr, pj = 1 - r, (t - 1) // 2

        for g in range(2):

            @pl.when(t >= 2)
            def _():
                arrive(r, g)

            for u in range(g * 8, (g + 1) * 8, 2):
                for d in range(DEVS):
                    form_y(r, d, (u,))

        for d in range(DEVS):
            if d == FORM_BEFORE:
                advance(pr, pj, t == 2 * STEPS - 1)
            if d == COLLECT_BEFORE:

                @pl.when(t >= 2)
                def _():
                    collect(r, j - 1)

            form_out(d, (z_buf0, z_buf1)[d % 2], d == 0)

        share(r)

        @pl.when(t < 2 * STEPS - 1)
        def _():
            relay(pr)

        post(pr)

    advance(1, STEPS - 1, jnp.bool_(True))
    post(1)
    collect(0, STEPS - 1)
    collect(1, STEPS - 1)
    alpha_ref[...] = numbers[0, 0:2, 0:STEPS]
    beta_ref[...] = numbers[1, 0:2, 0:STEPS]


def solution(mesh):
    def device_fn(psi, left_loc, phys_loc, right_loc):
        roots = psi.shape[0]
        vm = pl.BlockSpec(memory_space=pltpu.VMEM)
        dma = pltpu.SemaphoreType.DMA
        return pl.pallas_call(
            kernel,
            out_shape=(
                jax.ShapeDtypeStruct((roots, STEPS + 1, ROWS) + psi.shape[2:], F32),
                jax.ShapeDtypeStruct((roots, STEPS), F32),
                jax.ShapeDtypeStruct((roots, STEPS), F32),
            ),
            in_specs=[vm] * 4,
            out_specs=(vm, vm, vm),
            scratch_shapes=[
                pltpu.VMEM((DEVS, TERMS, BOND, BOND), BF16),
                pltpu.VMEM((DEVS, TERMS, ROWS, BOND), BF16),
                pltpu.VMEM((DEVS, TERMS, PAIRS * PAIRS), BF16),
                pltpu.VMEM((DEVS, TERMS, BOND, BOND), BF16),
                pltpu.VMEM((roots, DEVS, PAIRS, ROWS, BOND), BF16),
                pltpu.VMEM((DEVS, TERMS, 2, BOND, BOND), BF16),
                pltpu.VMEM((2 * BOND, TERMS * BOND), BF16),
                pltpu.VMEM((2 * BOND, TERMS * BOND), BF16),
                pltpu.VMEM((2 * BOND, BOND), F32),
                pltpu.VMEM((roots, 2 * BOND, BOND), F32),
                pltpu.VMEM((roots, 2 * BOND, BOND), F32),
                pltpu.VMEM((roots, 2 * BOND, BOND), F32),
                pltpu.VMEM((roots, 8, BOND), F32),
                pltpu.VMEM((roots, DEVS, 8, BOND), F32),
                pltpu.VMEM((roots, 8, BOND), F32),
                pltpu.VMEM((roots, 2, BOND, BOND), F32),
                pltpu.VMEM((roots, DEVS, 2, ROWS, BOND), F32),
                pltpu.VMEM((PAIRS, BOND, BOND), F32),
                pltpu.VMEM((2, 8, BOND), F32),
                pltpu.VMEM((TERMS, PAIRS * PAIRS), BF16),
                dma((DEVS,)), dma((DEVS,)), dma((DEVS,)), dma((DEVS,)), dma((DEVS,)), dma((DEVS,)),
                dma((roots, DEVS)), dma((roots, DEVS)), dma((roots, 2, DEVS)), dma((roots, 2, DEVS)),
                dma((roots, DEVS)), dma((roots, DEVS)),
            ],
            compiler_params=pltpu.CompilerParams(
                collective_id=0, has_side_effects=True, vmem_limit_bytes=56 * 1024 * 1024
            ),
        )(psi, left_loc, right_loc, phys_loc)

    return jax.shard_map(
        device_fn, mesh=mesh, in_specs=(P(), P("terms"), P("terms"), P("terms")),
        out_specs=(P(None, None, "terms"), P(), P()), check_vma=False,
    )
```

```python
import functools

import jax
import jax.numpy as jnp
from jax import lax
from jax.experimental import pallas as pl
from jax.experimental.pallas import tpu as pltpu
from jax.sharding import PartitionSpec as P

STEPS = 6
DEVS = 8
TERMS = 16
PAIRS = 16
BOND = 128
ROWS = 16
N_ELEMS = float(BOND * PAIRS * BOND)
FORM_BEFORE = 0
COLLECT_BEFORE = 4
POST_BEFORE = 6
MESH = pl.DeviceIdType.MESH
F32 = jnp.float32
BF16 = jnp.bfloat16


def flip(dev, bits):
    out = dev
    if bits & 1:
        out = out + 1 - 2 * lax.rem(dev, 2)
    if bits & 2:
        out = out + 2 - 4 * lax.rem(dev // 2, 2)
    if bits & 4:
        out = out + 4 - 8 * lax.rem(dev // 4, 2)
    return out


def total(x):
    return jnp.sum(jnp.sum(x, axis=0, keepdims=True), axis=1, keepdims=True)


def kernel(
    psi_ref, left_ref, right_ref, phys_ref, out_ref, alpha_ref, beta_ref,
    left, right, phys, wide, v_in, y_buf, z_buf0, z_buf1, acc, sig, v_cur, v_prev, beta_old, stats, mine,
    turned, got, got_end, across, numbers, dense,
    r_send, r_recv, w_send, w_recv, l_send, l_recv, s_send, s_recv, g_send, g_recv, o_send, o_recv, e_send, e_recv,
):
    me = lax.axis_index("terms")
    peers = {e: flip(me, e) for e in range(1, DEVS)}

    barrier = pltpu.get_barrier_semaphore()
    for e in range(1, DEVS):
        pl.semaphore_signal(barrier, inc=1, device_id=(peers[e],), device_id_type=MESH)
    pl.semaphore_wait(barrier, DEVS - 1)

    def copy(src, dst, send, recv, e):
        return pltpu.make_async_remote_copy(
            src_ref=src, dst_ref=dst, send_sem=send, recv_sem=recv, device_id=(peers[e],), device_id_type=MESH
        )

    def r_copy(e):
        rows = pl.ds(pl.multiple_of(peers[e] * ROWS, ROWS), ROWS)
        return copy(right_ref.at[:, rows, :], right.at[e], r_send.at[e], r_recv.at[e], e)

    def w_copy(e):
        return copy(dense, phys.at[e], w_send.at[e], w_recv.at[e], e)

    def half(x):
        return pl.ds(x * (TERMS // 2), TERMS // 2)

    def l_copy(e, x):
        return copy(left_ref.at[half(x)], left.at[e, half(x)], l_send.at[e, x], l_recv.at[e, x], e)

    def l_far(x):
        e = (2, 4)[x]
        return copy(left.at[e, half(x)], left.at[6, half(x)], l_send.at[6, x], l_recv.at[6, x], 6 - e)

    def l_pass(e, x):
        return copy(left.at[e, half(x)], left.at[e + 1, half(x)], l_send.at[e + 1, x], l_recv.at[e + 1, x], 1)

    def s_copy(r, e):
        return copy(mine.at[r], stats.at[r, me], s_send.at[r, e], s_recv.at[r, e], e)

    def g_copy(r, g, e):
        slot = v_in.at[r, me, g * 8 : (g + 1) * 8]
        return copy(slot, slot, g_send.at[r, g, e], g_recv.at[r, g, e], e)

    def g_pass(r, g, e):
        slot = v_in.at[r, peers[e], g * 8 : (g + 1) * 8]
        return copy(slot, slot, g_send.at[r, g, e + 1], g_recv.at[r, g, e + 1], 1)

    def o_copy(r, e):
        rows = pl.ds(pl.multiple_of(peers[e] * ROWS, ROWS), ROWS)
        return copy(turned.at[r, :, rows, :], got.at[r, me], o_send.at[r, e], o_recv.at[r, e], e)

    def e_copy(e):
        rows = pl.ds(pl.multiple_of(peers[e] * ROWS, ROWS), ROWS)
        return copy(turned.at[1, :, rows, :], got_end.at[me], e_send.at[e], e_recv.at[e], e)

    w_own = phys_ref[...].astype(F32)
    row_u = lax.broadcasted_iota(jnp.int32, (PAIRS, PAIRS * PAIRS), 0)
    col_qu = lax.broadcasted_iota(jnp.int32, (PAIRS, PAIRS * PAIRS), 1)
    flat = jnp.zeros((TERMS, PAIRS * PAIRS), F32)
    for q in range(PAIRS):
        put = jnp.where(col_qu == row_u + q * PAIRS, 1.0, 0.0).astype(BF16)
        flat += jnp.dot(w_own[:, q, :].astype(BF16), put, preferred_element_type=F32)
    dense[...] = flat.astype(BF16)
    for e in (6, 7, 2, 3, 4, 5, 1):
        r_copy(e).start()
        w_copy(e).start()
    for e, x in ((1, 0), (1, 1), (2, 0), (4, 1), (2, 1), (4, 0)):
        l_copy(e, x).start()
    own = pl.ds(pl.multiple_of(me * ROWS, ROWS), ROWS)
    right[0] = right_ref[:, own, :]
    phys[0] = dense[...]
    left[0] = left_ref[...]
    v_prev[...] = jnp.zeros_like(v_prev)
    beta_old[...] = jnp.zeros_like(beta_old)
    numbers[...] = jnp.zeros_like(numbers)

    @pl.loop(0, 2)
    def _(r):
        acc[0:BOND, :] = jnp.zeros((BOND, BOND), F32)

        @pl.loop(0, 4)
        def _(s):
            for t in range(4):
                x = psi_ref[r, :, s, t, :]
                acc[0:BOND, :] += x * x
                across[s * 4 + t] = x.T

        norm = jnp.sqrt(total(acc[0:BOND, :]) / N_ELEMS)

        @pl.loop(0, PAIRS)
        def _(u):
            v_in[r, :, u] = (across[u] / norm).astype(BF16).reshape(DEVS, ROWS, BOND)
            two = across[u, own, :] / norm
            row = pl.multiple_of(u * 8, 8)
            v_cur[r, pl.ds(row, 8), :] = two[0:8]
            v_cur[r, pl.ds(row + BOND, 8), :] = two[8:16]

        out_ref[r, 0] = psi_ref[r, own] / norm.reshape(1, 1, 1, 1)

    sub = lax.broadcasted_iota(jnp.int32, (8, BOND), 0)
    lane = lax.broadcasted_iota(jnp.int32, (8, BOND), 1)
    eye = jnp.where(lax.rem(lane, 8) == sub, 1.0, 0.0).astype(F32)
    pick_row = lax.broadcasted_iota(jnp.int32, (PAIRS * PAIRS, BOND), 0)
    pick_col = lax.broadcasted_iota(jnp.int32, (PAIRS * PAIRS, BOND), 1) // 8

    def widen(d):
        w_d = phys[d]
        spread = []
        for q in range(PAIRS):
            pick = jnp.where(pick_row == pick_col + q * PAIRS, 1.0, 0.0).astype(BF16)
            spread.append(jnp.dot(w_d, pick, preferred_element_type=F32))
        for k in range(TERMS):
            for q in range(0, PAIRS, 2):
                two = [jnp.broadcast_to(spread[q + i][k : k + 1, :], (8, BOND)) * eye for i in range(2)]
                wide[d, k, q * 8 : q * 8 + 16, :] = jnp.concatenate(two, axis=0).astype(BF16)

    def form_y(r, d, pairs):
        r_d = right[d].reshape(TERMS * ROWS, BOND)
        for u in pairs:
            v_u = jnp.concatenate([v_in[r, :, u + i].reshape(BOND, BOND) for i in range(2)], axis=1)
            y = jnp.dot(r_d, v_u, preferred_element_type=F32).reshape(TERMS, 2, 8, 2 * BOND)
            y = jnp.concatenate([y[..., :BOND], y[..., BOND:]], axis=2)
            y_buf[d, :, :, u * 8 : u * 8 + 16, :] = y.astype(BF16)

    def form_out(d, z_buf, first):
        for k in range(TERMS):
            y_k = jnp.concatenate([y_buf[d, k, 0], y_buf[d, k, 1]], axis=1)
            z = jnp.dot(wide[d, k], y_k, preferred_element_type=F32).astype(BF16)
            for h in range(2):
                z_buf[h * BOND : (h + 1) * BOND, k * BOND : (k + 1) * BOND] = z[:, h * BOND : (h + 1) * BOND]
        part = jnp.dot(z_buf[...], left[d].reshape(TERMS * BOND, BOND), preferred_element_type=F32)
        if first:
            acc[...] = part
        else:
            acc[...] += part

    def share(r):
        s, v, vp = acc[...], v_cur[r], v_prev[r]
        d_p, n_p = total(s * v), total(v * v)
        guess = jnp.where(n_p > 0.0, d_p / jnp.where(n_p > 0.0, n_p, 1.0), 0.0)
        s = s - guess * v - beta_old[r, 0:1, :] * vp
        sig[r] = s
        rows = [d_p, n_p, guess, total(s * s), total(s * v)]
        tile = jnp.zeros((8, BOND), F32)
        for i, row in enumerate(rows):
            tile = jnp.where(sub == i, row, tile)
        mine[r] = tile
        stats[r, me] = tile
        for e in (6, 7, 2, 3, 4, 5, 1):
            s_copy(r, e).start()

    def scalars(r, j):
        for e in range(1, DEVS):
            s_copy(r, e).wait()
        alpha = jnp.zeros((1, BOND), F32)
        for p in range(DEVS):
            alpha = alpha + stats[r, p, 0:1, :]
        alpha = alpha / N_ELEMS
        square = jnp.zeros((1, BOND), F32)
        for p in range(DEVS):
            d_p = alpha - stats[r, p, 2:3, :]
            square = square + (stats[r, p, 3:4, :] - 2.0 * d_p * stats[r, p, 4:5, :] + d_p * d_p * stats[r, p, 1:2, :])
        beta = jnp.sqrt(jnp.maximum(square, 0.0) / N_ELEMS)
        here = jnp.logical_and(sub == r, lane == j)
        numbers[0] = jnp.where(here, alpha, numbers[0])
        numbers[1] = jnp.where(here, beta, numbers[1])
        return alpha, beta

    def turn(r, joined):
        for g in range(2):
            turned[r, g] = joined[g * 8 : (g + 1) * 8].reshape(BOND, BOND).T

    def advance(r, j, last):
        alpha, beta = scalars(r, j)
        shift = alpha - mine[r, 2:3, :]
        v = v_cur[r]
        nxt = (sig[r] - shift * v) / beta
        v_prev[r] = v
        v_cur[r] = nxt
        beta_old[r] = jnp.broadcast_to(beta, (8, BOND))
        halves = nxt.reshape(2, PAIRS, 8, BOND)
        joined = jnp.concatenate([halves[0], halves[1]], axis=1)

        @pl.when(jnp.logical_not(last))
        def _():
            v_in[r, me] = joined.astype(BF16)
            for g in range(2):
                for e in (6, 2, 4, 1):
                    g_copy(r, g, e).start()

        turn(r, joined)

    def post(r):
        for e in (6, 7, 2, 3, 4, 5, 1):
            o_copy(r, e).start()
        got[r, me] = turned[r, :, own, :]

    def relay(r):
        for g in range(2):
            for e in (4, 6, 2):
                g_copy(r, g, e).wait()
                g_pass(r, g, e).start()

    def arrive(r, g):
        g_copy(r, g, 1).wait()
        for e in (4, 6, 2):
            g_pass(r, g, e).wait()

    def assemble(read):
        chunk_of = lax.broadcasted_iota(jnp.int32, (ROWS, BOND), 1) // 16
        pairs = []
        for g in range(2):
            x = [read(p, g) for p in range(DEVS)]
            for bit in (1, 2, 4):
                odd = lax.rem(chunk_of // bit, 2) == 1
                for p in range(DEVS):
                    if p & bit:
                        continue
                    low, high = x[p], x[p + bit]
                    x[p] = jnp.where(odd, pltpu.roll(high, 16 * bit, 1), low)
                    x[p + bit] = jnp.where(odd, high, pltpu.roll(low, BOND - 16 * bit, 1))
            pairs += x
        return pairs

    def collect(r, j):
        for e in range(1, DEVS):
            o_copy(r, e).wait()
        for q, x in enumerate(assemble(lambda p, g: got[r, p, g])):
            out_ref[r, j + 1, :, q // 4, q % 4, :] = x

    acc[...] = jnp.zeros_like(acc)

    @pl.loop(0, DEVS)
    def _(d):
        for e in range(1, DEVS):

            @pl.when(d == e)
            def _():
                r_copy(e).wait()
                w_copy(e).wait()

        widen(d)
        form_y(0, d, range(0, PAIRS, 2))

    @pl.loop(0, DEVS)
    def _(d):
        @pl.when(d == 1)
        def _():
            l_copy(1, 0).wait()
            l_copy(1, 1).wait()

        @pl.when(d == 2)
        def _():
            for e, x in ((2, 0), (4, 1)):
                l_copy(e, x).wait()
                l_far(x).start()
                l_pass(e, x).start()
            for e, x in ((2, 1), (4, 0)):
                l_copy(e, x).wait()
                l_pass(e, x).start()

        @pl.when(d == 6)
        def _():
            for x in range(2):
                l_far(x).wait()
                l_pass(6, x).start()

        for e in (3, 5, 7):

            @pl.when(d == e)
            def _():
                for x in range(2):
                    l_pass(e - 1, x).wait()

        form_out(d, z_buf0, False)

    share(0)

    @pl.loop(1, 2 * STEPS)
    def _(t):
        r, j = lax.rem(t, 2), t // 2
        pr, pj = 1 - r, (t - 1) // 2

        for g in range(2):

            @pl.when(t >= 2)
            def _():
                arrive(r, g)

            for u in range(g * 8, (g + 1) * 8, 2):
                for d in range(DEVS):
                    form_y(r, d, (u,))

        for d in range(DEVS):
            if d == FORM_BEFORE:
                advance(pr, pj, t == 2 * STEPS - 1)
            if d == COLLECT_BEFORE:

                @pl.when(t >= 2)
                def _():
                    collect(r, j - 1)

            if d == POST_BEFORE:
                post(pr)
            form_out(d, (z_buf0, z_buf1)[d % 2], d == 0)

        share(r)

        @pl.when(t < 2 * STEPS - 1)
        def _():
            relay(pr)

    halves = sig[1].reshape(2, PAIRS, 8, BOND)
    turn(1, jnp.concatenate([halves[0], halves[1]], axis=1))
    for e in (6, 7, 2, 3, 4, 5, 1):
        e_copy(e).start()
    got_end[me] = turned[1, :, own, :]
    collect(0, STEPS - 1)
    alpha, beta = scalars(1, STEPS - 1)
    shift = jnp.zeros((1, BOND), F32)
    for p in range(DEVS):
        shift = jnp.where(lane[0:1] // 16 == p, alpha - stats[1, p, 2:3, :], shift)
    for e in range(1, DEVS):
        e_copy(e).wait()
    for q, x in enumerate(assemble(lambda p, g: got_end[p, g])):
        v = out_ref[1, STEPS - 1, :, q // 4, q % 4, :]
        out_ref[1, STEPS, :, q // 4, q % 4, :] = (x - shift * v) / beta
    alpha_ref[...] = numbers[0, 0:2, 0:STEPS]
    beta_ref[...] = numbers[1, 0:2, 0:STEPS]


def solution(mesh):
    def device_fn(psi, left_loc, phys_loc, right_loc):
        roots = psi.shape[0]
        vm = pl.BlockSpec(memory_space=pltpu.VMEM)
        dma = pltpu.SemaphoreType.DMA
        return pl.pallas_call(
            kernel,
            out_shape=(
                jax.ShapeDtypeStruct((roots, STEPS + 1, ROWS) + psi.shape[2:], F32),
                jax.ShapeDtypeStruct((roots, STEPS), F32),
                jax.ShapeDtypeStruct((roots, STEPS), F32),
            ),
            in_specs=[vm] * 4,
            out_specs=(vm, vm, vm),
            scratch_shapes=[
                pltpu.VMEM((DEVS, TERMS, BOND, BOND), BF16),
                pltpu.VMEM((DEVS, TERMS, ROWS, BOND), BF16),
                pltpu.VMEM((DEVS, TERMS, PAIRS * PAIRS), BF16),
                pltpu.VMEM((DEVS, TERMS, BOND, BOND), BF16),
                pltpu.VMEM((roots, DEVS, PAIRS, ROWS, BOND), BF16),
                pltpu.VMEM((DEVS, TERMS, 2, BOND, BOND), BF16),
                pltpu.VMEM((2 * BOND, TERMS * BOND), BF16),
                pltpu.VMEM((2 * BOND, TERMS * BOND), BF16),
                pltpu.VMEM((2 * BOND, BOND), F32),
                pltpu.VMEM((roots, 2 * BOND, BOND), F32),
                pltpu.VMEM((roots, 2 * BOND, BOND), F32),
                pltpu.VMEM((roots, 2 * BOND, BOND), F32),
                pltpu.VMEM((roots, 8, BOND), F32),
                pltpu.VMEM((roots, DEVS, 8, BOND), F32),
                pltpu.VMEM((roots, 8, BOND), F32),
                pltpu.VMEM((roots, 2, BOND, BOND), F32),
                pltpu.VMEM((roots, DEVS, 2, ROWS, BOND), F32),
                pltpu.VMEM((DEVS, 2, ROWS, BOND), F32),
                pltpu.VMEM((PAIRS, BOND, BOND), F32),
                pltpu.VMEM((2, 8, BOND), F32),
                pltpu.VMEM((TERMS, PAIRS * PAIRS), BF16),
                dma((DEVS,)), dma((DEVS,)), dma((DEVS,)), dma((DEVS,)), dma((DEVS, 2)), dma((DEVS, 2)),
                dma((roots, DEVS)), dma((roots, DEVS)), dma((roots, 2, DEVS)), dma((roots, 2, DEVS)),
                dma((roots, DEVS)), dma((roots, DEVS)), dma((DEVS,)), dma((DEVS,)),
            ],
            compiler_params=pltpu.CompilerParams(
                collective_id=0, has_side_effects=True, vmem_limit_bytes=56 * 1024 * 1024
            ),
        )(psi, left_loc, right_loc, phys_loc)

    return jax.shard_map(
        device_fn, mesh=mesh, in_specs=(P(), P("terms"), P("terms"), P("terms")),
        out_specs=(P(None, None, "terms"), P(), P()), check_vma=False,
    )
```

```python
import functools

import jax
import jax.numpy as jnp
from jax import lax
from jax.experimental import pallas as pl
from jax.experimental.pallas import tpu as pltpu
from jax.sharding import PartitionSpec as P

STEPS = 6
DEVS = 8
TERMS = 16
PAIRS = 16
BOND = 128
ROWS = 16
N_ELEMS = float(BOND * PAIRS * BOND)
FORM_BEFORE = 0
COLLECT_BEFORE = 4
POST_BEFORE = 6
MESH = pl.DeviceIdType.MESH
F32 = jnp.float32
BF16 = jnp.bfloat16


def flip(dev, bits):
    out = dev
    if bits & 1:
        out = out + 1 - 2 * lax.rem(dev, 2)
    if bits & 2:
        out = out + 2 - 4 * lax.rem(dev // 2, 2)
    if bits & 4:
        out = out + 4 - 8 * lax.rem(dev // 4, 2)
    return out


def total(x):
    return jnp.sum(jnp.sum(x, axis=0, keepdims=True), axis=1, keepdims=True)


def kernel(
    psi_hbm, left_ref, right_ref, phys_ref, out_ref, alpha_ref, beta_ref, scale_ref,
    left, right, phys, wide, v_in, y_buf, z_buf0, z_buf1, acc, sig, v_cur, v_prev, beta_old, stats, mine,
    turned, got, got_end, across, numbers, dense, psi_ref, psi_sem,
    r_send, r_recv, w_send, w_recv, l_send, l_recv, s_send, s_recv, g_send, g_recv, o_send, o_recv, e_send, e_recv,
):
    me = lax.axis_index("terms")
    peers = {e: flip(me, e) for e in range(1, DEVS)}

    psi_copies = [pltpu.make_async_copy(psi_hbm.at[r], psi_ref.at[r], psi_sem.at[r]) for r in range(2)]
    for psi_copy in psi_copies:
        psi_copy.start()

    def copy(src, dst, send, recv, e):
        return pltpu.make_async_remote_copy(
            src_ref=src, dst_ref=dst, send_sem=send, recv_sem=recv, device_id=(peers[e],), device_id_type=MESH
        )

    def r_copy(e):
        rows = pl.ds(pl.multiple_of(peers[e] * ROWS, ROWS), ROWS)
        return copy(right_ref.at[:, rows, :], right.at[e], r_send.at[e], r_recv.at[e], e)

    def w_copy(e):
        return copy(dense, phys.at[e], w_send.at[e], w_recv.at[e], e)

    def half(x):
        return pl.ds(x * (TERMS // 2), TERMS // 2)

    def l_copy(e, x):
        return copy(left_ref.at[half(x)], left.at[e, half(x)], l_send.at[e, x], l_recv.at[e, x], e)

    def l_far(x):
        e = (2, 4)[x]
        return copy(left.at[e, half(x)], left.at[6, half(x)], l_send.at[6, x], l_recv.at[6, x], 6 - e)

    def l_pass(e, x):
        return copy(left.at[e, half(x)], left.at[e + 1, half(x)], l_send.at[e + 1, x], l_recv.at[e + 1, x], 1)

    def s_copy(r, e):
        return copy(mine.at[r], stats.at[r, me], s_send.at[r, e], s_recv.at[r, e], e)

    def g_copy(r, g, e):
        slot = v_in.at[r, me, g * 8 : (g + 1) * 8]
        return copy(slot, slot, g_send.at[r, g, e], g_recv.at[r, g, e], e)

    def g_pass(r, g, e):
        slot = v_in.at[r, peers[e], g * 8 : (g + 1) * 8]
        return copy(slot, slot, g_send.at[r, g, e + 1], g_recv.at[r, g, e + 1], 1)

    def o_copy(r, e):
        rows = pl.ds(pl.multiple_of(peers[e] * ROWS, ROWS), ROWS)
        return copy(turned.at[r, :, rows, :], got.at[r, me], o_send.at[r, e], o_recv.at[r, e], e)

    def e_copy(e):
        rows = pl.ds(pl.multiple_of(peers[e] * ROWS, ROWS), ROWS)
        return copy(turned.at[1, :, rows, :], got_end.at[me], e_send.at[e], e_recv.at[e], e)

    w_own = phys_ref[...].astype(F32)
    row_u = lax.broadcasted_iota(jnp.int32, (PAIRS, PAIRS * PAIRS), 0)
    col_qu = lax.broadcasted_iota(jnp.int32, (PAIRS, PAIRS * PAIRS), 1)
    flat = jnp.zeros((TERMS, PAIRS * PAIRS), F32)
    for q in range(PAIRS):
        put = jnp.where(col_qu == row_u + q * PAIRS, 1.0, 0.0).astype(BF16)
        flat += jnp.dot(w_own[:, q, :].astype(BF16), put, preferred_element_type=F32)
    dense[...] = flat.astype(BF16)
    barrier = pltpu.get_barrier_semaphore()
    for e in range(1, DEVS):
        pl.semaphore_signal(barrier, inc=1, device_id=(peers[e],), device_id_type=MESH)
    pl.semaphore_wait(barrier, DEVS - 1)

    for e in (1, 2, 4, 3, 5, 6, 7):
        r_copy(e).start()
        w_copy(e).start()
    for e, x in ((1, 0), (1, 1), (2, 0), (4, 1), (2, 1), (4, 0)):
        l_copy(e, x).start()
    own = pl.ds(pl.multiple_of(me * ROWS, ROWS), ROWS)
    right[0] = right_ref[:, own, :]
    phys[0] = dense[...]
    left[0] = left_ref[...]
    v_prev[...] = jnp.zeros_like(v_prev)
    beta_old[...] = jnp.zeros_like(beta_old)
    numbers[...] = jnp.zeros_like(numbers)

    for psi_copy in psi_copies:
        psi_copy.wait()

    @pl.loop(0, 2)
    def _(r):
        acc[0:BOND, :] = jnp.zeros((BOND, BOND), F32)

        @pl.loop(0, 4)
        def _(s):
            for t in range(4):
                x = psi_ref[r, :, s, t, :]
                acc[0:BOND, :] += x * x
                across[s * 4 + t] = x.T

        norm = jnp.sqrt(total(acc[0:BOND, :]) / N_ELEMS)

        @pl.loop(0, PAIRS)
        def _(u):
            v_in[r, :, u] = (across[u] / norm).astype(BF16).reshape(DEVS, ROWS, BOND)
            two = across[u, own, :] / norm
            row = pl.multiple_of(u * 8, 8)
            v_cur[r, pl.ds(row, 8), :] = two[0:8]
            v_cur[r, pl.ds(row + BOND, 8), :] = two[8:16]

        out_ref[r, 0] = psi_ref[r, own] / norm.reshape(1, 1, 1, 1)

    sub = lax.broadcasted_iota(jnp.int32, (8, BOND), 0)
    lane = lax.broadcasted_iota(jnp.int32, (8, BOND), 1)
    eye = jnp.where(lax.rem(lane, 8) == sub, 1.0, 0.0).astype(F32)
    pick_row = lax.broadcasted_iota(jnp.int32, (PAIRS * PAIRS, BOND), 0)
    pick_col = lax.broadcasted_iota(jnp.int32, (PAIRS * PAIRS, BOND), 1) // 8

    def widen(d):
        w_d = phys[d]
        spread = []
        for q in range(PAIRS):
            pick = jnp.where(pick_row == pick_col + q * PAIRS, 1.0, 0.0).astype(BF16)
            spread.append(jnp.dot(w_d, pick, preferred_element_type=F32))
        for k in range(TERMS):
            for q in range(0, PAIRS, 2):
                two = [jnp.broadcast_to(spread[q + i][k : k + 1, :], (8, BOND)) * eye for i in range(2)]
                wide[d, k, q * 8 : q * 8 + 16, :] = jnp.concatenate(two, axis=0).astype(BF16)

    def form_y(r, d, pairs):
        r_d = right[d].reshape(TERMS * ROWS, BOND)
        for u in pairs:
            v_u = jnp.concatenate([v_in[r, :, u + i].reshape(BOND, BOND) for i in range(2)], axis=1)
            y = jnp.dot(r_d, v_u, preferred_element_type=F32).reshape(TERMS, 2, 8, 2 * BOND)
            y = jnp.concatenate([y[..., :BOND], y[..., BOND:]], axis=2)
            y_buf[d, :, :, u * 8 : u * 8 + 16, :] = y.astype(BF16)

    def form_out(d, z_buf, first):
        for k in range(TERMS):
            y_k = jnp.concatenate([y_buf[d, k, 0], y_buf[d, k, 1]], axis=1)
            z = jnp.dot(wide[d, k], y_k, preferred_element_type=F32).astype(BF16)
            for h in range(2):
                z_buf[h * BOND : (h + 1) * BOND, k * BOND : (k + 1) * BOND] = z[:, h * BOND : (h + 1) * BOND]
        part = jnp.dot(z_buf[...], left[d].reshape(TERMS * BOND, BOND), preferred_element_type=F32)
        if first:
            acc[...] = part
        else:
            acc[...] += part

    def share(r):
        s, v, vp = acc[...], v_cur[r], v_prev[r]
        d_p, n_p = total(s * v), total(v * v)
        guess = jnp.where(n_p > 0.0, d_p / jnp.where(n_p > 0.0, n_p, 1.0), 0.0)
        s = s - guess * v - beta_old[r, 0:1, :] * vp
        sig[r] = s
        rows = [d_p, n_p, guess, total(s * s), total(s * v)]
        tile = jnp.zeros((8, BOND), F32)
        for i, row in enumerate(rows):
            tile = jnp.where(sub == i, row, tile)
        mine[r] = tile
        stats[r, me] = tile
        for e in (6, 7, 2, 3, 4, 5, 1):
            s_copy(r, e).start()

    def scalars(r, j):
        for e in range(1, DEVS):
            s_copy(r, e).wait()
        alpha = jnp.zeros((1, BOND), F32)
        for p in range(DEVS):
            alpha = alpha + stats[r, p, 0:1, :]
        alpha = alpha / N_ELEMS
        square = jnp.zeros((1, BOND), F32)
        for p in range(DEVS):
            d_p = alpha - stats[r, p, 2:3, :]
            square = square + (stats[r, p, 3:4, :] - 2.0 * d_p * stats[r, p, 4:5, :] + d_p * d_p * stats[r, p, 1:2, :])
        beta = jnp.sqrt(jnp.maximum(square, 0.0) / N_ELEMS)
        here = jnp.logical_and(sub == r, lane == j)
        numbers[0] = jnp.where(here, alpha, numbers[0])
        numbers[1] = jnp.where(here, beta, numbers[1])
        return alpha, beta

    def turn(r, joined):
        for g in range(2):
            turned[r, g] = joined[g * 8 : (g + 1) * 8].reshape(BOND, BOND).T

    def advance(r, j, last):
        alpha, beta = scalars(r, j)
        shift = alpha - mine[r, 2:3, :]
        v = v_cur[r]
        nxt = (sig[r] - shift * v) / beta
        v_prev[r] = v
        v_cur[r] = nxt
        beta_old[r] = jnp.broadcast_to(beta, (8, BOND))
        halves = nxt.reshape(2, PAIRS, 8, BOND)
        joined = jnp.concatenate([halves[0], halves[1]], axis=1)

        @pl.when(jnp.logical_not(last))
        def _():
            v_in[r, me] = joined.astype(BF16)
            for g in range(2):
                for e in (6, 4, 2, 1):
                    g_copy(r, g, e).start()

        turn(r, joined)

    def post(r):
        for e in (6, 7, 2, 3, 4, 5, 1):
            o_copy(r, e).start()
        got[r, me] = turned[r, :, own, :]

    def relay(r):
        for g in range(2):
            for e in (4, 6, 2):
                g_copy(r, g, e).wait()
                g_pass(r, g, e).start()

    def arrive(r, g):
        g_copy(r, g, 1).wait()
        for e in (4, 6, 2):
            g_pass(r, g, e).wait()

    def assemble(read):
        chunk_of = lax.broadcasted_iota(jnp.int32, (ROWS, BOND), 1) // 16
        pairs = []
        for g in range(2):
            x = [read(p, g) for p in range(DEVS)]
            for bit in (1, 2, 4):
                odd = lax.rem(chunk_of // bit, 2) == 1
                for p in range(DEVS):
                    if p & bit:
                        continue
                    low, high = x[p], x[p + bit]
                    x[p] = jnp.where(odd, pltpu.roll(high, 16 * bit, 1), low)
                    x[p + bit] = jnp.where(odd, high, pltpu.roll(low, BOND - 16 * bit, 1))
            pairs += x
        return pairs

    def collect(r, j):
        for e in range(1, DEVS):
            o_copy(r, e).wait()
        for q, x in enumerate(assemble(lambda p, g: got[r, p, g])):
            out_ref[r, j + 1, :, q // 4, q % 4, :] = x

    acc[...] = jnp.zeros_like(acc)

    @pl.loop(0, DEVS)
    def _(d):
        for e in range(1, DEVS):

            @pl.when(d == e)
            def _():
                r_copy(e).wait()
                w_copy(e).wait()

        widen(d)
        form_y(0, d, range(0, PAIRS, 2))

    @pl.loop(0, DEVS)
    def _(d):
        @pl.when(d == 1)
        def _():
            l_copy(1, 0).wait()
            l_copy(1, 1).wait()

        @pl.when(d == 2)
        def _():
            for e, x in ((2, 0), (4, 1)):
                l_copy(e, x).wait()
                l_far(x).start()
                l_pass(e, x).start()
            for e, x in ((2, 1), (4, 0)):
                l_copy(e, x).wait()
                l_pass(e, x).start()

        @pl.when(d == 6)
        def _():
            for x in range(2):
                l_far(x).wait()
                l_pass(6, x).start()

        for e in (3, 5, 7):

            @pl.when(d == e)
            def _():
                for x in range(2):
                    l_pass(e - 1, x).wait()

        form_out(d, z_buf0, False)

    share(0)

    @pl.loop(1, 2 * STEPS)
    def _(t):
        r, j = lax.rem(t, 2), t // 2
        pr, pj = 1 - r, (t - 1) // 2

        for g in range(2):

            @pl.when(t >= 2)
            def _():
                arrive(r, g)

            for u in range(g * 8, (g + 1) * 8, 2):
                for d in range(DEVS):
                    form_y(r, d, (u,))

        for d in range(DEVS):
            if d == FORM_BEFORE:
                advance(pr, pj, t == 2 * STEPS - 1)
            if d == COLLECT_BEFORE:

                @pl.when(t >= 2)
                def _():
                    collect(r, j - 1)

            if d == POST_BEFORE:
                post(pr)
            form_out(d, (z_buf0, z_buf1)[d % 2], d == 0)

        share(r)

        @pl.when(t < 2 * STEPS - 1)
        def _():
            relay(pr)

    halves = sig[1].reshape(2, PAIRS, 8, BOND)
    turn(1, jnp.concatenate([halves[0], halves[1]], axis=1))
    for e in (6, 7, 2, 3, 4, 5, 1):
        e_copy(e).start()
    got_end[me] = turned[1, :, own, :]
    collect(0, STEPS - 1)
    alpha, beta = scalars(1, STEPS - 1)
    shift = jnp.zeros((1, BOND), F32)
    for p in range(DEVS):
        shift = jnp.where(lane[0:1] // 16 == p, alpha - stats[1, p, 2:3, :], shift)
    for e in range(1, DEVS):
        e_copy(e).wait()
    for q, x in enumerate(assemble(lambda p, g: got_end[p, g])):
        v = out_ref[1, STEPS - 1, :, q // 4, q % 4, :]
        out_ref[1, STEPS, :, q // 4, q % 4, :] = x - shift * v
    alpha_ref[...] = numbers[0, 0:2, 0:STEPS]
    beta_ref[...] = numbers[1, 0:2, 0:STEPS]
    end = jnp.logical_and(sub == 1, lane == STEPS)
    scale_ref[...] = jnp.where(end, 1.0 / beta, jnp.ones((8, BOND), F32))[0:2, 0 : STEPS + 1]


def solution(mesh):
    def device_fn(psi, left_loc, phys_loc, right_loc):
        roots = psi.shape[0]
        vm = pl.BlockSpec(memory_space=pltpu.VMEM)
        dma = pltpu.SemaphoreType.DMA
        vecs, alpha, beta, scale = pl.pallas_call(
            kernel,
            out_shape=(
                jax.ShapeDtypeStruct((roots, STEPS + 1, ROWS) + psi.shape[2:], F32),
                jax.ShapeDtypeStruct((roots, STEPS), F32),
                jax.ShapeDtypeStruct((roots, STEPS), F32),
                jax.ShapeDtypeStruct((roots, STEPS + 1), F32),
            ),
            in_specs=[pl.BlockSpec(memory_space=pl.ANY), vm, vm, vm],
            out_specs=(vm, vm, vm, vm),
            scratch_shapes=[
                pltpu.VMEM((DEVS, TERMS, BOND, BOND), BF16),
                pltpu.VMEM((DEVS, TERMS, ROWS, BOND), BF16),
                pltpu.VMEM((DEVS, TERMS, PAIRS * PAIRS), BF16),
                pltpu.VMEM((DEVS, TERMS, BOND, BOND), BF16),
                pltpu.VMEM((roots, DEVS, PAIRS, ROWS, BOND), BF16),
                pltpu.VMEM((DEVS, TERMS, 2, BOND, BOND), BF16),
                pltpu.VMEM((2 * BOND, TERMS * BOND), BF16),
                pltpu.VMEM((2 * BOND, TERMS * BOND), BF16),
                pltpu.VMEM((2 * BOND, BOND), F32),
                pltpu.VMEM((roots, 2 * BOND, BOND), F32),
                pltpu.VMEM((roots, 2 * BOND, BOND), F32),
                pltpu.VMEM((roots, 2 * BOND, BOND), F32),
                pltpu.VMEM((roots, 8, BOND), F32),
                pltpu.VMEM((roots, DEVS, 8, BOND), F32),
                pltpu.VMEM((roots, 8, BOND), F32),
                pltpu.VMEM((roots, 2, BOND, BOND), F32),
                pltpu.VMEM((roots, DEVS, 2, ROWS, BOND), F32),
                pltpu.VMEM((DEVS, 2, ROWS, BOND), F32),
                pltpu.VMEM((PAIRS, BOND, BOND), F32),
                pltpu.VMEM((2, 8, BOND), F32),
                pltpu.VMEM((TERMS, PAIRS * PAIRS), BF16),
                pltpu.VMEM(psi.shape, F32),
                dma((roots,)),
                dma((DEVS,)), dma((DEVS,)), dma((DEVS,)), dma((DEVS,)), dma((DEVS, 2)), dma((DEVS, 2)),
                dma((roots, DEVS)), dma((roots, DEVS)), dma((roots, 2, DEVS)), dma((roots, 2, DEVS)),
                dma((roots, DEVS)), dma((roots, DEVS)), dma((DEVS,)), dma((DEVS,)),
            ],
            compiler_params=pltpu.CompilerParams(
                collective_id=0, has_side_effects=True, vmem_limit_bytes=56 * 1024 * 1024
            ),
        )(psi, left_loc, right_loc, phys_loc)
        return vecs * scale[:, :, None, None, None, None], alpha, beta

    return jax.shard_map(
        device_fn, mesh=mesh, in_specs=(P(), P("terms"), P("terms"), P("terms")),
        out_specs=(P(None, None, "terms"), P(), P()), check_vma=False,
    )
```

```python
import functools

import jax
import jax.numpy as jnp
from jax import lax
from jax.experimental import pallas as pl
from jax.experimental.pallas import tpu as pltpu
from jax.sharding import PartitionSpec as P

STEPS = 6
DEVS = 8
TERMS = 16
PAIRS = 16
BOND = 128
PACKED = TERMS // 2 * BOND + 16
ROWS = 16
N_ELEMS = float(BOND * PAIRS * BOND)
FORM_BEFORE = 0
COLLECT_BEFORE = 4
POST_BEFORE = 6
MESH = pl.DeviceIdType.MESH
F32 = jnp.float32
BF16 = jnp.bfloat16


def flip(dev, bits):
    out = dev
    if bits & 1:
        out = out + 1 - 2 * lax.rem(dev, 2)
    if bits & 2:
        out = out + 2 - 4 * lax.rem(dev // 2, 2)
    if bits & 4:
        out = out + 4 - 8 * lax.rem(dev // 4, 2)
    return out


def total(x):
    return jnp.sum(jnp.sum(x, axis=0, keepdims=True), axis=1, keepdims=True)


def kernel(
    psi_hbm, left_ref, right_ref, phys_ref, out_ref, alpha_ref, beta_ref,
    left, right, phys, wide, v_in, y_buf, z_buf0, z_buf1, acc, sig, v_cur, v_prev, beta_old, stats, mine,
    turned, got, got_end, across, numbers, dense, psi_ref, psi_sem, tri,
    r_send, r_recv, w_send, w_recv, l_send, l_recv, s_send, s_recv, g_send, g_recv, o_send, o_recv, e_send, e_recv,
):
    me = lax.axis_index("terms")
    peers = {e: flip(me, e) for e in range(1, DEVS)}

    psi_copies = [pltpu.make_async_copy(psi_hbm.at[r], psi_ref.at[r], psi_sem.at[r]) for r in range(2)]
    for psi_copy in psi_copies:
        psi_copy.start()

    def copy(src, dst, send, recv, e):
        return pltpu.make_async_remote_copy(
            src_ref=src, dst_ref=dst, send_sem=send, recv_sem=recv, device_id=(peers[e],), device_id_type=MESH
        )

    def r_copy(e):
        rows = pl.ds(pl.multiple_of(peers[e] * ROWS, ROWS), ROWS)
        return copy(right_ref.at[:, rows, :], right.at[e], r_send.at[e], r_recv.at[e], e)

    def w_copy(e):
        return copy(dense, phys.at[e], w_send.at[e], w_recv.at[e], e)

    def part(x):
        return slice(0, 512) if x == 0 else slice(512, PACKED)

    def l_copy(e, x):
        return copy(tri.at[0, part(x)], tri.at[e, part(x)], l_send.at[e, x], l_recv.at[e, x], e)

    def l_far(x):
        e = (2, 4)[x]
        return copy(tri.at[e, part(x)], tri.at[6, part(x)], l_send.at[6, x], l_recv.at[6, x], 6 - e)

    def l_pass(e, x):
        return copy(tri.at[e, part(x)], tri.at[e + 1, part(x)], l_send.at[e + 1, x], l_recv.at[e + 1, x], 1)

    def s_copy(r, e):
        return copy(mine.at[r], stats.at[r, me], s_send.at[r, e], s_recv.at[r, e], e)

    def g_copy(r, g, e):
        slot = v_in.at[r, me, g * 8 : (g + 1) * 8]
        return copy(slot, slot, g_send.at[r, g, e], g_recv.at[r, g, e], e)

    def g_pass(r, g, e):
        slot = v_in.at[r, peers[e], g * 8 : (g + 1) * 8]
        return copy(slot, slot, g_send.at[r, g, e + 1], g_recv.at[r, g, e + 1], 1)

    def o_copy(r, e):
        rows = pl.ds(pl.multiple_of(peers[e] * ROWS, ROWS), ROWS)
        return copy(turned.at[r, :, rows, :], got.at[r, me], o_send.at[r, e], o_recv.at[r, e], e)

    def e_copy(e):
        rows = pl.ds(pl.multiple_of(peers[e] * ROWS, ROWS), ROWS)
        return copy(turned.at[1, :, rows, :], got_end.at[me], e_send.at[e], e_recv.at[e], e)

    row = lax.broadcasted_iota(jnp.int32, (BOND, BOND), 0)
    col = lax.broadcasted_iota(jnp.int32, (BOND, BOND), 1)
    diag_row = lax.broadcasted_iota(jnp.int32, (16, BOND), 0)
    diags = jnp.zeros((16, BOND), F32)
    for i in range(TERMS // 2):
        one, two = left_ref[2 * i].astype(F32), left_ref[2 * i + 1].astype(F32)
        tri[0, i * BOND : (i + 1) * BOND, :] = jnp.where(row < col, one, two).astype(BF16)
        diag = jnp.sum(jnp.where(row == col, one, 0.0), axis=0, keepdims=True)
        diags = jnp.where(diag_row == i, diag, diags)
    tri[0, PACKED - 16 : PACKED, :] = diags.astype(BF16)

    def unpack(d):
        diags = tri[d, PACKED - 16 : PACKED, :].astype(F32)
        for i in range(TERMS // 2):
            m = tri[d, i * BOND : (i + 1) * BOND, :].astype(F32)
            turned_m = m.T
            one = jnp.where(row < col, m, jnp.where(row > col, turned_m, diags[i : i + 1, :]))
            left[d, 2 * i] = one.astype(BF16)
            left[d, 2 * i + 1] = jnp.where(row < col, turned_m, m).astype(BF16)

    w_own = phys_ref[...].astype(F32)
    row_u = lax.broadcasted_iota(jnp.int32, (PAIRS, PAIRS * PAIRS), 0)
    col_qu = lax.broadcasted_iota(jnp.int32, (PAIRS, PAIRS * PAIRS), 1)
    flat = jnp.zeros((TERMS, PAIRS * PAIRS), F32)
    for q in range(PAIRS):
        put = jnp.where(col_qu == row_u + q * PAIRS, 1.0, 0.0).astype(BF16)
        flat += jnp.dot(w_own[:, q, :].astype(BF16), put, preferred_element_type=F32)
    dense[...] = flat.astype(BF16)
    barrier = pltpu.get_barrier_semaphore()
    for e in range(1, DEVS):
        pl.semaphore_signal(barrier, inc=1, device_id=(peers[e],), device_id_type=MESH)
    pl.semaphore_wait(barrier, DEVS - 1)

    for e in (1, 2, 4, 3, 5, 6, 7):
        r_copy(e).start()
        w_copy(e).start()
    for e, x in ((1, 0), (1, 1), (2, 0), (4, 1), (2, 1), (4, 0)):
        l_copy(e, x).start()
    own = pl.ds(pl.multiple_of(me * ROWS, ROWS), ROWS)
    right[0] = right_ref[:, own, :]
    phys[0] = dense[...]
    left[0] = left_ref[...]
    v_prev[...] = jnp.zeros_like(v_prev)
    beta_old[...] = jnp.zeros_like(beta_old)
    numbers[...] = jnp.zeros_like(numbers)

    for psi_copy in psi_copies:
        psi_copy.wait()

    @pl.loop(0, 2)
    def _(r):
        acc[0:BOND, :] = jnp.zeros((BOND, BOND), F32)

        @pl.loop(0, 4)
        def _(s):
            for t in range(4):
                x = psi_ref[r, :, s, t, :]
                acc[0:BOND, :] += x * x
                across[s * 4 + t] = x.T

        norm = jnp.sqrt(total(acc[0:BOND, :]) / N_ELEMS)

        @pl.loop(0, PAIRS)
        def _(u):
            v_in[r, :, u] = (across[u] / norm).astype(BF16).reshape(DEVS, ROWS, BOND)
            two = across[u, own, :] / norm
            row = pl.multiple_of(u * 8, 8)
            v_cur[r, pl.ds(row, 8), :] = two[0:8]
            v_cur[r, pl.ds(row + BOND, 8), :] = two[8:16]

        out_ref[r, 0] = psi_ref[r, own] / norm.reshape(1, 1, 1, 1)

    sub = lax.broadcasted_iota(jnp.int32, (8, BOND), 0)
    lane = lax.broadcasted_iota(jnp.int32, (8, BOND), 1)
    eye = jnp.where(lax.rem(lane, 8) == sub, 1.0, 0.0).astype(F32)
    pick_row = lax.broadcasted_iota(jnp.int32, (PAIRS * PAIRS, BOND), 0)
    pick_col = lax.broadcasted_iota(jnp.int32, (PAIRS * PAIRS, BOND), 1) // 8

    def widen(d):
        w_d = phys[d]
        spread = []
        for q in range(PAIRS):
            pick = jnp.where(pick_row == pick_col + q * PAIRS, 1.0, 0.0).astype(BF16)
            spread.append(jnp.dot(w_d, pick, preferred_element_type=F32))
        for k in range(TERMS):
            for q in range(0, PAIRS, 2):
                two = [jnp.broadcast_to(spread[q + i][k : k + 1, :], (8, BOND)) * eye for i in range(2)]
                wide[d, k, q * 8 : q * 8 + 16, :] = jnp.concatenate(two, axis=0).astype(BF16)

    def form_y(r, d, pairs):
        r_d = right[d].reshape(TERMS * ROWS, BOND)
        for u in pairs:
            v_u = jnp.concatenate([v_in[r, :, u + i].reshape(BOND, BOND) for i in range(2)], axis=1)
            y = jnp.dot(r_d, v_u, preferred_element_type=F32).reshape(TERMS, 2, 8, 2 * BOND)
            y = jnp.concatenate([y[..., :BOND], y[..., BOND:]], axis=2)
            y_buf[d, :, :, u * 8 : u * 8 + 16, :] = y.astype(BF16)

    def form_out(d, z_buf, first):
        for k in range(TERMS):
            y_k = jnp.concatenate([y_buf[d, k, 0], y_buf[d, k, 1]], axis=1)
            z = jnp.dot(wide[d, k], y_k, preferred_element_type=F32).astype(BF16)
            for h in range(2):
                z_buf[h * BOND : (h + 1) * BOND, k * BOND : (k + 1) * BOND] = z[:, h * BOND : (h + 1) * BOND]
        part = jnp.dot(z_buf[...], left[d].reshape(TERMS * BOND, BOND), preferred_element_type=F32)
        if first:
            acc[...] = part
        else:
            acc[...] += part

    def share(r):
        s, v, vp = acc[...], v_cur[r], v_prev[r]
        d_p, n_p = total(s * v), total(v * v)
        guess = jnp.where(n_p > 0.0, d_p / jnp.where(n_p > 0.0, n_p, 1.0), 0.0)
        s = s - guess * v - beta_old[r, 0:1, :] * vp
        sig[r] = s
        rows = [d_p, n_p, guess, total(s * s), total(s * v)]
        tile = jnp.zeros((8, BOND), F32)
        for i, row in enumerate(rows):
            tile = jnp.where(sub == i, row, tile)
        mine[r] = tile
        stats[r, me] = tile
        for e in (6, 7, 2, 3, 4, 5, 1):
            s_copy(r, e).start()

    def scalars(r, j):
        for e in range(1, DEVS):
            s_copy(r, e).wait()
        alpha = jnp.zeros((1, BOND), F32)
        for p in range(DEVS):
            alpha = alpha + stats[r, p, 0:1, :]
        alpha = alpha / N_ELEMS
        square = jnp.zeros((1, BOND), F32)
        for p in range(DEVS):
            d_p = alpha - stats[r, p, 2:3, :]
            square = square + (stats[r, p, 3:4, :] - 2.0 * d_p * stats[r, p, 4:5, :] + d_p * d_p * stats[r, p, 1:2, :])
        beta = jnp.sqrt(jnp.maximum(square, 0.0) / N_ELEMS)
        here = jnp.logical_and(sub == r, lane == j)
        numbers[0] = jnp.where(here, alpha, numbers[0])
        numbers[1] = jnp.where(here, beta, numbers[1])
        return alpha, beta

    def turn(r, joined):
        for g in range(2):
            turned[r, g] = joined[g * 8 : (g + 1) * 8].reshape(BOND, BOND).T

    def advance(r, j, last):
        alpha, beta = scalars(r, j)
        shift = alpha - mine[r, 2:3, :]
        v = v_cur[r]
        nxt = (sig[r] - shift * v) / beta
        v_prev[r] = v
        v_cur[r] = nxt
        beta_old[r] = jnp.broadcast_to(beta, (8, BOND))
        halves = nxt.reshape(2, PAIRS, 8, BOND)
        joined = jnp.concatenate([halves[0], halves[1]], axis=1)

        @pl.when(jnp.logical_not(last))
        def _():
            v_in[r, me] = joined.astype(BF16)
            for g in range(2):
                for e in (6, 4, 2, 1):
                    g_copy(r, g, e).start()

        turn(r, joined)

    def post(r):
        for e in (6, 7, 2, 3, 4, 5, 1):
            o_copy(r, e).start()
        got[r, me] = turned[r, :, own, :]

    def relay(r):
        for g in range(2):
            for e in (4, 6, 2):
                g_copy(r, g, e).wait()
                g_pass(r, g, e).start()

    def arrive(r, g):
        g_copy(r, g, 1).wait()
        for e in (4, 6, 2):
            g_pass(r, g, e).wait()

    def assemble(read):
        chunk_of = lax.broadcasted_iota(jnp.int32, (ROWS, BOND), 1) // 16
        pairs = []
        for g in range(2):
            x = [read(p, g) for p in range(DEVS)]
            for bit in (1, 2, 4):
                odd = lax.rem(chunk_of // bit, 2) == 1
                for p in range(DEVS):
                    if p & bit:
                        continue
                    low, high = x[p], x[p + bit]
                    x[p] = jnp.where(odd, pltpu.roll(high, 16 * bit, 1), low)
                    x[p + bit] = jnp.where(odd, high, pltpu.roll(low, BOND - 16 * bit, 1))
            pairs += x
        return pairs

    def collect(r, j):
        for e in range(1, DEVS):
            o_copy(r, e).wait()
        for q, x in enumerate(assemble(lambda p, g: got[r, p, g])):
            out_ref[r, j + 1, :, q // 4, q % 4, :] = x

    acc[...] = jnp.zeros_like(acc)

    @pl.loop(0, DEVS)
    def _(d):
        for e in range(1, DEVS):

            @pl.when(d == e)
            def _():
                r_copy(e).wait()
                w_copy(e).wait()

        widen(d)
        form_y(0, d, range(0, PAIRS, 2))

    @pl.loop(0, DEVS)
    def _(d):
        @pl.when(d == 1)
        def _():
            l_copy(1, 0).wait()
            l_copy(1, 1).wait()

        @pl.when(d == 2)
        def _():
            for e, x in ((2, 0), (4, 1)):
                l_copy(e, x).wait()
                l_far(x).start()
                l_pass(e, x).start()
            for e, x in ((2, 1), (4, 0)):
                l_copy(e, x).wait()
                l_pass(e, x).start()

        @pl.when(d == 6)
        def _():
            for x in range(2):
                l_far(x).wait()
                l_pass(6, x).start()

        for e in (3, 5, 7):

            @pl.when(d == e)
            def _():
                for x in range(2):
                    l_pass(e - 1, x).wait()

        @pl.when(d >= 1)
        def _():
            unpack(d)

        form_out(d, z_buf0, False)

    share(0)

    @pl.loop(1, 2 * STEPS)
    def _(t):
        r, j = lax.rem(t, 2), t // 2
        pr, pj = 1 - r, (t - 1) // 2

        for g in range(2):

            @pl.when(t >= 2)
            def _():
                arrive(r, g)

            for u in range(g * 8, (g + 1) * 8, 2):
                for d in range(DEVS):
                    form_y(r, d, (u,))

        for d in range(DEVS):
            if d == FORM_BEFORE:
                advance(pr, pj, t == 2 * STEPS - 1)
            if d == COLLECT_BEFORE:

                @pl.when(t >= 2)
                def _():
                    collect(r, j - 1)

            if d == POST_BEFORE:
                post(pr)
            form_out(d, (z_buf0, z_buf1)[d % 2], d == 0)

        share(r)

        @pl.when(t < 2 * STEPS - 1)
        def _():
            relay(pr)

    halves = sig[1].reshape(2, PAIRS, 8, BOND)
    turn(1, jnp.concatenate([halves[0], halves[1]], axis=1))
    for e in (6, 7, 2, 3, 4, 5, 1):
        e_copy(e).start()
    got_end[me] = turned[1, :, own, :]
    collect(0, STEPS - 1)
    alpha, beta = scalars(1, STEPS - 1)
    shift = jnp.zeros((1, BOND), F32)
    for p in range(DEVS):
        shift = jnp.where(lane[0:1] // 16 == p, alpha - stats[1, p, 2:3, :], shift)
    for e in range(1, DEVS):
        e_copy(e).wait()
    for q, x in enumerate(assemble(lambda p, g: got_end[p, g])):
        v = out_ref[1, STEPS - 1, :, q // 4, q % 4, :]
        out_ref[1, STEPS, :, q // 4, q % 4, :] = (x - shift * v) / beta
    alpha_ref[...] = numbers[0, 0:2, 0:STEPS]
    beta_ref[...] = numbers[1, 0:2, 0:STEPS]


def solution(mesh):
    def device_fn(psi, left_loc, phys_loc, right_loc):
        roots = psi.shape[0]
        vm = pl.BlockSpec(memory_space=pltpu.VMEM)
        dma = pltpu.SemaphoreType.DMA
        return pl.pallas_call(
            kernel,
            out_shape=(
                jax.ShapeDtypeStruct((roots, STEPS + 1, ROWS) + psi.shape[2:], F32),
                jax.ShapeDtypeStruct((roots, STEPS), F32),
                jax.ShapeDtypeStruct((roots, STEPS), F32),
            ),
            in_specs=[pl.BlockSpec(memory_space=pl.ANY), vm, vm, vm],
            out_specs=(vm, vm, vm),
            scratch_shapes=[
                pltpu.VMEM((DEVS, TERMS, BOND, BOND), BF16),
                pltpu.VMEM((DEVS, TERMS, ROWS, BOND), BF16),
                pltpu.VMEM((DEVS, TERMS, PAIRS * PAIRS), BF16),
                pltpu.VMEM((DEVS, TERMS, BOND, BOND), BF16),
                pltpu.VMEM((roots, DEVS, PAIRS, ROWS, BOND), BF16),
                pltpu.VMEM((DEVS, TERMS, 2, BOND, BOND), BF16),
                pltpu.VMEM((2 * BOND, TERMS * BOND), BF16),
                pltpu.VMEM((2 * BOND, TERMS * BOND), BF16),
                pltpu.VMEM((2 * BOND, BOND), F32),
                pltpu.VMEM((roots, 2 * BOND, BOND), F32),
                pltpu.VMEM((roots, 2 * BOND, BOND), F32),
                pltpu.VMEM((roots, 2 * BOND, BOND), F32),
                pltpu.VMEM((roots, 8, BOND), F32),
                pltpu.VMEM((roots, DEVS, 8, BOND), F32),
                pltpu.VMEM((roots, 8, BOND), F32),
                pltpu.VMEM((roots, 2, BOND, BOND), F32),
                pltpu.VMEM((roots, DEVS, 2, ROWS, BOND), F32),
                pltpu.VMEM((DEVS, 2, ROWS, BOND), F32),
                pltpu.VMEM((PAIRS, BOND, BOND), F32),
                pltpu.VMEM((2, 8, BOND), F32),
                pltpu.VMEM((TERMS, PAIRS * PAIRS), BF16),
                pltpu.VMEM(psi.shape, F32),
                dma((roots,)),
                pltpu.VMEM((DEVS, PACKED, BOND), BF16),
                dma((DEVS,)), dma((DEVS,)), dma((DEVS,)), dma((DEVS,)), dma((DEVS, 2)), dma((DEVS, 2)),
                dma((roots, DEVS)), dma((roots, DEVS)), dma((roots, 2, DEVS)), dma((roots, 2, DEVS)),
                dma((roots, DEVS)), dma((roots, DEVS)), dma((DEVS,)), dma((DEVS,)),
            ],
            compiler_params=pltpu.CompilerParams(
                collective_id=0, has_side_effects=True, vmem_limit_bytes=56 * 1024 * 1024
            ),
        )(psi, left_loc, right_loc, phys_loc)

    return jax.shard_map(
        device_fn, mesh=mesh, in_specs=(P(), P("terms"), P("terms"), P("terms")),
        out_specs=(P(None, None, "terms"), P(), P()), check_vma=False,
    )
```

```python
import functools

import jax
import jax.numpy as jnp
from jax import lax
from jax.experimental import pallas as pl
from jax.experimental.pallas import tpu as pltpu
from jax.sharding import PartitionSpec as P

STEPS = 6
DEVS = 8
TERMS = 16
PAIRS = 16
BOND = 128
PACKED = TERMS // 2 * BOND + 16
ROWS = 16
N_ELEMS = float(BOND * PAIRS * BOND)
FORM_BEFORE = 0
POST_BEFORE = 6
MESH = pl.DeviceIdType.MESH
F32 = jnp.float32
BF16 = jnp.bfloat16


def flip(dev, bits):
    out = dev
    if bits & 1:
        out = out + 1 - 2 * lax.rem(dev, 2)
    if bits & 2:
        out = out + 2 - 4 * lax.rem(dev // 2, 2)
    if bits & 4:
        out = out + 4 - 8 * lax.rem(dev // 4, 2)
    return out


def total(x):
    return jnp.sum(jnp.sum(x, axis=0, keepdims=True), axis=1, keepdims=True)


def kernel(
    psi_hbm, left_ref, right_ref, phys_ref, out_hbm, alpha_ref, beta_ref,
    left, right, phys, wide, v_in, y_buf, z_buf0, z_buf1, acc, sig, v_cur, v_prev, beta_old, stats, mine,
    turned, got, got_end, across, numbers, dense, psi_ref, psi_sem, tri, squares, out_ref, out_sem,
    r_send, r_recv, w_send, w_recv, l_send, l_recv, s_send, s_recv, g_send, g_recv, o_send, o_recv, e_send, e_recv,
):
    me = lax.axis_index("terms")
    peers = {e: flip(me, e) for e in range(1, DEVS)}

    psi_copies = [pltpu.make_async_copy(psi_hbm.at[r], psi_ref.at[r], psi_sem.at[r]) for r in range(2)]
    for psi_copy in psi_copies:
        psi_copy.start()

    def copy(src, dst, send, recv, e):
        return pltpu.make_async_remote_copy(
            src_ref=src, dst_ref=dst, send_sem=send, recv_sem=recv, device_id=(peers[e],), device_id_type=MESH
        )

    def r_copy(e):
        rows = pl.ds(pl.multiple_of(peers[e] * ROWS, ROWS), ROWS)
        return copy(right_ref.at[:, rows, :], right.at[e], r_send.at[e], r_recv.at[e], e)

    def w_copy(e):
        return copy(dense, phys.at[e], w_send.at[e], w_recv.at[e], e)

    def part(x):
        return slice(0, 512) if x == 0 else slice(512, PACKED)

    def l_copy(e, x):
        return copy(tri.at[0, part(x)], tri.at[e, part(x)], l_send.at[e, x], l_recv.at[e, x], e)

    def l_far(x):
        e = (2, 4)[x]
        return copy(tri.at[e, part(x)], tri.at[6, part(x)], l_send.at[6, x], l_recv.at[6, x], 6 - e)

    def l_pass(e, x):
        return copy(tri.at[e, part(x)], tri.at[e + 1, part(x)], l_send.at[e + 1, x], l_recv.at[e + 1, x], 1)

    def s_copy(r, e):
        return copy(mine.at[r], stats.at[r, me], s_send.at[r, e], s_recv.at[r, e], e)

    def g_copy(r, g, e):
        slot = v_in.at[r, me, g * 8 : (g + 1) * 8]
        return copy(slot, slot, g_send.at[r, g, e], g_recv.at[r, g, e], e)

    def g_pass(r, g, e):
        slot = v_in.at[r, peers[e], g * 8 : (g + 1) * 8]
        return copy(slot, slot, g_send.at[r, g, e + 1], g_recv.at[r, g, e + 1], 1)

    def o_copy(r, j, e):
        rows = pl.ds(pl.multiple_of(peers[e] * ROWS, ROWS), ROWS)
        way = lax.rem(j, 2)
        return copy(turned.at[r, :, rows, :], got.at[r, way, me], o_send.at[r, way, e], o_recv.at[r, way, e], e)

    def e_copy(e):
        rows = pl.ds(pl.multiple_of(peers[e] * ROWS, ROWS), ROWS)
        return copy(turned.at[1, :, rows, :], got_end.at[me], e_send.at[e], e_recv.at[e], e)

    row = lax.broadcasted_iota(jnp.int32, (BOND, BOND), 0)
    col = lax.broadcasted_iota(jnp.int32, (BOND, BOND), 1)
    diag_row = lax.broadcasted_iota(jnp.int32, (16, BOND), 0)
    diags = jnp.zeros((16, BOND), F32)
    for i in range(TERMS // 2):
        one, two = left_ref[2 * i].astype(F32), left_ref[2 * i + 1].astype(F32)
        tri[0, i * BOND : (i + 1) * BOND, :] = jnp.where(row < col, one, two).astype(BF16)
        diag = jnp.sum(jnp.where(row == col, one, 0.0), axis=0, keepdims=True)
        diags = jnp.where(diag_row == i, diag, diags)
    tri[0, PACKED - 16 : PACKED, :] = diags.astype(BF16)

    def unpack(d):
        diags = tri[d, PACKED - 16 : PACKED, :].astype(F32)
        for i in range(TERMS // 2):
            m = tri[d, i * BOND : (i + 1) * BOND, :].astype(F32)
            turned_m = m.T
            one = jnp.where(row < col, m, jnp.where(row > col, turned_m, diags[i : i + 1, :]))
            left[d, 2 * i] = one.astype(BF16)
            left[d, 2 * i + 1] = jnp.where(row < col, turned_m, m).astype(BF16)

    w_own = phys_ref[...].astype(F32)
    row_u = lax.broadcasted_iota(jnp.int32, (PAIRS, PAIRS * PAIRS), 0)
    col_qu = lax.broadcasted_iota(jnp.int32, (PAIRS, PAIRS * PAIRS), 1)
    flat = jnp.zeros((TERMS, PAIRS * PAIRS), F32)
    for q in range(PAIRS):
        put = jnp.where(col_qu == row_u + q * PAIRS, 1.0, 0.0).astype(BF16)
        flat += jnp.dot(w_own[:, q, :].astype(BF16), put, preferred_element_type=F32)
    dense[...] = flat.astype(BF16)
    barrier = pltpu.get_barrier_semaphore()
    for e in range(1, DEVS):
        pl.semaphore_signal(barrier, inc=1, device_id=(peers[e],), device_id_type=MESH)
    pl.semaphore_wait(barrier, DEVS - 1)

    for e in (1, 2, 4, 3, 5, 6, 7):
        r_copy(e).start()
        w_copy(e).start()
    for e, x in ((1, 0), (1, 1), (2, 0), (4, 1), (2, 1), (4, 0)):
        l_copy(e, x).start()
    own = pl.ds(pl.multiple_of(me * ROWS, ROWS), ROWS)
    right[0] = right_ref[:, own, :]
    phys[0] = dense[...]
    left[0] = left_ref[...]
    v_prev[...] = jnp.zeros_like(v_prev)
    beta_old[...] = jnp.zeros_like(beta_old)
    numbers[...] = jnp.zeros_like(numbers)

    def prepare(r):
        psi_copies[r].wait()
        squares[...] = jnp.zeros((BOND, BOND), F32)

        @pl.loop(0, 4)
        def _(s):
            for t in range(4):
                x = psi_ref[r, :, s, t, :]
                squares[...] += x * x
                across[s * 4 + t] = x.T

        norm = jnp.sqrt(total(squares[...]) / N_ELEMS)

        @pl.loop(0, PAIRS)
        def _(u):
            v_in[r, :, u] = (across[u] / norm).astype(BF16).reshape(DEVS, ROWS, BOND)
            two = across[u, own, :] / norm
            row = pl.multiple_of(u * 8, 8)
            v_cur[r, pl.ds(row, 8), :] = two[0:8]
            v_cur[r, pl.ds(row + BOND, 8), :] = two[8:16]

        out_ref[r, 0] = psi_ref[r, own] / norm.reshape(1, 1, 1, 1)

    prepare(0)

    sub = lax.broadcasted_iota(jnp.int32, (8, BOND), 0)
    lane = lax.broadcasted_iota(jnp.int32, (8, BOND), 1)
    eye = jnp.where(lax.rem(lane, 8) == sub, 1.0, 0.0).astype(F32)
    pick_row = lax.broadcasted_iota(jnp.int32, (PAIRS * PAIRS, BOND), 0)
    pick_col = lax.broadcasted_iota(jnp.int32, (PAIRS * PAIRS, BOND), 1) // 8

    def widen(d):
        w_d = phys[d]
        spread = []
        for q in range(PAIRS):
            pick = jnp.where(pick_row == pick_col + q * PAIRS, 1.0, 0.0).astype(BF16)
            spread.append(jnp.dot(w_d, pick, preferred_element_type=F32))
        for k in range(TERMS):
            for q in range(0, PAIRS, 2):
                two = [jnp.broadcast_to(spread[q + i][k : k + 1, :], (8, BOND)) * eye for i in range(2)]
                wide[d, k, q * 8 : q * 8 + 16, :] = jnp.concatenate(two, axis=0).astype(BF16)

    def form_y(r, d, pairs):
        r_d = right[d].reshape(TERMS * ROWS, BOND)
        for u in pairs:
            v_u = jnp.concatenate([v_in[r, :, u + i].reshape(BOND, BOND) for i in range(2)], axis=1)
            y = jnp.dot(r_d, v_u, preferred_element_type=F32).reshape(TERMS, 2, 8, 2 * BOND)
            y = jnp.concatenate([y[..., :BOND], y[..., BOND:]], axis=2)
            y_buf[d, :, :, u * 8 : u * 8 + 16, :] = y.astype(BF16)

    def form_out(d, z_buf, first):
        for k in range(TERMS):
            y_k = jnp.concatenate([y_buf[d, k, 0], y_buf[d, k, 1]], axis=1)
            z = jnp.dot(wide[d, k], y_k, preferred_element_type=F32).astype(BF16)
            for h in range(2):
                z_buf[h * BOND : (h + 1) * BOND, k * BOND : (k + 1) * BOND] = z[:, h * BOND : (h + 1) * BOND]
        part = jnp.dot(z_buf[...], left[d].reshape(TERMS * BOND, BOND), preferred_element_type=F32)
        if first:
            acc[...] = part
        else:
            acc[...] += part

    def share(r):
        s, v, vp = acc[...], v_cur[r], v_prev[r]
        d_p, n_p = total(s * v), total(v * v)
        guess = jnp.where(n_p > 0.0, d_p / jnp.where(n_p > 0.0, n_p, 1.0), 0.0)
        s = s - guess * v - beta_old[r, 0:1, :] * vp
        sig[r] = s
        rows = [d_p, n_p, guess, total(s * s), total(s * v)]
        tile = jnp.zeros((8, BOND), F32)
        for i, row in enumerate(rows):
            tile = jnp.where(sub == i, row, tile)
        mine[r] = tile
        stats[r, me] = tile
        for e in (6, 7, 2, 3, 4, 5, 1):
            s_copy(r, e).start()

    def scalars(r, j):
        for e in range(1, DEVS):
            s_copy(r, e).wait()
        alpha = jnp.zeros((1, BOND), F32)
        for p in range(DEVS):
            alpha = alpha + stats[r, p, 0:1, :]
        alpha = alpha / N_ELEMS
        square = jnp.zeros((1, BOND), F32)
        for p in range(DEVS):
            d_p = alpha - stats[r, p, 2:3, :]
            square = square + (stats[r, p, 3:4, :] - 2.0 * d_p * stats[r, p, 4:5, :] + d_p * d_p * stats[r, p, 1:2, :])
        beta = jnp.sqrt(jnp.maximum(square, 0.0) / N_ELEMS)
        here = jnp.logical_and(sub == r, lane == j)
        numbers[0] = jnp.where(here, alpha, numbers[0])
        numbers[1] = jnp.where(here, beta, numbers[1])
        return alpha, beta

    def turn(r, joined):
        for g in range(2):
            turned[r, g] = joined[g * 8 : (g + 1) * 8].reshape(BOND, BOND).T

    def advance(r, j, last):
        alpha, beta = scalars(r, j)
        shift = alpha - mine[r, 2:3, :]
        v = v_cur[r]
        nxt = (sig[r] - shift * v) / beta
        v_prev[r] = v
        v_cur[r] = nxt
        beta_old[r] = jnp.broadcast_to(beta, (8, BOND))
        halves = nxt.reshape(2, PAIRS, 8, BOND)
        joined = jnp.concatenate([halves[0], halves[1]], axis=1)

        @pl.when(jnp.logical_not(last))
        def _():
            v_in[r, me] = joined.astype(BF16)
            for g in range(2):
                for e in (6, 4, 2, 1):
                    g_copy(r, g, e).start()

        turn(r, joined)

    def post(r, j):
        for e in (6, 7, 2, 3, 4, 5, 1):
            o_copy(r, j, e).start()
        got[r, lax.rem(j, 2), me] = turned[r, :, own, :]

    def relay(r, g):
        for e in (4, 6, 2):
            g_copy(r, g, e).wait()
            g_pass(r, g, e).start()

    def arrive(r, g):
        g_copy(r, g, 1).wait()
        for e in (4, 6, 2):
            g_pass(r, g, e).wait()

    def assemble(read):
        chunk_of = lax.broadcasted_iota(jnp.int32, (ROWS, BOND), 1) // 16
        pairs = []
        for g in range(2):
            x = [read(p, g) for p in range(DEVS)]
            for bit in (1, 2, 4):
                odd = lax.rem(chunk_of // bit, 2) == 1
                for p in range(DEVS):
                    if p & bit:
                        continue
                    low, high = x[p], x[p + bit]
                    x[p] = jnp.where(odd, pltpu.roll(high, 16 * bit, 1), low)
                    x[p + bit] = jnp.where(odd, high, pltpu.roll(low, BOND - 16 * bit, 1))
            pairs += x
        return pairs

    def collect(r, j):
        for e in range(1, DEVS):
            o_copy(r, j, e).wait()
        for q, x in enumerate(assemble(lambda p, g: got[r, lax.rem(j, 2), p, g])):
            out_ref[r, j + 1, :, q // 4, q % 4, :] = x

    acc[...] = jnp.zeros_like(acc)

    @pl.loop(0, DEVS)
    def _(d):
        for e in range(1, DEVS):

            @pl.when(d == e)
            def _():
                r_copy(e).wait()
                w_copy(e).wait()

        widen(d)
        form_y(0, d, range(0, PAIRS, 2))

    @pl.loop(0, DEVS)
    def _(d):
        @pl.when(d == 1)
        def _():
            l_copy(1, 0).wait()
            l_copy(1, 1).wait()

        @pl.when(d == 2)
        def _():
            prepare(1)
            for e, x in ((2, 0), (4, 1)):
                l_copy(e, x).wait()
                l_far(x).start()
                l_pass(e, x).start()
            for e, x in ((2, 1), (4, 0)):
                l_copy(e, x).wait()
                l_pass(e, x).start()

        @pl.when(d == 6)
        def _():
            for x in range(2):
                l_far(x).wait()
                l_pass(6, x).start()

        for e in (3, 5, 7):

            @pl.when(d == e)
            def _():
                for x in range(2):
                    l_pass(e - 1, x).wait()

        @pl.when(d >= 1)
        def _():
            unpack(d)

        form_out(d, z_buf0, False)

    share(0)

    @pl.loop(1, 2 * STEPS)
    def _(t):
        r, j = lax.rem(t, 2), t // 2
        pr, pj = 1 - r, (t - 1) // 2

        for g in range(2):

            @pl.when(t >= 2)
            def _():
                arrive(r, g)

            for u in range(g * 8, (g + 1) * 8, 2):
                for d in range(DEVS):
                    form_y(r, d, (u,))

        for d in range(DEVS):
            if d == FORM_BEFORE:
                advance(pr, pj, t == 2 * STEPS - 1)
            if d == POST_BEFORE:
                post(pr, pj)
            form_out(d, (z_buf0, z_buf1)[d % 2], d == 0)

        share(r)

        @pl.when(t < 2 * STEPS - 1)
        def _():
            relay(pr, 0)

        @pl.when(t >= 2)
        def _():
            collect(r, j - 1)

        @pl.when(t < 2 * STEPS - 1)
        def _():
            relay(pr, 1)

    halves = sig[1].reshape(2, PAIRS, 8, BOND)
    turn(1, jnp.concatenate([halves[0], halves[1]], axis=1))
    for e in (6, 7, 2, 3, 4, 5, 1):
        e_copy(e).start()
    got_end[me] = turned[1, :, own, :]
    collect(0, STEPS - 1)
    done = [(slice(0, 1), slice(0, STEPS + 1)), (slice(1, 2), slice(0, STEPS)), (slice(1, 2), slice(STEPS, STEPS + 1))]
    writes = [pltpu.make_async_copy(out_ref.at[x, y], out_hbm.at[x, y], out_sem.at[i]) for i, (x, y) in enumerate(done)]
    writes[0].start()
    writes[1].start()
    alpha, beta = scalars(1, STEPS - 1)
    shift = jnp.zeros((1, BOND), F32)
    for p in range(DEVS):
        shift = jnp.where(lane[0:1] // 16 == p, alpha - stats[1, p, 2:3, :], shift)
    for e in range(1, DEVS):
        e_copy(e).wait()
    for q, x in enumerate(assemble(lambda p, g: got_end[p, g])):
        v = out_ref[1, STEPS - 1, :, q // 4, q % 4, :]
        out_ref[1, STEPS, :, q // 4, q % 4, :] = (x - shift * v) / beta
    writes[2].start()
    for write in writes:
        write.wait()
    alpha_ref[...] = numbers[0, 0:2, 0:STEPS]
    beta_ref[...] = numbers[1, 0:2, 0:STEPS]


def solution(mesh):
    def device_fn(psi, left_loc, phys_loc, right_loc):
        roots = psi.shape[0]
        vm = pl.BlockSpec(memory_space=pltpu.VMEM)
        dma = pltpu.SemaphoreType.DMA
        return pl.pallas_call(
            kernel,
            out_shape=(
                jax.ShapeDtypeStruct((roots, STEPS + 1, ROWS) + psi.shape[2:], F32),
                jax.ShapeDtypeStruct((roots, STEPS), F32),
                jax.ShapeDtypeStruct((roots, STEPS), F32),
            ),
            in_specs=[pl.BlockSpec(memory_space=pl.ANY), vm, vm, vm],
            out_specs=(pl.BlockSpec(memory_space=pl.ANY), vm, vm),
            scratch_shapes=[
                pltpu.VMEM((DEVS, TERMS, BOND, BOND), BF16),
                pltpu.VMEM((DEVS, TERMS, ROWS, BOND), BF16),
                pltpu.VMEM((DEVS, TERMS, PAIRS * PAIRS), BF16),
                pltpu.VMEM((DEVS, TERMS, BOND, BOND), BF16),
                pltpu.VMEM((roots, DEVS, PAIRS, ROWS, BOND), BF16),
                pltpu.VMEM((DEVS, TERMS, 2, BOND, BOND), BF16),
                pltpu.VMEM((2 * BOND, TERMS * BOND), BF16),
                pltpu.VMEM((2 * BOND, TERMS * BOND), BF16),
                pltpu.VMEM((2 * BOND, BOND), F32),
                pltpu.VMEM((roots, 2 * BOND, BOND), F32),
                pltpu.VMEM((roots, 2 * BOND, BOND), F32),
                pltpu.VMEM((roots, 2 * BOND, BOND), F32),
                pltpu.VMEM((roots, 8, BOND), F32),
                pltpu.VMEM((roots, DEVS, 8, BOND), F32),
                pltpu.VMEM((roots, 8, BOND), F32),
                pltpu.VMEM((roots, 2, BOND, BOND), F32),
                pltpu.VMEM((roots, 2, DEVS, 2, ROWS, BOND), F32),
                pltpu.VMEM((DEVS, 2, ROWS, BOND), F32),
                pltpu.VMEM((PAIRS, BOND, BOND), F32),
                pltpu.VMEM((2, 8, BOND), F32),
                pltpu.VMEM((TERMS, PAIRS * PAIRS), BF16),
                pltpu.VMEM(psi.shape, F32),
                dma((roots,)),
                pltpu.VMEM((DEVS, PACKED, BOND), BF16),
                pltpu.VMEM((BOND, BOND), F32),
                pltpu.VMEM((roots, STEPS + 1, ROWS) + psi.shape[2:], F32),
                dma((3,)),
                dma((DEVS,)), dma((DEVS,)), dma((DEVS,)), dma((DEVS,)), dma((DEVS, 2)), dma((DEVS, 2)),
                dma((roots, DEVS)), dma((roots, DEVS)), dma((roots, 2, DEVS)), dma((roots, 2, DEVS)),
                dma((roots, 2, DEVS)), dma((roots, 2, DEVS)), dma((DEVS,)), dma((DEVS,)),
            ],
            compiler_params=pltpu.CompilerParams(
                collective_id=0, has_side_effects=True, vmem_limit_bytes=56 * 1024 * 1024
            ),
        )(psi, left_loc, right_loc, phys_loc)

    return jax.shard_map(
        device_fn, mesh=mesh, in_specs=(P(), P("terms"), P("terms"), P("terms")),
        out_specs=(P(None, None, "terms"), P(), P()), check_vma=False,
    )
```

```python
import functools

import jax
import jax.numpy as jnp
from jax import lax
from jax.experimental import pallas as pl
from jax.experimental.pallas import tpu as pltpu
from jax.sharding import PartitionSpec as P

STEPS = 6
DEVS = 8
TERMS = 16
PAIRS = 16
BOND = 128
PACKED = TERMS // 2 * BOND + 16
ROWS = 16
N_ELEMS = float(BOND * PAIRS * BOND)
FORM_BEFORE = 0
MESH = pl.DeviceIdType.MESH
F32 = jnp.float32
BF16 = jnp.bfloat16


def flip(dev, bits):
    out = dev
    if bits & 1:
        out = out + 1 - 2 * lax.rem(dev, 2)
    if bits & 2:
        out = out + 2 - 4 * lax.rem(dev // 2, 2)
    if bits & 4:
        out = out + 4 - 8 * lax.rem(dev // 4, 2)
    return out


def total(x):
    return jnp.sum(jnp.sum(x, axis=0, keepdims=True), axis=1, keepdims=True)


def kernel(
    psi_hbm, left_hbm, right_hbm, phys_hbm, out_hbm, alpha_ref, beta_ref,
    left, right, phys, wide, v_in, y_buf, z_buf0, z_buf1, acc, sig, v_cur, v_prev, beta_old, stats, mine,
    turned, got, got_end, across, numbers, dense, psi_ref, psi_sem, tri, squares, out_ref, out_sem,
    left_ref, right_ref, phys_ref, in_sem,
    r_send, r_recv, w_send, w_recv, l_send, l_recv, s_send, s_recv, g_send, g_recv, o_send, o_recv, e_send, e_recv,
):
    me = lax.axis_index("terms")
    peers = {e: flip(me, e) for e in range(1, DEVS)}

    pairs = ((right_hbm, right_ref), (phys_hbm, phys_ref), (left_hbm, left_ref))
    in_copies = [pltpu.make_async_copy(src, dst, in_sem.at[i]) for i, (src, dst) in enumerate(pairs)]
    psi_copies = [pltpu.make_async_copy(psi_hbm.at[r], psi_ref.at[r], psi_sem.at[r]) for r in range(2)]
    for in_copy in in_copies + psi_copies:
        in_copy.start()
    barrier = pltpu.get_barrier_semaphore()
    for e in range(1, DEVS):
        pl.semaphore_signal(barrier, inc=1, device_id=(peers[e],), device_id_type=MESH)
    for in_copy in in_copies:
        in_copy.wait()

    def copy(src, dst, send, recv, e):
        return pltpu.make_async_remote_copy(
            src_ref=src, dst_ref=dst, send_sem=send, recv_sem=recv, device_id=(peers[e],), device_id_type=MESH
        )

    def r_copy(e):
        rows = pl.ds(pl.multiple_of(peers[e] * ROWS, ROWS), ROWS)
        return copy(right_ref.at[:, rows, :], right.at[e], r_send.at[e], r_recv.at[e], e)

    def w_copy(e):
        return copy(dense, phys.at[e], w_send.at[e], w_recv.at[e], e)

    def part(x):
        return slice(0, 512) if x == 0 else slice(512, PACKED)

    def l_copy(e, x):
        return copy(tri.at[0, part(x)], tri.at[e, part(x)], l_send.at[e, x], l_recv.at[e, x], e)

    def l_far(x):
        e = (2, 4)[x]
        return copy(tri.at[e, part(x)], tri.at[6, part(x)], l_send.at[6, x], l_recv.at[6, x], 6 - e)

    def l_pass(e, x):
        return copy(tri.at[e, part(x)], tri.at[e + 1, part(x)], l_send.at[e + 1, x], l_recv.at[e + 1, x], 1)

    def s_copy(r, e):
        return copy(mine.at[r], stats.at[r, me], s_send.at[r, e], s_recv.at[r, e], e)

    def g_copy(r, g, e):
        slot = v_in.at[r, me, g * 8 : (g + 1) * 8]
        return copy(slot, slot, g_send.at[r, g, e], g_recv.at[r, g, e], e)

    def g_pass(r, g, e):
        slot = v_in.at[r, peers[e], g * 8 : (g + 1) * 8]
        return copy(slot, slot, g_send.at[r, g, e + 1], g_recv.at[r, g, e + 1], 1)

    def o_copy(r, j, e):
        rows = pl.ds(pl.multiple_of(peers[e] * ROWS, ROWS), ROWS)
        way = lax.rem(j, 2)
        return copy(turned.at[r, :, rows, :], got.at[r, way, me], o_send.at[r, way, e], o_recv.at[r, way, e], e)

    def e_copy(e):
        rows = pl.ds(pl.multiple_of(peers[e] * ROWS, ROWS), ROWS)
        return copy(turned.at[1, :, rows, :], got_end.at[me], e_send.at[e], e_recv.at[e], e)

    row = lax.broadcasted_iota(jnp.int32, (BOND, BOND), 0)
    col = lax.broadcasted_iota(jnp.int32, (BOND, BOND), 1)
    diag_row = lax.broadcasted_iota(jnp.int32, (16, BOND), 0)
    diags = jnp.zeros((16, BOND), F32)
    for i in range(TERMS // 2):
        one, two = left_ref[2 * i].astype(F32), left_ref[2 * i + 1].astype(F32)
        tri[0, i * BOND : (i + 1) * BOND, :] = jnp.where(row < col, one, two).astype(BF16)
        diag = jnp.sum(jnp.where(row == col, one, 0.0), axis=0, keepdims=True)
        diags = jnp.where(diag_row == i, diag, diags)
    tri[0, PACKED - 16 : PACKED, :] = diags.astype(BF16)

    def unpack(d):
        diags = tri[d, PACKED - 16 : PACKED, :].astype(F32)
        for i in range(TERMS // 2):
            m = tri[d, i * BOND : (i + 1) * BOND, :].astype(F32)
            turned_m = m.T
            one = jnp.where(row < col, m, jnp.where(row > col, turned_m, diags[i : i + 1, :]))
            left[d, 2 * i] = one.astype(BF16)
            left[d, 2 * i + 1] = jnp.where(row < col, turned_m, m).astype(BF16)

    w_own = phys_ref[...].astype(F32)
    row_u = lax.broadcasted_iota(jnp.int32, (PAIRS, PAIRS * PAIRS), 0)
    col_qu = lax.broadcasted_iota(jnp.int32, (PAIRS, PAIRS * PAIRS), 1)
    flat = jnp.zeros((TERMS, PAIRS * PAIRS), F32)
    for q in range(PAIRS):
        put = jnp.where(col_qu == row_u + q * PAIRS, 1.0, 0.0).astype(BF16)
        flat += jnp.dot(w_own[:, q, :].astype(BF16), put, preferred_element_type=F32)
    dense[...] = flat.astype(BF16)
    pl.semaphore_wait(barrier, DEVS - 1)

    for e in (1, 2, 4, 3, 5, 6, 7):
        r_copy(e).start()
        w_copy(e).start()
    for e, x in ((1, 0), (1, 1), (2, 0), (4, 1), (2, 1), (4, 0)):
        l_copy(e, x).start()
    own = pl.ds(pl.multiple_of(me * ROWS, ROWS), ROWS)
    right[0] = right_ref[:, own, :]
    phys[0] = dense[...]
    left[0] = left_ref[...]
    v_prev[...] = jnp.zeros_like(v_prev)
    beta_old[...] = jnp.zeros_like(beta_old)
    numbers[...] = jnp.zeros_like(numbers)

    def prepare(r):
        psi_copies[r].wait()
        squares[...] = jnp.zeros((BOND, BOND), F32)

        @pl.loop(0, 4)
        def _(s):
            for t in range(4):
                x = psi_ref[r, :, s, t, :]
                squares[...] += x * x
                across[s * 4 + t] = x.T

        norm = jnp.sqrt(total(squares[...]) / N_ELEMS)

        @pl.loop(0, PAIRS)
        def _(u):
            v_in[r, :, u] = (across[u] / norm).astype(BF16).reshape(DEVS, ROWS, BOND)
            two = across[u, own, :] / norm
            row = pl.multiple_of(u * 8, 8)
            v_cur[r, pl.ds(row, 8), :] = two[0:8]
            v_cur[r, pl.ds(row + BOND, 8), :] = two[8:16]

        out_ref[r, 0] = psi_ref[r, own] / norm.reshape(1, 1, 1, 1)

    prepare(0)

    sub = lax.broadcasted_iota(jnp.int32, (8, BOND), 0)
    lane = lax.broadcasted_iota(jnp.int32, (8, BOND), 1)
    eye = jnp.where(lax.rem(lane, 8) == sub, 1.0, 0.0).astype(F32)
    pick_row = lax.broadcasted_iota(jnp.int32, (PAIRS * PAIRS, BOND), 0)
    pick_col = lax.broadcasted_iota(jnp.int32, (PAIRS * PAIRS, BOND), 1) // 8

    def widen(d):
        w_d = phys[d]
        spread = []
        for q in range(PAIRS):
            pick = jnp.where(pick_row == pick_col + q * PAIRS, 1.0, 0.0).astype(BF16)
            spread.append(jnp.dot(w_d, pick, preferred_element_type=F32))
        for k in range(TERMS):
            for q in range(0, PAIRS, 2):
                two = [jnp.broadcast_to(spread[q + i][k : k + 1, :], (8, BOND)) * eye for i in range(2)]
                wide[d, k, q * 8 : q * 8 + 16, :] = jnp.concatenate(two, axis=0).astype(BF16)

    def form_y(r, d, pairs):
        r_d = right[d].reshape(TERMS * ROWS, BOND)
        for u in pairs:
            v_u = jnp.concatenate([v_in[r, :, u + i].reshape(BOND, BOND) for i in range(2)], axis=1)
            y = jnp.dot(r_d, v_u, preferred_element_type=F32).reshape(TERMS, 2, 8, 2 * BOND)
            y = jnp.concatenate([y[..., :BOND], y[..., BOND:]], axis=2)
            y_buf[d, :, :, u * 8 : u * 8 + 16, :] = y.astype(BF16)

    def form_out(d, z_buf, first):
        for k in range(TERMS):
            y_k = jnp.concatenate([y_buf[d, k, 0], y_buf[d, k, 1]], axis=1)
            z = jnp.dot(wide[d, k], y_k, preferred_element_type=F32).astype(BF16)
            for h in range(2):
                z_buf[h * BOND : (h + 1) * BOND, k * BOND : (k + 1) * BOND] = z[:, h * BOND : (h + 1) * BOND]
        part = jnp.dot(z_buf[...], left[d].reshape(TERMS * BOND, BOND), preferred_element_type=F32)
        if first:
            acc[...] = part
        else:
            acc[...] += part

    def share(r):
        s, v, vp = acc[...], v_cur[r], v_prev[r]
        d_p, n_p = total(s * v), total(v * v)
        guess = jnp.where(n_p > 0.0, d_p / jnp.where(n_p > 0.0, n_p, 1.0), 0.0)
        s = s - guess * v - beta_old[r, 0:1, :] * vp
        sig[r] = s
        rows = [d_p, n_p, guess, total(s * s), total(s * v)]
        tile = jnp.zeros((8, BOND), F32)
        for i, row in enumerate(rows):
            tile = jnp.where(sub == i, row, tile)
        mine[r] = tile
        stats[r, me] = tile
        for e in (6, 7, 2, 3, 4, 5, 1):
            s_copy(r, e).start()

    def scalars(r, j):
        for e in range(1, DEVS):
            s_copy(r, e).wait()
        alpha = jnp.zeros((1, BOND), F32)
        for p in range(DEVS):
            alpha = alpha + stats[r, p, 0:1, :]
        alpha = alpha / N_ELEMS
        square = jnp.zeros((1, BOND), F32)
        for p in range(DEVS):
            d_p = alpha - stats[r, p, 2:3, :]
            square = square + (stats[r, p, 3:4, :] - 2.0 * d_p * stats[r, p, 4:5, :] + d_p * d_p * stats[r, p, 1:2, :])
        beta = jnp.sqrt(jnp.maximum(square, 0.0) / N_ELEMS)
        here = jnp.logical_and(sub == r, lane == j)
        numbers[0] = jnp.where(here, alpha, numbers[0])
        numbers[1] = jnp.where(here, beta, numbers[1])
        return alpha, beta

    def turn(r, joined):
        for g in range(2):
            turned[r, g] = joined[g * 8 : (g + 1) * 8].reshape(BOND, BOND).T

    def advance(r, j, last):
        alpha, beta = scalars(r, j)
        shift = alpha - mine[r, 2:3, :]
        v = v_cur[r]
        nxt = (sig[r] - shift * v) / beta
        v_prev[r] = v
        v_cur[r] = nxt
        beta_old[r] = jnp.broadcast_to(beta, (8, BOND))
        halves = nxt.reshape(2, PAIRS, 8, BOND)
        joined = jnp.concatenate([halves[0], halves[1]], axis=1)

        @pl.when(jnp.logical_not(last))
        def _():
            v_in[r, me] = joined.astype(BF16)
            for g in range(2):
                for e in (6, 4, 2, 1):
                    g_copy(r, g, e).start()


    def post(r, j):
        halves = v_cur[r].reshape(2, PAIRS, 8, BOND)
        turn(r, jnp.concatenate([halves[0], halves[1]], axis=1))
        for e in (6, 7, 2, 3, 4, 5, 1):
            o_copy(r, j, e).start()
        got[r, lax.rem(j, 2), me] = turned[r, :, own, :]

    def relay(r, g):
        for e in (4, 6, 2):
            g_copy(r, g, e).wait()
            g_pass(r, g, e).start()

    def arrive(r, g):
        g_copy(r, g, 1).wait()
        for e in (4, 6, 2):
            g_pass(r, g, e).wait()

    def assemble(read):
        chunk_of = lax.broadcasted_iota(jnp.int32, (ROWS, BOND), 1) // 16
        pairs = []
        for g in range(2):
            x = [read(p, g) for p in range(DEVS)]
            for bit in (1, 2, 4):
                odd = lax.rem(chunk_of // bit, 2) == 1
                for p in range(DEVS):
                    if p & bit:
                        continue
                    low, high = x[p], x[p + bit]
                    x[p] = jnp.where(odd, pltpu.roll(high, 16 * bit, 1), low)
                    x[p + bit] = jnp.where(odd, high, pltpu.roll(low, BOND - 16 * bit, 1))
            pairs += x
        return pairs

    def collect(r, j):
        for e in range(1, DEVS):
            o_copy(r, j, e).wait()
        for q, x in enumerate(assemble(lambda p, g: got[r, lax.rem(j, 2), p, g])):
            out_ref[r, j + 1, :, q // 4, q % 4, :] = x

    acc[...] = jnp.zeros_like(acc)

    @pl.loop(0, DEVS)
    def _(d):
        for e in range(1, DEVS):

            @pl.when(d == e)
            def _():
                r_copy(e).wait()
                w_copy(e).wait()

        widen(d)
        form_y(0, d, range(0, PAIRS, 2))

    @pl.loop(0, DEVS)
    def _(d):
        @pl.when(d == 1)
        def _():
            l_copy(1, 0).wait()
            l_copy(1, 1).wait()

        @pl.when(d == 2)
        def _():
            for e, x in ((2, 0), (4, 1)):
                l_copy(e, x).wait()
                l_far(x).start()
                l_pass(e, x).start()
            prepare(1)
            for e, x in ((2, 1), (4, 0)):
                l_copy(e, x).wait()
                l_pass(e, x).start()

        @pl.when(d == 6)
        def _():
            for x in range(2):
                l_far(x).wait()
                l_pass(6, x).start()

        for e in (3, 5, 7):

            @pl.when(d == e)
            def _():
                for x in range(2):
                    l_pass(e - 1, x).wait()

        @pl.when(d >= 1)
        def _():
            unpack(d)

        form_out(d, z_buf0, False)

    share(0)

    @pl.loop(1, 2 * STEPS)
    def _(t):
        r, j = lax.rem(t, 2), t // 2
        pr, pj = 1 - r, (t - 1) // 2

        for g in range(2):

            @pl.when(t >= 2)
            def _():
                arrive(r, g)

            for u in range(g * 8, (g + 1) * 8, 2):
                for d in range(DEVS):
                    form_y(r, d, (u,))

        for d in range(DEVS):
            if d == FORM_BEFORE:
                advance(pr, pj, t == 2 * STEPS - 1)

                @pl.when(t == 2 * STEPS - 1)
                def _():
                    post(pr, pj)

            form_out(d, (z_buf0, z_buf1)[d % 2], d == 0)

        share(r)

        @pl.when(t < 2 * STEPS - 1)
        def _():
            relay(pr, 0)
            post(pr, pj)

        @pl.when(t >= 2)
        def _():
            collect(r, j - 1)

        @pl.when(t < 2 * STEPS - 1)
        def _():
            relay(pr, 1)

    halves = sig[1].reshape(2, PAIRS, 8, BOND)
    turn(1, jnp.concatenate([halves[0], halves[1]], axis=1))
    for e in (6, 7, 2, 3, 4, 5, 1):
        e_copy(e).start()
    got_end[me] = turned[1, :, own, :]
    collect(0, STEPS - 1)
    done = [(slice(0, 1), slice(0, STEPS + 1)), (slice(1, 2), slice(0, STEPS)), (slice(1, 2), slice(STEPS, STEPS + 1))]
    writes = [pltpu.make_async_copy(out_ref.at[x, y], out_hbm.at[x, y], out_sem.at[i]) for i, (x, y) in enumerate(done)]
    writes[0].start()
    writes[1].start()
    alpha, beta = scalars(1, STEPS - 1)
    shift = jnp.zeros((1, BOND), F32)
    for p in range(DEVS):
        shift = jnp.where(lane[0:1] // 16 == p, alpha - stats[1, p, 2:3, :], shift)
    for e in range(1, DEVS):
        e_copy(e).wait()
    for q, x in enumerate(assemble(lambda p, g: got_end[p, g])):
        v = out_ref[1, STEPS - 1, :, q // 4, q % 4, :]
        out_ref[1, STEPS, :, q // 4, q % 4, :] = (x - shift * v) / beta
    writes[2].start()
    for write in writes:
        write.wait()
    alpha_ref[...] = numbers[0, 0:2, 0:STEPS]
    beta_ref[...] = numbers[1, 0:2, 0:STEPS]


def solution(mesh):
    def device_fn(psi, left_loc, phys_loc, right_loc):
        roots = psi.shape[0]
        vm = pl.BlockSpec(memory_space=pltpu.VMEM)
        dma = pltpu.SemaphoreType.DMA
        return pl.pallas_call(
            kernel,
            out_shape=(
                jax.ShapeDtypeStruct((roots, STEPS + 1, ROWS) + psi.shape[2:], F32),
                jax.ShapeDtypeStruct((roots, STEPS), F32),
                jax.ShapeDtypeStruct((roots, STEPS), F32),
            ),
            in_specs=[pl.BlockSpec(memory_space=pl.ANY)] * 4,
            out_specs=(pl.BlockSpec(memory_space=pl.ANY), vm, vm),
            scratch_shapes=[
                pltpu.VMEM((DEVS, TERMS, BOND, BOND), BF16),
                pltpu.VMEM((DEVS, TERMS, ROWS, BOND), BF16),
                pltpu.VMEM((DEVS, TERMS, PAIRS * PAIRS), BF16),
                pltpu.VMEM((DEVS, TERMS, BOND, BOND), BF16),
                pltpu.VMEM((roots, DEVS, PAIRS, ROWS, BOND), BF16),
                pltpu.VMEM((DEVS, TERMS, 2, BOND, BOND), BF16),
                pltpu.VMEM((2 * BOND, TERMS * BOND), BF16),
                pltpu.VMEM((2 * BOND, TERMS * BOND), BF16),
                pltpu.VMEM((2 * BOND, BOND), F32),
                pltpu.VMEM((roots, 2 * BOND, BOND), F32),
                pltpu.VMEM((roots, 2 * BOND, BOND), F32),
                pltpu.VMEM((roots, 2 * BOND, BOND), F32),
                pltpu.VMEM((roots, 8, BOND), F32),
                pltpu.VMEM((roots, DEVS, 8, BOND), F32),
                pltpu.VMEM((roots, 8, BOND), F32),
                pltpu.VMEM((roots, 2, BOND, BOND), F32),
                pltpu.VMEM((roots, 2, DEVS, 2, ROWS, BOND), F32),
                pltpu.VMEM((DEVS, 2, ROWS, BOND), F32),
                pltpu.VMEM((PAIRS, BOND, BOND), F32),
                pltpu.VMEM((2, 8, BOND), F32),
                pltpu.VMEM((TERMS, PAIRS * PAIRS), BF16),
                pltpu.VMEM(psi.shape, F32),
                dma((roots,)),
                pltpu.VMEM((DEVS, PACKED, BOND), BF16),
                pltpu.VMEM((BOND, BOND), F32),
                pltpu.VMEM((roots, STEPS + 1, ROWS) + psi.shape[2:], F32),
                dma((3,)),
                pltpu.VMEM((TERMS, BOND, BOND), BF16),
                pltpu.VMEM((TERMS, BOND, BOND), BF16),
                pltpu.VMEM((TERMS, PAIRS, PAIRS), BF16),
                dma((3,)),
                dma((DEVS,)), dma((DEVS,)), dma((DEVS,)), dma((DEVS,)), dma((DEVS, 2)), dma((DEVS, 2)),
                dma((roots, DEVS)), dma((roots, DEVS)), dma((roots, 2, DEVS)), dma((roots, 2, DEVS)),
                dma((roots, 2, DEVS)), dma((roots, 2, DEVS)), dma((DEVS,)), dma((DEVS,)),
            ],
            compiler_params=pltpu.CompilerParams(
                collective_id=0, has_side_effects=True, vmem_limit_bytes=56 * 1024 * 1024
            ),
        )(psi, left_loc, right_loc, phys_loc)

    return jax.shard_map(
        device_fn, mesh=mesh, in_specs=(P(), P("terms"), P("terms"), P("terms")),
        out_specs=(P(None, None, "terms"), P(), P()), check_vma=False,
    )
```

```python
import functools

import jax
import jax.numpy as jnp
from jax import lax
from jax.experimental import pallas as pl
from jax.experimental.pallas import tpu as pltpu
from jax.sharding import PartitionSpec as P

STEPS = 6
DEVS = 8
TERMS = 16
PAIRS = 16
BOND = 128
PACKED = TERMS // 2 * BOND + 16
ROWS = 16
N_ELEMS = float(BOND * PAIRS * BOND)
FORM_BEFORE = 0
MESH = pl.DeviceIdType.MESH
F32 = jnp.float32
BF16 = jnp.bfloat16


def flip(dev, bits):
    out = dev
    if bits & 1:
        out = out + 1 - 2 * lax.rem(dev, 2)
    if bits & 2:
        out = out + 2 - 4 * lax.rem(dev // 2, 2)
    if bits & 4:
        out = out + 4 - 8 * lax.rem(dev // 4, 2)
    return out


def total(x):
    return jnp.sum(jnp.sum(x, axis=0, keepdims=True), axis=1, keepdims=True)


def kernel(
    psi_hbm, left_hbm, right_hbm, phys_hbm, out_hbm, alpha_hbm, beta_hbm, scale_hbm,
    left, right, phys, wide, v_in, y_buf, z_buf0, z_buf1, acc, sig, v_cur, v_prev, beta_old, stats, mine,
    turned, got, got_end, across, numbers, dense, psi_ref, psi_sem, tri, squares, out_ref, out_sem,
    left_ref, right_ref, phys_ref, in_sem, alpha_ref, beta_ref, scale_ref,
    r_send, r_recv, w_send, w_recv, l_send, l_recv, s_send, s_recv, g_send, g_recv, o_send, o_recv, e_send, e_recv,
):
    me = lax.axis_index("terms")
    peers = {e: flip(me, e) for e in range(1, DEVS)}

    pairs = ((right_hbm, right_ref), (phys_hbm, phys_ref), (left_hbm, left_ref))
    in_copies = [pltpu.make_async_copy(src, dst, in_sem.at[i]) for i, (src, dst) in enumerate(pairs)]
    psi_copies = [pltpu.make_async_copy(psi_hbm.at[r], psi_ref.at[r], psi_sem.at[r]) for r in range(2)]
    for in_copy in in_copies + psi_copies:
        in_copy.start()
    barrier = pltpu.get_barrier_semaphore()
    for e in range(1, DEVS):
        pl.semaphore_signal(barrier, inc=1, device_id=(peers[e],), device_id_type=MESH)
    for in_copy in in_copies:
        in_copy.wait()

    def copy(src, dst, send, recv, e):
        return pltpu.make_async_remote_copy(
            src_ref=src, dst_ref=dst, send_sem=send, recv_sem=recv, device_id=(peers[e],), device_id_type=MESH
        )

    def r_copy(e):
        rows = pl.ds(pl.multiple_of(peers[e] * ROWS, ROWS), ROWS)
        return copy(right_ref.at[:, rows, :], right.at[e], r_send.at[e], r_recv.at[e], e)

    def w_copy(e):
        return copy(dense, phys.at[e], w_send.at[e], w_recv.at[e], e)

    def part(x):
        return slice(0, 512) if x == 0 else slice(512, PACKED)

    def l_copy(e, x):
        return copy(tri.at[0, part(x)], tri.at[e, part(x)], l_send.at[e, x], l_recv.at[e, x], e)

    def l_far(x):
        e = (2, 4)[x]
        return copy(tri.at[e, part(x)], tri.at[6, part(x)], l_send.at[6, x], l_recv.at[6, x], 6 - e)

    def l_pass(e, x):
        return copy(tri.at[e, part(x)], tri.at[e + 1, part(x)], l_send.at[e + 1, x], l_recv.at[e + 1, x], 1)

    def s_copy(r, e):
        return copy(mine.at[r], stats.at[r, me], s_send.at[r, e], s_recv.at[r, e], e)

    def g_copy(r, g, e):
        slot = v_in.at[r, me, g * 8 : (g + 1) * 8]
        return copy(slot, slot, g_send.at[r, g, e], g_recv.at[r, g, e], e)

    def g_pass(r, g, e):
        slot = v_in.at[r, peers[e], g * 8 : (g + 1) * 8]
        return copy(slot, slot, g_send.at[r, g, e + 1], g_recv.at[r, g, e + 1], 1)

    def o_copy(r, j, e):
        rows = pl.ds(pl.multiple_of(peers[e] * ROWS, ROWS), ROWS)
        way = lax.rem(j, 2)
        return copy(turned.at[r, :, rows, :], got.at[r, way, me], o_send.at[r, way, e], o_recv.at[r, way, e], e)

    def e_copy(e):
        rows = pl.ds(pl.multiple_of(peers[e] * ROWS, ROWS), ROWS)
        return copy(turned.at[1, :, rows, :], got_end.at[me], e_send.at[e], e_recv.at[e], e)

    row = lax.broadcasted_iota(jnp.int32, (BOND, BOND), 0)
    col = lax.broadcasted_iota(jnp.int32, (BOND, BOND), 1)
    diag_row = lax.broadcasted_iota(jnp.int32, (16, BOND), 0)
    diags = jnp.zeros((16, BOND), F32)
    for i in range(TERMS // 2):
        one, two = left_ref[2 * i].astype(F32), left_ref[2 * i + 1].astype(F32)
        tri[0, i * BOND : (i + 1) * BOND, :] = jnp.where(row < col, one, two).astype(BF16)
        diag = jnp.sum(jnp.where(row == col, one, 0.0), axis=0, keepdims=True)
        diags = jnp.where(diag_row == i, diag, diags)
    tri[0, PACKED - 16 : PACKED, :] = diags.astype(BF16)

    def unpack(d):
        diags = tri[d, PACKED - 16 : PACKED, :].astype(F32)
        for i in range(TERMS // 2):
            m = tri[d, i * BOND : (i + 1) * BOND, :].astype(F32)
            turned_m = m.T
            one = jnp.where(row < col, m, jnp.where(row > col, turned_m, diags[i : i + 1, :]))
            left[d, 2 * i] = one.astype(BF16)
            left[d, 2 * i + 1] = jnp.where(row < col, turned_m, m).astype(BF16)

    w_own = phys_ref[...].astype(F32)
    row_u = lax.broadcasted_iota(jnp.int32, (PAIRS, PAIRS * PAIRS), 0)
    col_qu = lax.broadcasted_iota(jnp.int32, (PAIRS, PAIRS * PAIRS), 1)
    flat = jnp.zeros((TERMS, PAIRS * PAIRS), F32)
    for q in range(PAIRS):
        put = jnp.where(col_qu == row_u + q * PAIRS, 1.0, 0.0).astype(BF16)
        flat += jnp.dot(w_own[:, q, :].astype(BF16), put, preferred_element_type=F32)
    dense[...] = flat.astype(BF16)
    pl.semaphore_wait(barrier, DEVS - 1)

    for e in (1, 2, 4, 3, 5, 6, 7):
        r_copy(e).start()
        w_copy(e).start()
    for e, x in ((1, 0), (1, 1), (2, 0), (4, 1), (2, 1), (4, 0)):
        l_copy(e, x).start()
    own = pl.ds(pl.multiple_of(me * ROWS, ROWS), ROWS)
    right[0] = right_ref[:, own, :]
    phys[0] = dense[...]
    left[0] = left_ref[...]
    v_prev[...] = jnp.zeros_like(v_prev)
    beta_old[...] = jnp.zeros_like(beta_old)
    numbers[...] = jnp.zeros_like(numbers)

    def prepare(r):
        psi_copies[r].wait()
        squares[...] = jnp.zeros((BOND, BOND), F32)

        @pl.loop(0, 4)
        def _(s):
            for t in range(4):
                x = psi_ref[r, :, s, t, :]
                squares[...] += x * x
                across[s * 4 + t] = x.T

        norm = jnp.sqrt(total(squares[...]) / N_ELEMS)

        @pl.loop(0, PAIRS)
        def _(u):
            v_in[r, :, u] = (across[u] / norm).astype(BF16).reshape(DEVS, ROWS, BOND)
            two = across[u, own, :] / norm
            row = pl.multiple_of(u * 8, 8)
            v_cur[r, pl.ds(row, 8), :] = two[0:8]
            v_cur[r, pl.ds(row + BOND, 8), :] = two[8:16]

        for q in range(PAIRS):
            out_ref[r, 0, :, q, :] = psi_ref[r, own, q // 4, q % 4, :] / norm

    prepare(0)

    sub = lax.broadcasted_iota(jnp.int32, (8, BOND), 0)
    lane = lax.broadcasted_iota(jnp.int32, (8, BOND), 1)
    eye = jnp.where(lax.rem(lane, 8) == sub, 1.0, 0.0).astype(F32)
    pick_row = lax.broadcasted_iota(jnp.int32, (PAIRS * PAIRS, BOND), 0)
    pick_col = lax.broadcasted_iota(jnp.int32, (PAIRS * PAIRS, BOND), 1) // 8

    def widen(d):
        w_d = phys[d]
        spread = []
        for q in range(PAIRS):
            pick = jnp.where(pick_row == pick_col + q * PAIRS, 1.0, 0.0).astype(BF16)
            spread.append(jnp.dot(w_d, pick, preferred_element_type=F32))
        for k in range(TERMS):
            for q in range(0, PAIRS, 2):
                two = [jnp.broadcast_to(spread[q + i][k : k + 1, :], (8, BOND)) * eye for i in range(2)]
                wide[d, k, q * 8 : q * 8 + 16, :] = jnp.concatenate(two, axis=0).astype(BF16)

    def form_y(r, d, pairs):
        r_d = right[d].reshape(TERMS * ROWS, BOND)
        for u in pairs:
            v_u = jnp.concatenate([v_in[r, :, u + i].reshape(BOND, BOND) for i in range(2)], axis=1)
            y = jnp.dot(r_d, v_u, preferred_element_type=F32).reshape(TERMS, 2, 8, 2 * BOND)
            y = jnp.concatenate([y[..., :BOND], y[..., BOND:]], axis=2)
            y_buf[d, :, :, u * 8 : u * 8 + 16, :] = y.astype(BF16)

    def form_out(d, z_buf, first):
        for k in range(TERMS):
            y_k = jnp.concatenate([y_buf[d, k, 0], y_buf[d, k, 1]], axis=1)
            z = jnp.dot(wide[d, k], y_k, preferred_element_type=F32).astype(BF16)
            for h in range(2):
                z_buf[h * BOND : (h + 1) * BOND, k * BOND : (k + 1) * BOND] = z[:, h * BOND : (h + 1) * BOND]
        part = jnp.dot(z_buf[...], left[d].reshape(TERMS * BOND, BOND), preferred_element_type=F32)
        if first:
            acc[...] = part
        else:
            acc[...] += part

    def share(r):
        s, v, vp = acc[...], v_cur[r], v_prev[r]
        d_p, n_p = total(s * v), total(v * v)
        guess = jnp.where(n_p > 0.0, d_p / jnp.where(n_p > 0.0, n_p, 1.0), 0.0)
        s = s - guess * v - beta_old[r, 0:1, :] * vp
        sig[r] = s
        rows = [d_p, n_p, guess, total(s * s), total(s * v)]
        tile = jnp.zeros((8, BOND), F32)
        for i, row in enumerate(rows):
            tile = jnp.where(sub == i, row, tile)
        mine[r] = tile
        stats[r, me] = tile
        for e in (6, 7, 2, 3, 4, 5, 1):
            s_copy(r, e).start()

    def scalars(r, j):
        for e in range(1, DEVS):
            s_copy(r, e).wait()
        alpha = jnp.zeros((1, BOND), F32)
        for p in range(DEVS):
            alpha = alpha + stats[r, p, 0:1, :]
        alpha = alpha / N_ELEMS
        square = jnp.zeros((1, BOND), F32)
        for p in range(DEVS):
            d_p = alpha - stats[r, p, 2:3, :]
            square = square + (stats[r, p, 3:4, :] - 2.0 * d_p * stats[r, p, 4:5, :] + d_p * d_p * stats[r, p, 1:2, :])
        beta = jnp.sqrt(jnp.maximum(square, 0.0) / N_ELEMS)
        here = jnp.logical_and(sub == r, lane == j)
        numbers[0] = jnp.where(here, alpha, numbers[0])
        numbers[1] = jnp.where(here, beta, numbers[1])
        return alpha, beta

    def turn(r, joined):
        for g in range(2):
            turned[r, g] = joined[g * 8 : (g + 1) * 8].reshape(BOND, BOND).T

    def advance(r, j, last):
        alpha, beta = scalars(r, j)
        shift = alpha - mine[r, 2:3, :]
        v = v_cur[r]
        nxt = (sig[r] - shift * v) / beta
        v_prev[r] = v
        v_cur[r] = nxt
        beta_old[r] = jnp.broadcast_to(beta, (8, BOND))
        halves = nxt.reshape(2, PAIRS, 8, BOND)
        joined = jnp.concatenate([halves[0], halves[1]], axis=1)

        @pl.when(jnp.logical_not(last))
        def _():
            v_in[r, me] = joined.astype(BF16)
            for g in range(2):
                for e in (6, 4, 2, 1):
                    g_copy(r, g, e).start()


    def post(r, j):
        halves = v_cur[r].reshape(2, PAIRS, 8, BOND)
        turn(r, jnp.concatenate([halves[0], halves[1]], axis=1))
        for e in (6, 7, 2, 3, 4, 5, 1):
            o_copy(r, j, e).start()
        got[r, lax.rem(j, 2), me] = turned[r, :, own, :]

    def relay(r, g):
        for e in (4, 6, 2):
            g_copy(r, g, e).wait()
            g_pass(r, g, e).start()

    def arrive(r, g):
        g_copy(r, g, 1).wait()
        for e in (4, 6, 2):
            g_pass(r, g, e).wait()

    def assemble(read):
        chunk_of = lax.broadcasted_iota(jnp.int32, (ROWS, BOND), 1) // 16
        pairs = []
        for g in range(2):
            x = [read(p, g) for p in range(DEVS)]
            for bit in (1, 2, 4):
                odd = lax.rem(chunk_of // bit, 2) == 1
                for p in range(DEVS):
                    if p & bit:
                        continue
                    low, high = x[p], x[p + bit]
                    x[p] = jnp.where(odd, pltpu.roll(high, 16 * bit, 1), low)
                    x[p + bit] = jnp.where(odd, high, pltpu.roll(low, BOND - 16 * bit, 1))
            pairs += x
        return pairs

    def collect(r, j):
        for e in range(1, DEVS):
            o_copy(r, j, e).wait()
        for q, x in enumerate(assemble(lambda p, g: got[r, lax.rem(j, 2), p, g])):
            out_ref[r, j + 1, :, q, :] = x


    @pl.loop(0, DEVS)
    def _(d):
        for e in range(1, DEVS):

            @pl.when(d == e)
            def _():
                r_copy(e).wait()
                w_copy(e).wait()

        widen(d)
        form_y(0, d, range(0, PAIRS, 2))

    for d in range(DEVS):
        nxt = d + 1
        if nxt == 1:
            l_copy(1, 0).wait()
            l_copy(1, 1).wait()
        elif nxt == 2:
            for e, x in ((2, 0), (4, 1)):
                l_copy(e, x).wait()
                l_far(x).start()
                l_pass(e, x).start()
            prepare(1)
            for e, x in ((2, 1), (4, 0)):
                l_copy(e, x).wait()
                l_pass(e, x).start()
        elif nxt == 6:
            for x in range(2):
                l_far(x).wait()
                l_pass(6, x).start()
        elif nxt in (3, 5, 7):
            for x in range(2):
                l_pass(nxt - 1, x).wait()
        if nxt < DEVS:
            unpack(nxt)
        form_out(d, (z_buf0, z_buf1)[d % 2], d == 0)

    share(0)

    @pl.loop(1, 2 * STEPS)
    def _(t):
        r, j = lax.rem(t, 2), t // 2
        pr, pj = 1 - r, (t - 1) // 2

        for g in range(2):

            @pl.when(t >= 2)
            def _():
                arrive(r, g)

            for u in range(g * 8, (g + 1) * 8, 2):
                for d in range(DEVS):
                    form_y(r, d, (u,))

        for d in range(DEVS):
            if d == FORM_BEFORE:
                advance(pr, pj, t == 2 * STEPS - 1)

                @pl.when(t == 2 * STEPS - 1)
                def _():
                    post(pr, pj)

            form_out(d, (z_buf0, z_buf1)[d % 2], d == 0)

        share(r)

        @pl.when(t < 2 * STEPS - 1)
        def _():
            relay(pr, 0)
            post(pr, pj)

        @pl.when(t >= 2)
        def _():
            collect(r, j - 1)

        @pl.when(t < 2 * STEPS - 1)
        def _():
            relay(pr, 1)

    halves = sig[1].reshape(2, PAIRS, 8, BOND)
    turn(1, jnp.concatenate([halves[0], halves[1]], axis=1))
    for e in (6, 7, 2, 3, 4, 5, 1):
        e_copy(e).start()
    got_end[me] = turned[1, :, own, :]
    collect(0, STEPS - 1)
    done = [(slice(0, 1), slice(0, STEPS + 1)), (slice(1, 2), slice(0, STEPS)), (slice(1, 2), slice(STEPS, STEPS + 1))]
    writes = [pltpu.make_async_copy(out_ref.at[x, y], out_hbm.at[x, y], out_sem.at[i]) for i, (x, y) in enumerate(done)]
    writes[0].start()
    writes[1].start()
    alpha, beta = scalars(1, STEPS - 1)
    shift = jnp.zeros((1, BOND), F32)
    for p in range(DEVS):
        shift = jnp.where(lane[0:1] // 16 == p, alpha - stats[1, p, 2:3, :], shift)
    for e in range(1, DEVS):
        e_copy(e).wait()
    for q, x in enumerate(assemble(lambda p, g: got_end[p, g])):
        v = out_ref[1, STEPS - 1, :, q, :]
        out_ref[1, STEPS, :, q, :] = x - shift * v
    alpha_ref[...] = numbers[0, 0:2, 0:STEPS]
    beta_ref[...] = numbers[1, 0:2, 0:STEPS]
    end = jnp.logical_and(sub == 1, lane == STEPS)
    scale_ref[...] = jnp.where(end, 1.0 / beta, jnp.ones((8, BOND), F32))[0:2, 0 : STEPS + 1]
    writes.append(pltpu.make_async_copy(scale_ref, scale_hbm, out_sem.at[5]))
    writes.append(pltpu.make_async_copy(alpha_ref, alpha_hbm, out_sem.at[3]))
    writes.append(pltpu.make_async_copy(beta_ref, beta_hbm, out_sem.at[4]))
    for write in writes[2:]:
        write.start()
    for write in writes:
        write.wait()


def solution(mesh):
    def device_fn(psi, left_loc, phys_loc, right_loc):
        roots = psi.shape[0]
        anywhere = pl.BlockSpec(memory_space=pl.ANY)
        dma = pltpu.SemaphoreType.DMA
        vecs, alpha, beta, scale = pl.pallas_call(
            kernel,
            out_shape=(
                jax.ShapeDtypeStruct((roots, STEPS + 1, ROWS, PAIRS, BOND), F32),
                jax.ShapeDtypeStruct((roots, STEPS), F32),
                jax.ShapeDtypeStruct((roots, STEPS), F32),
                jax.ShapeDtypeStruct((roots, STEPS + 1), F32),
            ),
            in_specs=[anywhere] * 4,
            out_specs=[anywhere] * 4,
            scratch_shapes=[
                pltpu.VMEM((DEVS, TERMS, BOND, BOND), BF16),
                pltpu.VMEM((DEVS, TERMS, ROWS, BOND), BF16),
                pltpu.VMEM((DEVS, TERMS, PAIRS * PAIRS), BF16),
                pltpu.VMEM((DEVS, TERMS, BOND, BOND), BF16),
                pltpu.VMEM((roots, DEVS, PAIRS, ROWS, BOND), BF16),
                pltpu.VMEM((DEVS, TERMS, 2, BOND, BOND), BF16),
                pltpu.VMEM((2 * BOND, TERMS * BOND), BF16),
                pltpu.VMEM((2 * BOND, TERMS * BOND), BF16),
                pltpu.VMEM((2 * BOND, BOND), F32),
                pltpu.VMEM((roots, 2 * BOND, BOND), F32),
                pltpu.VMEM((roots, 2 * BOND, BOND), F32),
                pltpu.VMEM((roots, 2 * BOND, BOND), F32),
                pltpu.VMEM((roots, 8, BOND), F32),
                pltpu.VMEM((roots, DEVS, 8, BOND), F32),
                pltpu.VMEM((roots, 8, BOND), F32),
                pltpu.VMEM((roots, 2, BOND, BOND), F32),
                pltpu.VMEM((roots, 2, DEVS, 2, ROWS, BOND), F32),
                pltpu.VMEM((DEVS, 2, ROWS, BOND), F32),
                pltpu.VMEM((PAIRS, BOND, BOND), F32),
                pltpu.VMEM((2, 8, BOND), F32),
                pltpu.VMEM((TERMS, PAIRS * PAIRS), BF16),
                pltpu.VMEM(psi.shape, F32),
                dma((roots,)),
                pltpu.VMEM((DEVS, PACKED, BOND), BF16),
                pltpu.VMEM((BOND, BOND), F32),
                pltpu.VMEM((roots, STEPS + 1, ROWS, PAIRS, BOND), F32),
                dma((6,)),
                pltpu.VMEM((TERMS, BOND, BOND), BF16),
                pltpu.VMEM((TERMS, BOND, BOND), BF16),
                pltpu.VMEM((TERMS, PAIRS, PAIRS), BF16),
                dma((3,)),
                pltpu.VMEM((roots, STEPS), F32),
                pltpu.VMEM((roots, STEPS), F32),
                pltpu.VMEM((roots, STEPS + 1), F32),
                dma((DEVS,)), dma((DEVS,)), dma((DEVS,)), dma((DEVS,)), dma((DEVS, 2)), dma((DEVS, 2)),
                dma((roots, DEVS)), dma((roots, DEVS)), dma((roots, 2, DEVS)), dma((roots, 2, DEVS)),
                dma((roots, 2, DEVS)), dma((roots, 2, DEVS)), dma((DEVS,)), dma((DEVS,)),
            ],
            compiler_params=pltpu.CompilerParams(
                collective_id=0, has_side_effects=True, vmem_limit_bytes=56 * 1024 * 1024
            ),
        )(psi, left_loc, right_loc, phys_loc)
        vecs = vecs * scale[:, :, None, None, None]
        return vecs.reshape(roots, STEPS + 1, ROWS, *psi.shape[2:]), alpha, beta

    return jax.shard_map(
        device_fn, mesh=mesh, in_specs=(P(), P("terms"), P("terms"), P("terms")),
        out_specs=(P(None, None, "terms"), P(), P()), check_vma=False,
    )
```

```python
import functools

import jax
import jax.numpy as jnp
from jax import lax
from jax.experimental import pallas as pl
from jax.experimental.pallas import tpu as pltpu
from jax.sharding import PartitionSpec as P

STEPS = 6
DEVS = 8
TERMS = 16
PAIRS = 16
BOND = 128
PACKED = TERMS // 2 * BOND + 16
ROWS = 16
N_ELEMS = float(BOND * PAIRS * BOND)
FORM_BEFORE = 0
MESH = pl.DeviceIdType.MESH
F32 = jnp.float32
BF16 = jnp.bfloat16


def flip(dev, bits):
    out = dev
    if bits & 1:
        out = out + 1 - 2 * lax.rem(dev, 2)
    if bits & 2:
        out = out + 2 - 4 * lax.rem(dev // 2, 2)
    if bits & 4:
        out = out + 4 - 8 * lax.rem(dev // 4, 2)
    return out


def total(x):
    return jnp.sum(jnp.sum(x, axis=0, keepdims=True), axis=1, keepdims=True)


def kernel(
    psi_hbm, left_ref, right_ref, phys_ref, out_ref, alpha_ref, beta_ref, scale_ref,
    left, right, phys, wide, v_in, y_buf, z_buf0, z_buf1, acc, sig, v_cur, v_prev, beta_old, stats, mine,
    turned, got, got_end, across, numbers, dense, psi_ref, psi_sem, tri, squares,
    r_send, r_recv, w_send, w_recv, l_send, l_recv, s_send, s_recv, g_send, g_recv, o_send, o_recv, e_send, e_recv,
):
    me = lax.axis_index("terms")
    peers = {e: flip(me, e) for e in range(1, DEVS)}

    psi_copies = [pltpu.make_async_copy(psi_hbm.at[r], psi_ref.at[r], psi_sem.at[r]) for r in range(2)]
    for psi_copy in psi_copies:
        psi_copy.start()
    barrier = pltpu.get_barrier_semaphore()
    for e in range(1, DEVS):
        pl.semaphore_signal(barrier, inc=1, device_id=(peers[e],), device_id_type=MESH)

    def copy(src, dst, send, recv, e):
        return pltpu.make_async_remote_copy(
            src_ref=src, dst_ref=dst, send_sem=send, recv_sem=recv, device_id=(peers[e],), device_id_type=MESH
        )

    def r_copy(e):
        rows = pl.ds(pl.multiple_of(peers[e] * ROWS, ROWS), ROWS)
        return copy(right_ref.at[:, rows, :], right.at[e], r_send.at[e], r_recv.at[e], e)

    def w_copy(e):
        return copy(dense, phys.at[e], w_send.at[e], w_recv.at[e], e)

    def part(x):
        return slice(0, 512) if x == 0 else slice(512, PACKED)

    def l_copy(e, x):
        return copy(tri.at[0, part(x)], tri.at[e, part(x)], l_send.at[e, x], l_recv.at[e, x], e)

    def l_far(x):
        e = (2, 4)[x]
        return copy(tri.at[e, part(x)], tri.at[6, part(x)], l_send.at[6, x], l_recv.at[6, x], 6 - e)

    def l_pass(e, x):
        return copy(tri.at[e, part(x)], tri.at[e + 1, part(x)], l_send.at[e + 1, x], l_recv.at[e + 1, x], 1)

    def s_copy(r, e):
        return copy(mine.at[r], stats.at[r, me], s_send.at[r, e], s_recv.at[r, e], e)

    def g_copy(r, g, e):
        slot = v_in.at[r, me, g * 8 : (g + 1) * 8]
        return copy(slot, slot, g_send.at[r, g, e], g_recv.at[r, g, e], e)

    def g_pass(r, g, e):
        slot = v_in.at[r, peers[e], g * 8 : (g + 1) * 8]
        return copy(slot, slot, g_send.at[r, g, e + 1], g_recv.at[r, g, e + 1], 1)

    def o_copy(r, j, e):
        rows = pl.ds(pl.multiple_of(peers[e] * ROWS, ROWS), ROWS)
        way = lax.rem(j, 2)
        return copy(turned.at[r, :, rows, :], got.at[r, way, me], o_send.at[r, way, e], o_recv.at[r, way, e], e)

    def e_copy(e):
        rows = pl.ds(pl.multiple_of(peers[e] * ROWS, ROWS), ROWS)
        return copy(turned.at[1, :, rows, :], got_end.at[me], e_send.at[e], e_recv.at[e], e)

    row = lax.broadcasted_iota(jnp.int32, (BOND, BOND), 0)
    col = lax.broadcasted_iota(jnp.int32, (BOND, BOND), 1)
    diag_row = lax.broadcasted_iota(jnp.int32, (16, BOND), 0)
    diags = jnp.zeros((16, BOND), F32)
    for i in range(TERMS // 2):
        one, two = left_ref[2 * i].astype(F32), left_ref[2 * i + 1].astype(F32)
        tri[0, i * BOND : (i + 1) * BOND, :] = jnp.where(row < col, one, two).astype(BF16)
        diag = jnp.sum(jnp.where(row == col, one, 0.0), axis=0, keepdims=True)
        diags = jnp.where(diag_row == i, diag, diags)
    tri[0, PACKED - 16 : PACKED, :] = diags.astype(BF16)

    def unpack(d):
        diags = tri[d, PACKED - 16 : PACKED, :].astype(F32)
        for i in range(TERMS // 2):
            m = tri[d, i * BOND : (i + 1) * BOND, :].astype(F32)
            turned_m = m.T
            one = jnp.where(row < col, m, jnp.where(row > col, turned_m, diags[i : i + 1, :]))
            left[d, 2 * i] = one.astype(BF16)
            left[d, 2 * i + 1] = jnp.where(row < col, turned_m, m).astype(BF16)

    w_own = phys_ref[...].astype(F32)
    row_u = lax.broadcasted_iota(jnp.int32, (PAIRS, PAIRS * PAIRS), 0)
    col_qu = lax.broadcasted_iota(jnp.int32, (PAIRS, PAIRS * PAIRS), 1)
    flat = jnp.zeros((TERMS, PAIRS * PAIRS), F32)
    for q in range(PAIRS):
        put = jnp.where(col_qu == row_u + q * PAIRS, 1.0, 0.0).astype(BF16)
        flat += jnp.dot(w_own[:, q, :].astype(BF16), put, preferred_element_type=F32)
    dense[...] = flat.astype(BF16)
    pl.semaphore_wait(barrier, DEVS - 1)

    for e in (1, 2, 4, 3, 5, 6, 7):
        r_copy(e).start()
        w_copy(e).start()
    for e, x in ((1, 0), (1, 1), (2, 0), (4, 1), (2, 1), (4, 0)):
        l_copy(e, x).start()
    own = pl.ds(pl.multiple_of(me * ROWS, ROWS), ROWS)
    right[0] = right_ref[:, own, :]
    phys[0] = dense[...]
    left[0] = left_ref[...]
    v_prev[...] = jnp.zeros_like(v_prev)
    beta_old[...] = jnp.zeros_like(beta_old)
    numbers[...] = jnp.zeros_like(numbers)

    def prepare(r):
        psi_copies[r].wait()
        squares[...] = jnp.zeros((BOND, BOND), F32)

        @pl.loop(0, 4)
        def _(s):
            for t in range(4):
                x = psi_ref[r, :, s, t, :]
                squares[...] += x * x
                across[s * 4 + t] = x.T

        norm = jnp.sqrt(total(squares[...]) / N_ELEMS)

        @pl.loop(0, PAIRS)
        def _(u):
            v_in[r, :, u] = (across[u] / norm).astype(BF16).reshape(DEVS, ROWS, BOND)
            two = across[u, own, :] / norm
            row = pl.multiple_of(u * 8, 8)
            v_cur[r, pl.ds(row, 8), :] = two[0:8]
            v_cur[r, pl.ds(row + BOND, 8), :] = two[8:16]

        for q in range(PAIRS):
            out_ref[r, 0, :, q, :] = psi_ref[r, own, q // 4, q % 4, :] / norm

    prepare(0)

    sub = lax.broadcasted_iota(jnp.int32, (8, BOND), 0)
    lane = lax.broadcasted_iota(jnp.int32, (8, BOND), 1)
    eye = jnp.where(lax.rem(lane, 8) == sub, 1.0, 0.0).astype(F32)
    pick_row = lax.broadcasted_iota(jnp.int32, (PAIRS * PAIRS, BOND), 0)
    pick_col = lax.broadcasted_iota(jnp.int32, (PAIRS * PAIRS, BOND), 1) // 8

    def widen(d):
        w_d = phys[d]
        spread = []
        for q in range(PAIRS):
            pick = jnp.where(pick_row == pick_col + q * PAIRS, 1.0, 0.0).astype(BF16)
            spread.append(jnp.dot(w_d, pick, preferred_element_type=F32))
        for k in range(TERMS):
            for q in range(0, PAIRS, 2):
                two = [jnp.broadcast_to(spread[q + i][k : k + 1, :], (8, BOND)) * eye for i in range(2)]
                wide[d, k, q * 8 : q * 8 + 16, :] = jnp.concatenate(two, axis=0).astype(BF16)

    def form_y(r, d, pairs):
        r_d = right[d].reshape(TERMS * ROWS, BOND)
        for u in pairs:
            v_u = jnp.concatenate([v_in[r, :, u + i].reshape(BOND, BOND) for i in range(2)], axis=1)
            y = jnp.dot(r_d, v_u, preferred_element_type=F32).reshape(TERMS, 2, 8, 2 * BOND)
            y = jnp.concatenate([y[..., :BOND], y[..., BOND:]], axis=2)
            y_buf[d, :, :, u * 8 : u * 8 + 16, :] = y.astype(BF16)

    def form_out(d, z_buf, first):
        for k in range(TERMS):
            y_k = jnp.concatenate([y_buf[d, k, 0], y_buf[d, k, 1]], axis=1)
            z = jnp.dot(wide[d, k], y_k, preferred_element_type=F32).astype(BF16)
            for h in range(2):
                z_buf[h * BOND : (h + 1) * BOND, k * BOND : (k + 1) * BOND] = z[:, h * BOND : (h + 1) * BOND]
        part = jnp.dot(z_buf[...], left[d].reshape(TERMS * BOND, BOND), preferred_element_type=F32)
        if first:
            acc[...] = part
        else:
            acc[...] += part

    def share(r):
        s, v, vp = acc[...], v_cur[r], v_prev[r]
        d_p, n_p = total(s * v), total(v * v)
        guess = jnp.where(n_p > 0.0, d_p / jnp.where(n_p > 0.0, n_p, 1.0), 0.0)
        s = s - guess * v - beta_old[r, 0:1, :] * vp
        sig[r] = s
        rows = [d_p, n_p, guess, total(s * s), total(s * v)]
        tile = jnp.zeros((8, BOND), F32)
        for i, row in enumerate(rows):
            tile = jnp.where(sub == i, row, tile)
        mine[r] = tile
        stats[r, me] = tile
        for e in (6, 7, 2, 3, 4, 5, 1):
            s_copy(r, e).start()

    def scalars(r, j):
        for e in range(1, DEVS):
            s_copy(r, e).wait()
        alpha = jnp.zeros((1, BOND), F32)
        for p in range(DEVS):
            alpha = alpha + stats[r, p, 0:1, :]
        alpha = alpha / N_ELEMS
        square = jnp.zeros((1, BOND), F32)
        for p in range(DEVS):
            d_p = alpha - stats[r, p, 2:3, :]
            square = square + (stats[r, p, 3:4, :] - 2.0 * d_p * stats[r, p, 4:5, :] + d_p * d_p * stats[r, p, 1:2, :])
        beta = jnp.sqrt(jnp.maximum(square, 0.0) / N_ELEMS)
        here = jnp.logical_and(sub == r, lane == j)
        numbers[0] = jnp.where(here, alpha, numbers[0])
        numbers[1] = jnp.where(here, beta, numbers[1])
        return alpha, beta

    def turn(r, joined):
        for g in range(2):
            turned[r, g] = joined[g * 8 : (g + 1) * 8].reshape(BOND, BOND).T

    def advance(r, j, last):
        alpha, beta = scalars(r, j)
        shift = alpha - mine[r, 2:3, :]
        v = v_cur[r]
        nxt = (sig[r] - shift * v) / beta
        v_prev[r] = v
        v_cur[r] = nxt
        beta_old[r] = jnp.broadcast_to(beta, (8, BOND))
        halves = nxt.reshape(2, PAIRS, 8, BOND)
        joined = jnp.concatenate([halves[0], halves[1]], axis=1)

        @pl.when(jnp.logical_not(last))
        def _():
            v_in[r, me] = joined.astype(BF16)
            for g in range(2):
                for e in (6, 4, 2, 1):
                    g_copy(r, g, e).start()


    def post(r, j):
        halves = v_cur[r].reshape(2, PAIRS, 8, BOND)
        turn(r, jnp.concatenate([halves[0], halves[1]], axis=1))
        for e in (6, 7, 2, 3, 4, 5, 1):
            o_copy(r, j, e).start()
        got[r, lax.rem(j, 2), me] = turned[r, :, own, :]

    def relay(r, g):
        for e in (4, 6, 2):
            g_copy(r, g, e).wait()
            g_pass(r, g, e).start()

    def arrive(r, g):
        g_copy(r, g, 1).wait()
        for e in (4, 6, 2):
            g_pass(r, g, e).wait()

    def assemble(read):
        chunk_of = lax.broadcasted_iota(jnp.int32, (ROWS, BOND), 1) // 16
        pairs = []
        for g in range(2):
            x = [read(p, g) for p in range(DEVS)]
            for bit in (1, 2, 4):
                odd = lax.rem(chunk_of // bit, 2) == 1
                for p in range(DEVS):
                    if p & bit:
                        continue
                    low, high = x[p], x[p + bit]
                    x[p] = jnp.where(odd, pltpu.roll(high, 16 * bit, 1), low)
                    x[p + bit] = jnp.where(odd, high, pltpu.roll(low, BOND - 16 * bit, 1))
            pairs += x
        return pairs

    def collect(r, j):
        for e in range(1, DEVS):
            o_copy(r, j, e).wait()
        for q, x in enumerate(assemble(lambda p, g: got[r, lax.rem(j, 2), p, g])):
            out_ref[r, j + 1, :, q, :] = x


    @pl.loop(0, DEVS)
    def _(d):
        for e in range(1, DEVS):

            @pl.when(d == e)
            def _():
                r_copy(e).wait()
                w_copy(e).wait()

        widen(d)
        form_y(0, d, range(0, PAIRS, 2))

    for d in range(DEVS):
        nxt = d + 1
        if nxt == 1:
            l_copy(1, 0).wait()
            l_copy(1, 1).wait()
        elif nxt == 2:
            for e, x in ((2, 0), (4, 1)):
                l_copy(e, x).wait()
                l_far(x).start()
                l_pass(e, x).start()
            prepare(1)
            for e, x in ((2, 1), (4, 0)):
                l_copy(e, x).wait()
                l_pass(e, x).start()
        elif nxt == 6:
            for x in range(2):
                l_far(x).wait()
                l_pass(6, x).start()
        elif nxt in (3, 5, 7):
            for x in range(2):
                l_pass(nxt - 1, x).wait()
        if nxt < DEVS:
            unpack(nxt)
        form_out(d, (z_buf0, z_buf1)[d % 2], d == 0)

    share(0)

    @pl.loop(1, 2 * STEPS)
    def _(t):
        r, j = lax.rem(t, 2), t // 2
        pr, pj = 1 - r, (t - 1) // 2

        for g in range(2):

            @pl.when(t >= 2)
            def _():
                arrive(r, g)

            for u in range(g * 8, (g + 1) * 8, 2):
                for d in range(DEVS):
                    form_y(r, d, (u,))

        for d in range(DEVS):
            if d == FORM_BEFORE:
                advance(pr, pj, t == 2 * STEPS - 1)

                @pl.when(t == 2 * STEPS - 1)
                def _():
                    post(pr, pj)

            form_out(d, (z_buf0, z_buf1)[d % 2], d == 0)

        share(r)

        @pl.when(t < 2 * STEPS - 1)
        def _():
            relay(pr, 0)
            post(pr, pj)

        @pl.when(t >= 2)
        def _():
            collect(r, j - 1)

        @pl.when(t < 2 * STEPS - 1)
        def _():
            relay(pr, 1)

    halves = sig[1].reshape(2, PAIRS, 8, BOND)
    turn(1, jnp.concatenate([halves[0], halves[1]], axis=1))
    for e in (6, 7, 2, 3, 4, 5, 1):
        e_copy(e).start()
    got_end[me] = turned[1, :, own, :]
    collect(0, STEPS - 1)
    alpha, beta = scalars(1, STEPS - 1)
    shift = jnp.zeros((1, BOND), F32)
    for p in range(DEVS):
        shift = jnp.where(lane[0:1] // 16 == p, alpha - stats[1, p, 2:3, :], shift)
    for e in range(1, DEVS):
        e_copy(e).wait()
    for q, x in enumerate(assemble(lambda p, g: got_end[p, g])):
        v = out_ref[1, STEPS - 1, :, q, :]
        out_ref[1, STEPS, :, q, :] = x - shift * v
    alpha_ref[...] = numbers[0, 0:2, 0:STEPS]
    beta_ref[...] = numbers[1, 0:2, 0:STEPS]
    end = jnp.logical_and(sub == 1, lane == STEPS)
    scale_ref[...] = jnp.where(end, 1.0 / beta, jnp.ones((8, BOND), F32))[0:2, 0 : STEPS + 1]


def solution(mesh):
    def device_fn(psi, left_loc, phys_loc, right_loc):
        roots = psi.shape[0]
        anywhere, vm = pl.BlockSpec(memory_space=pl.ANY), pl.BlockSpec(memory_space=pltpu.VMEM)
        dma = pltpu.SemaphoreType.DMA
        vecs, alpha, beta, scale = pl.pallas_call(
            kernel,
            out_shape=(
                jax.ShapeDtypeStruct((roots, STEPS + 1, ROWS, PAIRS, BOND), F32),
                jax.ShapeDtypeStruct((roots, STEPS), F32),
                jax.ShapeDtypeStruct((roots, STEPS), F32),
                jax.ShapeDtypeStruct((roots, STEPS + 1), F32),
            ),
            in_specs=[anywhere, vm, vm, vm],
            out_specs=[vm] * 4,
            scratch_shapes=[
                pltpu.VMEM((DEVS, TERMS, BOND, BOND), BF16),
                pltpu.VMEM((DEVS, TERMS, ROWS, BOND), BF16),
                pltpu.VMEM((DEVS, TERMS, PAIRS * PAIRS), BF16),
                pltpu.VMEM((DEVS, TERMS, BOND, BOND), BF16),
                pltpu.VMEM((roots, DEVS, PAIRS, ROWS, BOND), BF16),
                pltpu.VMEM((DEVS, TERMS, 2, BOND, BOND), BF16),
                pltpu.VMEM((2 * BOND, TERMS * BOND), BF16),
                pltpu.VMEM((2 * BOND, TERMS * BOND), BF16),
                pltpu.VMEM((2 * BOND, BOND), F32),
                pltpu.VMEM((roots, 2 * BOND, BOND), F32),
                pltpu.VMEM((roots, 2 * BOND, BOND), F32),
                pltpu.VMEM((roots, 2 * BOND, BOND), F32),
                pltpu.VMEM((roots, 8, BOND), F32),
                pltpu.VMEM((roots, DEVS, 8, BOND), F32),
                pltpu.VMEM((roots, 8, BOND), F32),
                pltpu.VMEM((roots, 2, BOND, BOND), F32),
                pltpu.VMEM((roots, 2, DEVS, 2, ROWS, BOND), F32),
                pltpu.VMEM((DEVS, 2, ROWS, BOND), F32),
                pltpu.VMEM((PAIRS, BOND, BOND), F32),
                pltpu.VMEM((2, 8, BOND), F32),
                pltpu.VMEM((TERMS, PAIRS * PAIRS), BF16),
                pltpu.VMEM(psi.shape, F32),
                dma((roots,)),
                pltpu.VMEM((DEVS, PACKED, BOND), BF16),
                pltpu.VMEM((BOND, BOND), F32),
                dma((DEVS,)), dma((DEVS,)), dma((DEVS,)), dma((DEVS,)), dma((DEVS, 2)), dma((DEVS, 2)),
                dma((roots, DEVS)), dma((roots, DEVS)), dma((roots, 2, DEVS)), dma((roots, 2, DEVS)),
                dma((roots, 2, DEVS)), dma((roots, 2, DEVS)), dma((DEVS,)), dma((DEVS,)),
            ],
            compiler_params=pltpu.CompilerParams(
                collective_id=0, has_side_effects=True, vmem_limit_bytes=50 * 1024 * 1024
            ),
        )(psi, left_loc, right_loc, phys_loc)
        vecs = vecs * scale[:, :, None, None, None]
        return vecs.reshape(roots, STEPS + 1, ROWS, *psi.shape[2:]), alpha, beta

    return jax.shard_map(
        device_fn, mesh=mesh, in_specs=(P(), P("terms"), P("terms"), P("terms")),
        out_specs=(P(None, None, "terms"), P(), P()), check_vma=False,
    )
```

```python
import functools

import jax
import jax.numpy as jnp
from jax import lax
from jax.experimental import pallas as pl
from jax.experimental.pallas import tpu as pltpu
from jax.sharding import PartitionSpec as P

STEPS = 6
DEVS = 8
TERMS = 16
PAIRS = 16
BOND = 128
PACKED = TERMS // 2 * BOND + 16
ROWS = 16
N_ELEMS = float(BOND * PAIRS * BOND)
FORM_BEFORE = 0
MESH = pl.DeviceIdType.MESH
F32 = jnp.float32
BF16 = jnp.bfloat16


def flip(dev, bits):
    out = dev
    if bits & 1:
        out = out + 1 - 2 * lax.rem(dev, 2)
    if bits & 2:
        out = out + 2 - 4 * lax.rem(dev // 2, 2)
    if bits & 4:
        out = out + 4 - 8 * lax.rem(dev // 4, 2)
    return out


def total(x):
    return jnp.sum(jnp.sum(x, axis=0, keepdims=True), axis=1, keepdims=True)


def kernel(
    psi_hbm, left_hbm, right_hbm, phys_hbm, out_ref, alpha_ref, beta_ref, scale_ref,
    left, right, phys, wide, v_in, y_buf, z_buf0, z_buf1, acc, sig, v_cur, v_prev, beta_old, stats, mine,
    turned, got, got_end, across, numbers, dense, psi_ref, psi_sem, tri, squares,
    left_ref, right_ref, phys_ref, in_sem,
    r_send, r_recv, w_send, w_recv, l_send, l_recv, s_send, s_recv, g_send, g_recv, o_send, o_recv, e_send, e_recv,
):
    me = lax.axis_index("terms")
    peers = {e: flip(me, e) for e in range(1, DEVS)}

    pairs = ((right_hbm, right_ref), (phys_hbm, phys_ref), (left_hbm, left_ref))
    in_copies = [pltpu.make_async_copy(src, dst, in_sem.at[i]) for i, (src, dst) in enumerate(pairs)]
    psi_copies = [pltpu.make_async_copy(psi_hbm.at[r], psi_ref.at[r], psi_sem.at[r]) for r in range(2)]
    for in_copy in in_copies + psi_copies:
        in_copy.start()
    barrier = pltpu.get_barrier_semaphore()
    for e in range(1, DEVS):
        pl.semaphore_signal(barrier, inc=1, device_id=(peers[e],), device_id_type=MESH)
    for in_copy in in_copies:
        in_copy.wait()

    def copy(src, dst, send, recv, e):
        return pltpu.make_async_remote_copy(
            src_ref=src, dst_ref=dst, send_sem=send, recv_sem=recv, device_id=(peers[e],), device_id_type=MESH
        )

    def r_copy(e):
        rows = pl.ds(pl.multiple_of(peers[e] * ROWS, ROWS), ROWS)
        return copy(right_ref.at[:, rows, :], right.at[e], r_send.at[e], r_recv.at[e], e)

    def w_copy(e):
        return copy(dense, phys.at[e], w_send.at[e], w_recv.at[e], e)

    def part(x):
        return slice(0, 512) if x == 0 else slice(512, PACKED)

    def l_copy(e, x):
        return copy(tri.at[0, part(x)], tri.at[e, part(x)], l_send.at[e, x], l_recv.at[e, x], e)

    def l_far(x):
        e = (2, 4)[x]
        return copy(tri.at[e, part(x)], tri.at[6, part(x)], l_send.at[6, x], l_recv.at[6, x], 6 - e)

    def l_pass(e, x):
        return copy(tri.at[e, part(x)], tri.at[e + 1, part(x)], l_send.at[e + 1, x], l_recv.at[e + 1, x], 1)

    def s_copy(r, e):
        return copy(mine.at[r], stats.at[r, me], s_send.at[r, e], s_recv.at[r, e], e)

    def g_copy(r, g, e):
        slot = v_in.at[r, me, g * 8 : (g + 1) * 8]
        return copy(slot, slot, g_send.at[r, g, e], g_recv.at[r, g, e], e)

    def g_pass(r, g, e):
        slot = v_in.at[r, peers[e], g * 8 : (g + 1) * 8]
        return copy(slot, slot, g_send.at[r, g, e + 1], g_recv.at[r, g, e + 1], 1)

    def o_copy(r, j, e):
        rows = pl.ds(pl.multiple_of(peers[e] * ROWS, ROWS), ROWS)
        way = lax.rem(j, 2)
        return copy(turned.at[r, :, rows, :], got.at[r, way, me], o_send.at[r, way, e], o_recv.at[r, way, e], e)

    def e_copy(e):
        rows = pl.ds(pl.multiple_of(peers[e] * ROWS, ROWS), ROWS)
        return copy(turned.at[1, :, rows, :], got_end.at[me], e_send.at[e], e_recv.at[e], e)

    row = lax.broadcasted_iota(jnp.int32, (BOND, BOND), 0)
    col = lax.broadcasted_iota(jnp.int32, (BOND, BOND), 1)
    diag_row = lax.broadcasted_iota(jnp.int32, (16, BOND), 0)
    diags = jnp.zeros((16, BOND), F32)
    for i in range(TERMS // 2):
        one, two = left_ref[2 * i].astype(F32), left_ref[2 * i + 1].astype(F32)
        tri[0, i * BOND : (i + 1) * BOND, :] = jnp.where(row < col, one, two).astype(BF16)
        diag = jnp.sum(jnp.where(row == col, one, 0.0), axis=0, keepdims=True)
        diags = jnp.where(diag_row == i, diag, diags)
    tri[0, PACKED - 16 : PACKED, :] = diags.astype(BF16)

    def unpack(d):
        diags = tri[d, PACKED - 16 : PACKED, :].astype(F32)
        for i in range(TERMS // 2):
            m = tri[d, i * BOND : (i + 1) * BOND, :].astype(F32)
            turned_m = m.T
            one = jnp.where(row < col, m, jnp.where(row > col, turned_m, diags[i : i + 1, :]))
            left[d, 2 * i] = one.astype(BF16)
            left[d, 2 * i + 1] = jnp.where(row < col, turned_m, m).astype(BF16)

    w_own = phys_ref[...].astype(F32)
    row_u = lax.broadcasted_iota(jnp.int32, (PAIRS, PAIRS * PAIRS), 0)
    col_qu = lax.broadcasted_iota(jnp.int32, (PAIRS, PAIRS * PAIRS), 1)
    flat = jnp.zeros((TERMS, PAIRS * PAIRS), F32)
    for q in range(PAIRS):
        put = jnp.where(col_qu == row_u + q * PAIRS, 1.0, 0.0).astype(BF16)
        flat += jnp.dot(w_own[:, q, :].astype(BF16), put, preferred_element_type=F32)
    dense[...] = flat.astype(BF16)
    pl.semaphore_wait(barrier, DEVS - 1)

    for e in (1, 2, 4, 3, 5, 6, 7):
        r_copy(e).start()
        w_copy(e).start()
    for e, x in ((1, 0), (1, 1), (2, 0), (4, 1), (2, 1), (4, 0)):
        l_copy(e, x).start()
    own = pl.ds(pl.multiple_of(me * ROWS, ROWS), ROWS)
    right[0] = right_ref[:, own, :]
    phys[0] = dense[...]
    left[0] = left_ref[...]
    v_prev[...] = jnp.zeros_like(v_prev)
    beta_old[...] = jnp.zeros_like(beta_old)
    numbers[...] = jnp.zeros_like(numbers)

    def prepare(r):
        psi_copies[r].wait()
        squares[...] = jnp.zeros((BOND, BOND), F32)

        @pl.loop(0, 4)
        def _(s):
            for t in range(4):
                x = psi_ref[r, :, s, t, :]
                squares[...] += x * x
                across[s * 4 + t] = x.T

        norm = jnp.sqrt(total(squares[...]) / N_ELEMS)

        @pl.loop(0, PAIRS)
        def _(u):
            v_in[r, :, u] = (across[u] / norm).astype(BF16).reshape(DEVS, ROWS, BOND)
            two = across[u, own, :] / norm
            row = pl.multiple_of(u * 8, 8)
            v_cur[r, pl.ds(row, 8), :] = two[0:8]
            v_cur[r, pl.ds(row + BOND, 8), :] = two[8:16]

        for q in range(PAIRS):
            out_ref[r, 0, :, q, :] = psi_ref[r, own, q // 4, q % 4, :] / norm

    prepare(0)

    sub = lax.broadcasted_iota(jnp.int32, (8, BOND), 0)
    lane = lax.broadcasted_iota(jnp.int32, (8, BOND), 1)
    eye = jnp.where(lax.rem(lane, 8) == sub, 1.0, 0.0).astype(F32)
    pick_row = lax.broadcasted_iota(jnp.int32, (PAIRS * PAIRS, BOND), 0)
    pick_col = lax.broadcasted_iota(jnp.int32, (PAIRS * PAIRS, BOND), 1) // 8

    def widen(d):
        w_d = phys[d]
        spread = []
        for q in range(PAIRS):
            pick = jnp.where(pick_row == pick_col + q * PAIRS, 1.0, 0.0).astype(BF16)
            spread.append(jnp.dot(w_d, pick, preferred_element_type=F32))
        for k in range(TERMS):
            for q in range(0, PAIRS, 2):
                two = [jnp.broadcast_to(spread[q + i][k : k + 1, :], (8, BOND)) * eye for i in range(2)]
                wide[d, k, q * 8 : q * 8 + 16, :] = jnp.concatenate(two, axis=0).astype(BF16)

    def form_y(r, d, pairs):
        r_d = right[d].reshape(TERMS * ROWS, BOND)
        for u in pairs:
            v_u = jnp.concatenate([v_in[r, :, u + i].reshape(BOND, BOND) for i in range(2)], axis=1)
            y = jnp.dot(r_d, v_u, preferred_element_type=F32).reshape(TERMS, 2, 8, 2 * BOND)
            y = jnp.concatenate([y[..., :BOND], y[..., BOND:]], axis=2)
            y_buf[d, :, :, u * 8 : u * 8 + 16, :] = y.astype(BF16)

    def form_out(d, z_buf, first):
        for k in range(TERMS):
            y_k = jnp.concatenate([y_buf[d, k, 0], y_buf[d, k, 1]], axis=1)
            z = jnp.dot(wide[d, k], y_k, preferred_element_type=F32).astype(BF16)
            for h in range(2):
                z_buf[h * BOND : (h + 1) * BOND, k * BOND : (k + 1) * BOND] = z[:, h * BOND : (h + 1) * BOND]
        part = jnp.dot(z_buf[...], left[d].reshape(TERMS * BOND, BOND), preferred_element_type=F32)
        if first:
            acc[...] = part
        else:
            acc[...] += part

    def share(r):
        s, v, vp = acc[...], v_cur[r], v_prev[r]
        d_p, n_p = total(s * v), total(v * v)
        guess = jnp.where(n_p > 0.0, d_p / jnp.where(n_p > 0.0, n_p, 1.0), 0.0)
        s = s - guess * v - beta_old[r, 0:1, :] * vp
        sig[r] = s
        rows = [d_p, n_p, guess, total(s * s), total(s * v)]
        tile = jnp.zeros((8, BOND), F32)
        for i, row in enumerate(rows):
            tile = jnp.where(sub == i, row, tile)
        mine[r] = tile
        stats[r, me] = tile
        for e in (6, 7, 2, 3, 4, 5, 1):
            s_copy(r, e).start()

    def scalars(r, j):
        for e in range(1, DEVS):
            s_copy(r, e).wait()
        alpha = jnp.zeros((1, BOND), F32)
        for p in range(DEVS):
            alpha = alpha + stats[r, p, 0:1, :]
        alpha = alpha / N_ELEMS
        square = jnp.zeros((1, BOND), F32)
        for p in range(DEVS):
            d_p = alpha - stats[r, p, 2:3, :]
            square = square + (stats[r, p, 3:4, :] - 2.0 * d_p * stats[r, p, 4:5, :] + d_p * d_p * stats[r, p, 1:2, :])
        beta = jnp.sqrt(jnp.maximum(square, 0.0) / N_ELEMS)
        here = jnp.logical_and(sub == r, lane == j)
        numbers[0] = jnp.where(here, alpha, numbers[0])
        numbers[1] = jnp.where(here, beta, numbers[1])
        return alpha, beta

    def turn(r, joined):
        for g in range(2):
            turned[r, g] = joined[g * 8 : (g + 1) * 8].reshape(BOND, BOND).T

    def advance(r, j, last):
        alpha, beta = scalars(r, j)
        shift = alpha - mine[r, 2:3, :]
        v = v_cur[r]
        nxt = (sig[r] - shift * v) / beta
        v_prev[r] = v
        v_cur[r] = nxt
        beta_old[r] = jnp.broadcast_to(beta, (8, BOND))
        halves = nxt.reshape(2, PAIRS, 8, BOND)
        joined = jnp.concatenate([halves[0], halves[1]], axis=1)

        @pl.when(jnp.logical_not(last))
        def _():
            v_in[r, me] = joined.astype(BF16)
            for g in range(2):
                for e in (6, 4, 2, 1):
                    g_copy(r, g, e).start()


    def post(r, j):
        halves = v_cur[r].reshape(2, PAIRS, 8, BOND)
        turn(r, jnp.concatenate([halves[0], halves[1]], axis=1))
        for e in (6, 7, 2, 3, 4, 5, 1):
            o_copy(r, j, e).start()
        got[r, lax.rem(j, 2), me] = turned[r, :, own, :]

    def relay(r, g):
        for e in (4, 6, 2):
            g_copy(r, g, e).wait()
            g_pass(r, g, e).start()

    def arrive(r, g):
        g_copy(r, g, 1).wait()
        for e in (4, 6, 2):
            g_pass(r, g, e).wait()

    def assemble(read):
        chunk_of = lax.broadcasted_iota(jnp.int32, (ROWS, BOND), 1) // 16
        pairs = []
        for g in range(2):
            x = [read(p, g) for p in range(DEVS)]
            for bit in (1, 2, 4):
                odd = lax.rem(chunk_of // bit, 2) == 1
                for p in range(DEVS):
                    if p & bit:
                        continue
                    low, high = x[p], x[p + bit]
                    x[p] = jnp.where(odd, pltpu.roll(high, 16 * bit, 1), low)
                    x[p + bit] = jnp.where(odd, high, pltpu.roll(low, BOND - 16 * bit, 1))
            pairs += x
        return pairs

    def collect(r, j):
        for e in range(1, DEVS):
            o_copy(r, j, e).wait()
        for q, x in enumerate(assemble(lambda p, g: got[r, lax.rem(j, 2), p, g])):
            out_ref[r, j + 1, :, q, :] = x


    @pl.loop(0, DEVS)
    def _(d):
        for e in range(1, DEVS):

            @pl.when(d == e)
            def _():
                r_copy(e).wait()
                w_copy(e).wait()

        widen(d)
        form_y(0, d, range(0, PAIRS, 2))

    for d in range(DEVS):
        nxt = d + 1
        if nxt == 1:
            l_copy(1, 0).wait()
            l_copy(1, 1).wait()
        elif nxt == 2:
            for e, x in ((2, 0), (4, 1)):
                l_copy(e, x).wait()
                l_far(x).start()
                l_pass(e, x).start()
            prepare(1)
            for e, x in ((2, 1), (4, 0)):
                l_copy(e, x).wait()
                l_pass(e, x).start()
        elif nxt == 6:
            for x in range(2):
                l_far(x).wait()
                l_pass(6, x).start()
        elif nxt in (3, 5, 7):
            for x in range(2):
                l_pass(nxt - 1, x).wait()
        if nxt < DEVS:
            unpack(nxt)
        form_out(d, (z_buf0, z_buf1)[d % 2], d == 0)

    share(0)

    @pl.loop(1, 2 * STEPS)
    def _(t):
        r, j = lax.rem(t, 2), t // 2
        pr, pj = 1 - r, (t - 1) // 2

        for g in range(2):

            @pl.when(t >= 2)
            def _():
                arrive(r, g)

            for u in range(g * 8, (g + 1) * 8, 2):
                for d in range(DEVS):
                    form_y(r, d, (u,))

        for d in range(DEVS):
            if d == FORM_BEFORE:
                advance(pr, pj, t == 2 * STEPS - 1)

                @pl.when(t == 2 * STEPS - 1)
                def _():
                    post(pr, pj)

            form_out(d, (z_buf0, z_buf1)[d % 2], d == 0)

        share(r)

        @pl.when(t < 2 * STEPS - 1)
        def _():
            relay(pr, 0)
            post(pr, pj)

        @pl.when(t >= 2)
        def _():
            collect(r, j - 1)

        @pl.when(t < 2 * STEPS - 1)
        def _():
            relay(pr, 1)

    halves = sig[1].reshape(2, PAIRS, 8, BOND)
    turn(1, jnp.concatenate([halves[0], halves[1]], axis=1))
    for e in (6, 7, 2, 3, 4, 5, 1):
        e_copy(e).start()
    got_end[me] = turned[1, :, own, :]
    collect(0, STEPS - 1)
    alpha, beta = scalars(1, STEPS - 1)
    shift = jnp.zeros((1, BOND), F32)
    for p in range(DEVS):
        shift = jnp.where(lane[0:1] // 16 == p, alpha - stats[1, p, 2:3, :], shift)
    for e in range(1, DEVS):
        e_copy(e).wait()
    for q, x in enumerate(assemble(lambda p, g: got_end[p, g])):
        v = out_ref[1, STEPS - 1, :, q, :]
        out_ref[1, STEPS, :, q, :] = x - shift * v
    alpha_ref[...] = numbers[0, 0:2, 0:STEPS]
    beta_ref[...] = numbers[1, 0:2, 0:STEPS]
    end = jnp.logical_and(sub == 1, lane == STEPS)
    scale_ref[...] = jnp.where(end, 1.0 / beta, jnp.ones((8, BOND), F32))[0:2, 0 : STEPS + 1]


def solution(mesh):
    def device_fn(psi, left_loc, phys_loc, right_loc):
        roots = psi.shape[0]
        dma = pltpu.SemaphoreType.DMA
        vecs, alpha, beta, scale = pl.pallas_call(
            kernel,
            out_shape=(
                jax.ShapeDtypeStruct((roots, STEPS + 1, ROWS, PAIRS, BOND), F32),
                jax.ShapeDtypeStruct((roots, STEPS), F32),
                jax.ShapeDtypeStruct((roots, STEPS), F32),
                jax.ShapeDtypeStruct((roots, STEPS + 1), F32),
            ),
            in_specs=[pl.BlockSpec(memory_space=pltpu.HBM)] * 4,
            out_specs=[pl.BlockSpec(memory_space=pltpu.VMEM)] * 4,
            scratch_shapes=[
                pltpu.VMEM((DEVS, TERMS, BOND, BOND), BF16),
                pltpu.VMEM((DEVS, TERMS, ROWS, BOND), BF16),
                pltpu.VMEM((DEVS, TERMS, PAIRS * PAIRS), BF16),
                pltpu.VMEM((DEVS, TERMS, BOND, BOND), BF16),
                pltpu.VMEM((roots, DEVS, PAIRS, ROWS, BOND), BF16),
                pltpu.VMEM((DEVS, TERMS, 2, BOND, BOND), BF16),
                pltpu.VMEM((2 * BOND, TERMS * BOND), BF16),
                pltpu.VMEM((2 * BOND, TERMS * BOND), BF16),
                pltpu.VMEM((2 * BOND, BOND), F32),
                pltpu.VMEM((roots, 2 * BOND, BOND), F32),
                pltpu.VMEM((roots, 2 * BOND, BOND), F32),
                pltpu.VMEM((roots, 2 * BOND, BOND), F32),
                pltpu.VMEM((roots, 8, BOND), F32),
                pltpu.VMEM((roots, DEVS, 8, BOND), F32),
                pltpu.VMEM((roots, 8, BOND), F32),
                pltpu.VMEM((roots, 2, BOND, BOND), F32),
                pltpu.VMEM((roots, 2, DEVS, 2, ROWS, BOND), F32),
                pltpu.VMEM((DEVS, 2, ROWS, BOND), F32),
                pltpu.VMEM((PAIRS, BOND, BOND), F32),
                pltpu.VMEM((2, 8, BOND), F32),
                pltpu.VMEM((TERMS, PAIRS * PAIRS), BF16),
                pltpu.VMEM(psi.shape, F32),
                dma((roots,)),
                pltpu.VMEM((DEVS, PACKED, BOND), BF16),
                pltpu.VMEM((BOND, BOND), F32),
                pltpu.VMEM((TERMS, BOND, BOND), BF16),
                pltpu.VMEM((TERMS, BOND, BOND), BF16),
                pltpu.VMEM((TERMS, PAIRS, PAIRS), BF16),
                dma((3,)),
                dma((DEVS,)), dma((DEVS,)), dma((DEVS,)), dma((DEVS,)), dma((DEVS, 2)), dma((DEVS, 2)),
                dma((roots, DEVS)), dma((roots, DEVS)), dma((roots, 2, DEVS)), dma((roots, 2, DEVS)),
                dma((roots, 2, DEVS)), dma((roots, 2, DEVS)), dma((DEVS,)), dma((DEVS,)),
            ],
            compiler_params=pltpu.CompilerParams(
                collective_id=0, has_side_effects=True, vmem_limit_bytes=50 * 1024 * 1024
            ),
        )(*[pltpu.with_memory_space_constraint(x, pltpu.HBM) for x in (psi, left_loc, right_loc, phys_loc)])
        vecs = vecs * scale[:, :, None, None, None]
        return vecs.reshape(roots, STEPS + 1, ROWS, *psi.shape[2:]), alpha, beta

    return jax.shard_map(
        device_fn, mesh=mesh, in_specs=(P(), P("terms"), P("terms"), P("terms")),
        out_specs=(P(None, None, "terms"), P(), P()), check_vma=False,
    )
```

```python
import functools

import jax
import jax.numpy as jnp
from jax import lax
from jax.experimental import pallas as pl
from jax.experimental.pallas import tpu as pltpu
from jax.sharding import PartitionSpec as P

STEPS = 6
DEVS = 8
TERMS = 16
PAIRS = 16
BOND = 128
PACKED = TERMS // 2 * BOND + 16
ROWS = 16
N_ELEMS = float(BOND * PAIRS * BOND)
FORM_BEFORE = 0
MESH = pl.DeviceIdType.MESH
F32 = jnp.float32
BF16 = jnp.bfloat16


def flip(dev, bits):
    out = dev
    if bits & 1:
        out = out + 1 - 2 * lax.rem(dev, 2)
    if bits & 2:
        out = out + 2 - 4 * lax.rem(dev // 2, 2)
    if bits & 4:
        out = out + 4 - 8 * lax.rem(dev // 4, 2)
    return out


def total(x):
    return jnp.sum(jnp.sum(x, axis=0, keepdims=True), axis=1, keepdims=True)


def kernel(
    psi_hbm, left_hbm, right_hbm, phys_hbm, out_ref, number_ref, scale_ref,
    left, right, phys, wide, v_in, y_buf, z_buf0, z_buf1, acc, sig, v_cur, v_prev, beta_old, stats, mine,
    turned, got, got_end, across, numbers, dense, psi_ref, psi_sem, tri, squares,
    left_ref, right_ref, phys_ref, in_sem,
    r_send, r_recv, w_send, w_recv, l_send, l_recv, s_send, s_recv, g_send, g_recv, o_send, o_recv, e_send, e_recv,
):
    me = lax.axis_index("terms")
    peers = {e: flip(me, e) for e in range(1, DEVS)}

    pairs = ((right_hbm, right_ref), (phys_hbm, phys_ref), (left_hbm, left_ref))
    in_copies = [pltpu.make_async_copy(src, dst, in_sem.at[i]) for i, (src, dst) in enumerate(pairs)]
    psi_copies = [pltpu.make_async_copy(psi_hbm.at[r], psi_ref.at[r], psi_sem.at[r]) for r in range(2)]
    for in_copy in in_copies + psi_copies:
        in_copy.start()
    barrier = pltpu.get_barrier_semaphore()
    for e in range(1, DEVS):
        pl.semaphore_signal(barrier, inc=1, device_id=(peers[e],), device_id_type=MESH)
    for in_copy in in_copies:
        in_copy.wait()

    def copy(src, dst, send, recv, e):
        return pltpu.make_async_remote_copy(
            src_ref=src, dst_ref=dst, send_sem=send, recv_sem=recv, device_id=(peers[e],), device_id_type=MESH
        )

    def r_copy(e):
        rows = pl.ds(pl.multiple_of(peers[e] * ROWS, ROWS), ROWS)
        return copy(right_ref.at[:, rows, :], right.at[e], r_send.at[e], r_recv.at[e], e)

    def w_copy(e):
        return copy(dense, phys.at[e], w_send.at[e], w_recv.at[e], e)

    def part(x):
        return slice(0, 512) if x == 0 else slice(512, PACKED)

    def l_copy(e, x):
        return copy(tri.at[0, part(x)], tri.at[e, part(x)], l_send.at[e, x], l_recv.at[e, x], e)

    def l_far(x):
        e = (2, 4)[x]
        return copy(tri.at[e, part(x)], tri.at[6, part(x)], l_send.at[6, x], l_recv.at[6, x], 6 - e)

    def l_pass(e, x):
        return copy(tri.at[e, part(x)], tri.at[e + 1, part(x)], l_send.at[e + 1, x], l_recv.at[e + 1, x], 1)

    def s_copy(r, e):
        return copy(mine.at[r], stats.at[r, me], s_send.at[r, e], s_recv.at[r, e], e)

    def g_copy(r, g, e):
        slot = v_in.at[r, me, g * 8 : (g + 1) * 8]
        return copy(slot, slot, g_send.at[r, g, e], g_recv.at[r, g, e], e)

    def g_pass(r, g, e):
        slot = v_in.at[r, peers[e], g * 8 : (g + 1) * 8]
        return copy(slot, slot, g_send.at[r, g, e + 1], g_recv.at[r, g, e + 1], 1)

    def o_copy(r, j, e):
        rows = pl.ds(pl.multiple_of(peers[e] * ROWS, ROWS), ROWS)
        way = lax.rem(j, 2)
        return copy(turned.at[r, :, rows, :], got.at[r, way, me], o_send.at[r, way, e], o_recv.at[r, way, e], e)

    def e_copy(e):
        rows = pl.ds(pl.multiple_of(peers[e] * ROWS, ROWS), ROWS)
        return copy(turned.at[1, :, rows, :], got_end.at[me], e_send.at[e], e_recv.at[e], e)

    row = lax.broadcasted_iota(jnp.int32, (BOND, BOND), 0)
    col = lax.broadcasted_iota(jnp.int32, (BOND, BOND), 1)
    diag_row = lax.broadcasted_iota(jnp.int32, (16, BOND), 0)
    diags = jnp.zeros((16, BOND), F32)
    for i in range(TERMS // 2):
        one, two = left_ref[2 * i].astype(F32), left_ref[2 * i + 1].astype(F32)
        tri[0, i * BOND : (i + 1) * BOND, :] = jnp.where(row < col, one, two).astype(BF16)
        diag = jnp.sum(jnp.where(row == col, one, 0.0), axis=0, keepdims=True)
        diags = jnp.where(diag_row == i, diag, diags)
    tri[0, PACKED - 16 : PACKED, :] = diags.astype(BF16)

    def unpack(d):
        diags = tri[d, PACKED - 16 : PACKED, :].astype(F32)
        for i in range(TERMS // 2):
            m = tri[d, i * BOND : (i + 1) * BOND, :].astype(F32)
            turned_m = m.T
            one = jnp.where(row < col, m, jnp.where(row > col, turned_m, diags[i : i + 1, :]))
            left[d, 2 * i] = one.astype(BF16)
            left[d, 2 * i + 1] = jnp.where(row < col, turned_m, m).astype(BF16)

    w_own = phys_ref[...].astype(F32)
    row_u = lax.broadcasted_iota(jnp.int32, (PAIRS, PAIRS * PAIRS), 0)
    col_qu = lax.broadcasted_iota(jnp.int32, (PAIRS, PAIRS * PAIRS), 1)
    flat = jnp.zeros((TERMS, PAIRS * PAIRS), F32)
    for q in range(PAIRS):
        put = jnp.where(col_qu == row_u + q * PAIRS, 1.0, 0.0).astype(BF16)
        flat += jnp.dot(w_own[:, q, :].astype(BF16), put, preferred_element_type=F32)
    dense[...] = flat.astype(BF16)
    pl.semaphore_wait(barrier, DEVS - 1)

    for e in (1, 2, 4, 3, 5, 6, 7):
        r_copy(e).start()
        w_copy(e).start()
    for e, x in ((1, 0), (1, 1), (2, 0), (4, 1), (2, 1), (4, 0)):
        l_copy(e, x).start()
    own = pl.ds(pl.multiple_of(me * ROWS, ROWS), ROWS)
    right[0] = right_ref[:, own, :]
    phys[0] = dense[...]
    left[0] = left_ref[...]
    v_prev[...] = jnp.zeros_like(v_prev)
    beta_old[...] = jnp.zeros_like(beta_old)
    numbers[...] = jnp.zeros_like(numbers)

    def prepare(r):
        psi_copies[r].wait()
        squares[...] = jnp.zeros((BOND, BOND), F32)

        @pl.loop(0, 4)
        def _(s):
            for t in range(4):
                x = psi_ref[r, :, s, t, :]
                squares[...] += x * x
                across[s * 4 + t] = x.T

        norm = jnp.sqrt(total(squares[...]) / N_ELEMS)

        @pl.loop(0, PAIRS)
        def _(u):
            v_in[r, :, u] = (across[u] / norm).astype(BF16).reshape(DEVS, ROWS, BOND)
            two = across[u, own, :] / norm
            row = pl.multiple_of(u * 8, 8)
            v_cur[r, pl.ds(row, 8), :] = two[0:8]
            v_cur[r, pl.ds(row + BOND, 8), :] = two[8:16]

        for q in range(PAIRS):
            out_ref[r, 0, :, q, :] = psi_ref[r, own, q // 4, q % 4, :] / norm

    prepare(0)

    sub = lax.broadcasted_iota(jnp.int32, (8, BOND), 0)
    lane = lax.broadcasted_iota(jnp.int32, (8, BOND), 1)
    eye = jnp.where(lax.rem(lane, 8) == sub, 1.0, 0.0).astype(F32)
    pick_row = lax.broadcasted_iota(jnp.int32, (PAIRS * PAIRS, BOND), 0)
    pick_col = lax.broadcasted_iota(jnp.int32, (PAIRS * PAIRS, BOND), 1) // 8

    def widen(d):
        w_d = phys[d]
        spread = []
        for q in range(PAIRS):
            pick = jnp.where(pick_row == pick_col + q * PAIRS, 1.0, 0.0).astype(BF16)
            spread.append(jnp.dot(w_d, pick, preferred_element_type=F32))
        for k in range(TERMS):
            for q in range(0, PAIRS, 2):
                two = [jnp.broadcast_to(spread[q + i][k : k + 1, :], (8, BOND)) * eye for i in range(2)]
                wide[d, k, q * 8 : q * 8 + 16, :] = jnp.concatenate(two, axis=0).astype(BF16)

    def form_y(r, d, pairs):
        r_d = right[d].reshape(TERMS * ROWS, BOND)
        for u in pairs:
            v_u = jnp.concatenate([v_in[r, :, u + i].reshape(BOND, BOND) for i in range(2)], axis=1)
            y = jnp.dot(r_d, v_u, preferred_element_type=F32).reshape(TERMS, 2, 8, 2 * BOND)
            y = jnp.concatenate([y[..., :BOND], y[..., BOND:]], axis=2)
            y_buf[d, :, :, u * 8 : u * 8 + 16, :] = y.astype(BF16)

    def form_out(d, z_buf, first):
        for k in range(TERMS):
            y_k = jnp.concatenate([y_buf[d, k, 0], y_buf[d, k, 1]], axis=1)
            z = jnp.dot(wide[d, k], y_k, preferred_element_type=F32).astype(BF16)
            for h in range(2):
                z_buf[h * BOND : (h + 1) * BOND, k * BOND : (k + 1) * BOND] = z[:, h * BOND : (h + 1) * BOND]
        part = jnp.dot(z_buf[...], left[d].reshape(TERMS * BOND, BOND), preferred_element_type=F32)
        if first:
            acc[...] = part
        else:
            acc[...] += part

    def share(r):
        s, v, vp = acc[...], v_cur[r], v_prev[r]
        d_p, n_p = total(s * v), total(v * v)
        guess = jnp.where(n_p > 0.0, d_p / jnp.where(n_p > 0.0, n_p, 1.0), 0.0)
        s = s - guess * v - beta_old[r, 0:1, :] * vp
        sig[r] = s
        rows = [d_p, n_p, guess, total(s * s), total(s * v)]
        tile = jnp.zeros((8, BOND), F32)
        for i, row in enumerate(rows):
            tile = jnp.where(sub == i, row, tile)
        mine[r] = tile
        stats[r, me] = tile
        for e in (6, 7, 2, 3, 4, 5, 1):
            s_copy(r, e).start()

    def scalars(r, j):
        for e in range(1, DEVS):
            s_copy(r, e).wait()
        alpha = jnp.zeros((1, BOND), F32)
        for p in range(DEVS):
            alpha = alpha + stats[r, p, 0:1, :]
        alpha = alpha / N_ELEMS
        square = jnp.zeros((1, BOND), F32)
        for p in range(DEVS):
            d_p = alpha - stats[r, p, 2:3, :]
            square = square + (stats[r, p, 3:4, :] - 2.0 * d_p * stats[r, p, 4:5, :] + d_p * d_p * stats[r, p, 1:2, :])
        beta = jnp.sqrt(jnp.maximum(square, 0.0) / N_ELEMS)
        here = jnp.logical_and(sub == r, lane == j)
        numbers[0] = jnp.where(here, alpha, numbers[0])
        numbers[1] = jnp.where(here, beta, numbers[1])
        return alpha, beta

    def turn(r, joined):
        for g in range(2):
            turned[r, g] = joined[g * 8 : (g + 1) * 8].reshape(BOND, BOND).T

    def advance(r, j, last):
        alpha, beta = scalars(r, j)
        shift = alpha - mine[r, 2:3, :]
        v = v_cur[r]
        nxt = (sig[r] - shift * v) / beta
        v_prev[r] = v
        v_cur[r] = nxt
        beta_old[r] = jnp.broadcast_to(beta, (8, BOND))
        halves = nxt.reshape(2, PAIRS, 8, BOND)
        joined = jnp.concatenate([halves[0], halves[1]], axis=1)

        @pl.when(jnp.logical_not(last))
        def _():
            v_in[r, me] = joined.astype(BF16)
            for g in range(2):
                for e in (6, 4, 2, 1):
                    g_copy(r, g, e).start()


    def post(r, j):
        halves = v_cur[r].reshape(2, PAIRS, 8, BOND)
        turn(r, jnp.concatenate([halves[0], halves[1]], axis=1))
        for e in (6, 7, 2, 3, 4, 5, 1):
            o_copy(r, j, e).start()
        got[r, lax.rem(j, 2), me] = turned[r, :, own, :]

    def relay(r, g):
        for e in (4, 6, 2):
            g_copy(r, g, e).wait()
            g_pass(r, g, e).start()

    def arrive(r, g):
        g_copy(r, g, 1).wait()
        for e in (4, 6, 2):
            g_pass(r, g, e).wait()

    def assemble(read):
        chunk_of = lax.broadcasted_iota(jnp.int32, (ROWS, BOND), 1) // 16
        pairs = []
        for g in range(2):
            x = [read(p, g) for p in range(DEVS)]
            for bit in (1, 2, 4):
                odd = lax.rem(chunk_of // bit, 2) == 1
                for p in range(DEVS):
                    if p & bit:
                        continue
                    low, high = x[p], x[p + bit]
                    x[p] = jnp.where(odd, pltpu.roll(high, 16 * bit, 1), low)
                    x[p + bit] = jnp.where(odd, high, pltpu.roll(low, BOND - 16 * bit, 1))
            pairs += x
        return pairs

    def collect(r, j):
        for e in range(1, DEVS):
            o_copy(r, j, e).wait()
        for q, x in enumerate(assemble(lambda p, g: got[r, lax.rem(j, 2), p, g])):
            out_ref[r, j + 1, :, q, :] = x


    @pl.loop(0, DEVS)
    def _(d):
        for e in range(1, DEVS):

            @pl.when(d == e)
            def _():
                r_copy(e).wait()
                w_copy(e).wait()

        widen(d)
        form_y(0, d, range(0, PAIRS, 2))

    for d in range(DEVS):
        nxt = d + 1
        if nxt == 1:
            l_copy(1, 0).wait()
            l_copy(1, 1).wait()
        elif nxt == 2:
            for e, x in ((2, 0), (4, 1)):
                l_copy(e, x).wait()
                l_far(x).start()
                l_pass(e, x).start()
            prepare(1)
            for e, x in ((2, 1), (4, 0)):
                l_copy(e, x).wait()
                l_pass(e, x).start()
        elif nxt == 6:
            for x in range(2):
                l_far(x).wait()
                l_pass(6, x).start()
        elif nxt in (3, 5, 7):
            for x in range(2):
                l_pass(nxt - 1, x).wait()
        if nxt < DEVS:
            unpack(nxt)
        form_out(d, (z_buf0, z_buf1)[d % 2], d == 0)

    share(0)

    @pl.loop(1, 2 * STEPS)
    def _(t):
        r, j = lax.rem(t, 2), t // 2
        pr, pj = 1 - r, (t - 1) // 2

        for g in range(2):

            @pl.when(t >= 2)
            def _():
                arrive(r, g)

            for u in range(g * 8, (g + 1) * 8, 2):
                for d in range(DEVS):
                    form_y(r, d, (u,))

        for d in range(DEVS):
            if d == FORM_BEFORE:
                advance(pr, pj, t == 2 * STEPS - 1)

                @pl.when(t == 2 * STEPS - 1)
                def _():
                    post(pr, pj)

            form_out(d, (z_buf0, z_buf1)[d % 2], d == 0)

        share(r)

        @pl.when(t < 2 * STEPS - 1)
        def _():
            relay(pr, 0)
            post(pr, pj)

        @pl.when(t >= 2)
        def _():
            collect(r, j - 1)

        @pl.when(t < 2 * STEPS - 1)
        def _():
            relay(pr, 1)

    halves = sig[1].reshape(2, PAIRS, 8, BOND)
    turn(1, jnp.concatenate([halves[0], halves[1]], axis=1))
    for e in (6, 7, 2, 3, 4, 5, 1):
        e_copy(e).start()
    got_end[me] = turned[1, :, own, :]
    collect(0, STEPS - 1)
    alpha, beta = scalars(1, STEPS - 1)
    shift = jnp.zeros((1, BOND), F32)
    for p in range(DEVS):
        shift = jnp.where(lane[0:1] // 16 == p, alpha - stats[1, p, 2:3, :], shift)
    for e in range(1, DEVS):
        e_copy(e).wait()
    for q, x in enumerate(assemble(lambda p, g: got_end[p, g])):
        v = out_ref[1, STEPS - 1, :, q, :]
        out_ref[1, STEPS, :, q, :] = x - shift * v
    number_ref[...] = numbers[...]
    end = jnp.logical_and(sub == 1, lane == STEPS)
    scale_ref[...] = jnp.where(end, 1.0 / beta, jnp.ones((8, BOND), F32))[0:2, 0 : STEPS + 1]


def solution(mesh):
    def device_fn(psi, left_loc, phys_loc, right_loc):
        roots = psi.shape[0]
        dma = pltpu.SemaphoreType.DMA
        vecs, both, scale = pl.pallas_call(
            kernel,
            out_shape=(
                jax.ShapeDtypeStruct((roots, STEPS + 1, ROWS, PAIRS, BOND), F32),
                jax.ShapeDtypeStruct((2, 8, BOND), F32),
                jax.ShapeDtypeStruct((roots, STEPS + 1), F32),
            ),
            in_specs=[pl.BlockSpec(memory_space=pltpu.HBM)] * 4,
            out_specs=[pl.BlockSpec(memory_space=pltpu.VMEM)] * 3,
            scratch_shapes=[
                pltpu.VMEM((DEVS, TERMS, BOND, BOND), BF16),
                pltpu.VMEM((DEVS, TERMS, ROWS, BOND), BF16),
                pltpu.VMEM((DEVS, TERMS, PAIRS * PAIRS), BF16),
                pltpu.VMEM((DEVS, TERMS, BOND, BOND), BF16),
                pltpu.VMEM((roots, DEVS, PAIRS, ROWS, BOND), BF16),
                pltpu.VMEM((DEVS, TERMS, 2, BOND, BOND), BF16),
                pltpu.VMEM((2 * BOND, TERMS * BOND), BF16),
                pltpu.VMEM((2 * BOND, TERMS * BOND), BF16),
                pltpu.VMEM((2 * BOND, BOND), F32),
                pltpu.VMEM((roots, 2 * BOND, BOND), F32),
                pltpu.VMEM((roots, 2 * BOND, BOND), F32),
                pltpu.VMEM((roots, 2 * BOND, BOND), F32),
                pltpu.VMEM((roots, 8, BOND), F32),
                pltpu.VMEM((roots, DEVS, 8, BOND), F32),
                pltpu.VMEM((roots, 8, BOND), F32),
                pltpu.VMEM((roots, 2, BOND, BOND), F32),
                pltpu.VMEM((roots, 2, DEVS, 2, ROWS, BOND), F32),
                pltpu.VMEM((DEVS, 2, ROWS, BOND), F32),
                pltpu.VMEM((PAIRS, BOND, BOND), F32),
                pltpu.VMEM((2, 8, BOND), F32),
                pltpu.VMEM((TERMS, PAIRS * PAIRS), BF16),
                pltpu.VMEM(psi.shape, F32),
                dma((roots,)),
                pltpu.VMEM((DEVS, PACKED, BOND), BF16),
                pltpu.VMEM((BOND, BOND), F32),
                pltpu.VMEM((TERMS, BOND, BOND), BF16),
                pltpu.VMEM((TERMS, BOND, BOND), BF16),
                pltpu.VMEM((TERMS, PAIRS, PAIRS), BF16),
                dma((3,)),
                dma((DEVS,)), dma((DEVS,)), dma((DEVS,)), dma((DEVS,)), dma((DEVS, 2)), dma((DEVS, 2)),
                dma((roots, DEVS)), dma((roots, DEVS)), dma((roots, 2, DEVS)), dma((roots, 2, DEVS)),
                dma((roots, 2, DEVS)), dma((roots, 2, DEVS)), dma((DEVS,)), dma((DEVS,)),
            ],
            compiler_params=pltpu.CompilerParams(
                collective_id=0, has_side_effects=True, vmem_limit_bytes=50 * 1024 * 1024
            ),
        )(*[pltpu.with_memory_space_constraint(x, pltpu.HBM) for x in (psi, left_loc, right_loc, phys_loc)])
        vecs = vecs * scale[:, :, None, None, None]
        return vecs.reshape(roots, STEPS + 1, ROWS, *psi.shape[2:]), both[0, :roots, :STEPS], both[1, :roots, :STEPS]

    return jax.shard_map(
        device_fn, mesh=mesh, in_specs=(P(), P("terms"), P("terms"), P("terms")),
        out_specs=(P(None, None, "terms"), P(), P()), check_vma=False,
    )
```

```python
import functools

import jax
import jax.numpy as jnp
from jax import lax
from jax.experimental import pallas as pl
from jax.experimental.pallas import tpu as pltpu
from jax.sharding import PartitionSpec as P

STEPS = 6
DEVS = 8
TERMS = 16
PAIRS = 16
BOND = 128
PACKED = TERMS // 2 * BOND + 16
ROWS = 16
N_ELEMS = float(BOND * PAIRS * BOND)
FORM_BEFORE = 0
MESH = pl.DeviceIdType.MESH
F32 = jnp.float32
BF16 = jnp.bfloat16


def flip(dev, bits):
    out = dev
    if bits & 1:
        out = out + 1 - 2 * lax.rem(dev, 2)
    if bits & 2:
        out = out + 2 - 4 * lax.rem(dev // 2, 2)
    if bits & 4:
        out = out + 4 - 8 * lax.rem(dev // 4, 2)
    return out


def total(x):
    return jnp.sum(jnp.sum(x, axis=0, keepdims=True), axis=1, keepdims=True)


def kernel(
    psi_hbm, left_hbm, right_hbm, phys_hbm, out_ref, number_ref,
    left, right, phys, wide, v_in, y_buf, z_buf0, z_buf1, acc, sig, v_cur, v_prev, beta_old, stats, mine,
    turned, got, got_end, across, numbers, dense, psi_ref, psi_sem, tri, squares,
    left_ref, right_ref, phys_ref, in_sem,
    r_send, r_recv, w_send, w_recv, l_send, l_recv, s_send, s_recv, g_send, g_recv, o_send, o_recv, e_send, e_recv,
):
    me = lax.axis_index("terms")
    peers = {e: flip(me, e) for e in range(1, DEVS)}

    pairs = ((right_hbm, right_ref), (phys_hbm, phys_ref), (left_hbm, left_ref))
    in_copies = [pltpu.make_async_copy(src, dst, in_sem.at[i]) for i, (src, dst) in enumerate(pairs)]
    psi_copies = [pltpu.make_async_copy(psi_hbm.at[r], psi_ref.at[r], psi_sem.at[r]) for r in range(2)]
    for in_copy in in_copies + psi_copies:
        in_copy.start()
    barrier = pltpu.get_barrier_semaphore()
    for e in range(1, DEVS):
        pl.semaphore_signal(barrier, inc=1, device_id=(peers[e],), device_id_type=MESH)
    for in_copy in in_copies:
        in_copy.wait()

    def copy(src, dst, send, recv, e):
        return pltpu.make_async_remote_copy(
            src_ref=src, dst_ref=dst, send_sem=send, recv_sem=recv, device_id=(peers[e],), device_id_type=MESH
        )

    def r_copy(e):
        rows = pl.ds(pl.multiple_of(peers[e] * ROWS, ROWS), ROWS)
        return copy(right_ref.at[:, rows, :], right.at[e], r_send.at[e], r_recv.at[e], e)

    def w_copy(e):
        return copy(dense, phys.at[e], w_send.at[e], w_recv.at[e], e)

    def part(x):
        return slice(0, 512) if x == 0 else slice(512, PACKED)

    def l_copy(e, x):
        return copy(tri.at[0, part(x)], tri.at[e, part(x)], l_send.at[e, x], l_recv.at[e, x], e)

    def l_far(x):
        e = (2, 4)[x]
        return copy(tri.at[e, part(x)], tri.at[6, part(x)], l_send.at[6, x], l_recv.at[6, x], 6 - e)

    def l_pass(e, x):
        return copy(tri.at[e, part(x)], tri.at[e + 1, part(x)], l_send.at[e + 1, x], l_recv.at[e + 1, x], 1)

    def s_copy(r, e):
        return copy(mine.at[r], stats.at[r, me], s_send.at[r, e], s_recv.at[r, e], e)

    def g_copy(r, g, e):
        slot = v_in.at[r, me, g * 8 : (g + 1) * 8]
        return copy(slot, slot, g_send.at[r, g, e], g_recv.at[r, g, e], e)

    def g_pass(r, g, e):
        slot = v_in.at[r, peers[e], g * 8 : (g + 1) * 8]
        return copy(slot, slot, g_send.at[r, g, e + 1], g_recv.at[r, g, e + 1], 1)

    def o_copy(r, j, e):
        rows = pl.ds(pl.multiple_of(peers[e] * ROWS, ROWS), ROWS)
        way = lax.rem(j, 2)
        return copy(turned.at[r, :, rows, :], got.at[r, way, me], o_send.at[r, way, e], o_recv.at[r, way, e], e)

    def e_copy(e):
        rows = pl.ds(pl.multiple_of(peers[e] * ROWS, ROWS), ROWS)
        return copy(turned.at[1, :, rows, :], got_end.at[me], e_send.at[e], e_recv.at[e], e)

    row = lax.broadcasted_iota(jnp.int32, (BOND, BOND), 0)
    col = lax.broadcasted_iota(jnp.int32, (BOND, BOND), 1)
    diag_row = lax.broadcasted_iota(jnp.int32, (16, BOND), 0)
    diags = jnp.zeros((16, BOND), F32)
    for i in range(TERMS // 2):
        one, two = left_ref[2 * i].astype(F32), left_ref[2 * i + 1].astype(F32)
        tri[0, i * BOND : (i + 1) * BOND, :] = jnp.where(row < col, one, two).astype(BF16)
        diag = jnp.sum(jnp.where(row == col, one, 0.0), axis=0, keepdims=True)
        diags = jnp.where(diag_row == i, diag, diags)
    tri[0, PACKED - 16 : PACKED, :] = diags.astype(BF16)

    def unpack(d):
        diags = tri[d, PACKED - 16 : PACKED, :].astype(F32)
        for i in range(TERMS // 2):
            m = tri[d, i * BOND : (i + 1) * BOND, :].astype(F32)
            turned_m = m.T
            one = jnp.where(row < col, m, jnp.where(row > col, turned_m, diags[i : i + 1, :]))
            left[d, 2 * i] = one.astype(BF16)
            left[d, 2 * i + 1] = jnp.where(row < col, turned_m, m).astype(BF16)

    w_own = phys_ref[...].astype(F32)
    row_u = lax.broadcasted_iota(jnp.int32, (PAIRS, PAIRS * PAIRS), 0)
    col_qu = lax.broadcasted_iota(jnp.int32, (PAIRS, PAIRS * PAIRS), 1)
    flat = jnp.zeros((TERMS, PAIRS * PAIRS), F32)
    for q in range(PAIRS):
        put = jnp.where(col_qu == row_u + q * PAIRS, 1.0, 0.0).astype(BF16)
        flat += jnp.dot(w_own[:, q, :].astype(BF16), put, preferred_element_type=F32)
    dense[...] = flat.astype(BF16)
    pl.semaphore_wait(barrier, DEVS - 1)

    for e in (1, 2, 4, 3, 5, 6, 7):
        r_copy(e).start()
        w_copy(e).start()
    for e, x in ((1, 0), (1, 1), (2, 0), (4, 1), (2, 1), (4, 0)):
        l_copy(e, x).start()
    own = pl.ds(pl.multiple_of(me * ROWS, ROWS), ROWS)
    right[0] = right_ref[:, own, :]
    phys[0] = dense[...]
    left[0] = left_ref[...]
    v_prev[...] = jnp.zeros_like(v_prev)
    beta_old[...] = jnp.zeros_like(beta_old)
    numbers[...] = jnp.zeros_like(numbers)

    def prepare(r):
        psi_copies[r].wait()
        squares[...] = jnp.zeros((BOND, BOND), F32)

        @pl.loop(0, 4)
        def _(s):
            for t in range(4):
                x = psi_ref[r, :, s, t, :]
                squares[...] += x * x
                across[s * 4 + t] = x.T

        norm = jnp.sqrt(total(squares[...]) / N_ELEMS)

        @pl.loop(0, PAIRS)
        def _(u):
            v_in[r, :, u] = (across[u] / norm).astype(BF16).reshape(DEVS, ROWS, BOND)
            two = across[u, own, :] / norm
            row = pl.multiple_of(u * 8, 8)
            v_cur[r, pl.ds(row, 8), :] = two[0:8]
            v_cur[r, pl.ds(row + BOND, 8), :] = two[8:16]

        for q in range(PAIRS):
            out_ref[r, 0, :, q, :] = psi_ref[r, own, q // 4, q % 4, :] / norm

    prepare(0)

    sub = lax.broadcasted_iota(jnp.int32, (8, BOND), 0)
    lane = lax.broadcasted_iota(jnp.int32, (8, BOND), 1)
    eye = jnp.where(lax.rem(lane, 8) == sub, 1.0, 0.0).astype(F32)
    pick_row = lax.broadcasted_iota(jnp.int32, (PAIRS * PAIRS, BOND), 0)
    pick_col = lax.broadcasted_iota(jnp.int32, (PAIRS * PAIRS, BOND), 1) // 8

    def widen(d):
        w_d = phys[d]
        spread = []
        for q in range(PAIRS):
            pick = jnp.where(pick_row == pick_col + q * PAIRS, 1.0, 0.0).astype(BF16)
            spread.append(jnp.dot(w_d, pick, preferred_element_type=F32))
        for k in range(TERMS):
            for q in range(0, PAIRS, 2):
                two = [jnp.broadcast_to(spread[q + i][k : k + 1, :], (8, BOND)) * eye for i in range(2)]
                wide[d, k, q * 8 : q * 8 + 16, :] = jnp.concatenate(two, axis=0).astype(BF16)

    def form_y(r, d, pairs):
        r_d = right[d].reshape(TERMS * ROWS, BOND)
        for u in pairs:
            v_u = jnp.concatenate([v_in[r, :, u + i].reshape(BOND, BOND) for i in range(2)], axis=1)
            y = jnp.dot(r_d, v_u, preferred_element_type=F32).reshape(TERMS, 2, 8, 2 * BOND)
            y = jnp.concatenate([y[..., :BOND], y[..., BOND:]], axis=2)
            y_buf[d, :, :, u * 8 : u * 8 + 16, :] = y.astype(BF16)

    def form_out(d, z_buf, first):
        for k in range(TERMS):
            y_k = jnp.concatenate([y_buf[d, k, 0], y_buf[d, k, 1]], axis=1)
            z = jnp.dot(wide[d, k], y_k, preferred_element_type=F32).astype(BF16)
            for h in range(2):
                z_buf[h * BOND : (h + 1) * BOND, k * BOND : (k + 1) * BOND] = z[:, h * BOND : (h + 1) * BOND]
        part = jnp.dot(z_buf[...], left[d].reshape(TERMS * BOND, BOND), preferred_element_type=F32)
        if first:
            acc[...] = part
        else:
            acc[...] += part

    def share(r):
        s, v, vp = acc[...], v_cur[r], v_prev[r]
        d_p, n_p = total(s * v), total(v * v)
        guess = jnp.where(n_p > 0.0, d_p / jnp.where(n_p > 0.0, n_p, 1.0), 0.0)
        s = s - guess * v - beta_old[r, 0:1, :] * vp
        sig[r] = s
        rows = [d_p, n_p, guess, total(s * s), total(s * v)]
        tile = jnp.zeros((8, BOND), F32)
        for i, row in enumerate(rows):
            tile = jnp.where(sub == i, row, tile)
        mine[r] = tile
        stats[r, me] = tile
        for e in (6, 7, 2, 3, 4, 5, 1):
            s_copy(r, e).start()

    def scalars(r, j):
        for e in range(1, DEVS):
            s_copy(r, e).wait()
        alpha = jnp.zeros((1, BOND), F32)
        for p in range(DEVS):
            alpha = alpha + stats[r, p, 0:1, :]
        alpha = alpha / N_ELEMS
        square = jnp.zeros((1, BOND), F32)
        for p in range(DEVS):
            d_p = alpha - stats[r, p, 2:3, :]
            square = square + (stats[r, p, 3:4, :] - 2.0 * d_p * stats[r, p, 4:5, :] + d_p * d_p * stats[r, p, 1:2, :])
        beta = jnp.sqrt(jnp.maximum(square, 0.0) / N_ELEMS)
        here = jnp.logical_and(sub == r, lane == j)
        numbers[0] = jnp.where(here, alpha, numbers[0])
        numbers[1] = jnp.where(here, beta, numbers[1])
        return alpha, beta

    def turn(r, joined):
        for g in range(2):
            turned[r, g] = joined[g * 8 : (g + 1) * 8].reshape(BOND, BOND).T

    def advance(r, j, last):
        alpha, beta = scalars(r, j)
        shift = alpha - mine[r, 2:3, :]
        v = v_cur[r]
        nxt = (sig[r] - shift * v) / beta
        v_prev[r] = v
        v_cur[r] = nxt
        beta_old[r] = jnp.broadcast_to(beta, (8, BOND))
        halves = nxt.reshape(2, PAIRS, 8, BOND)
        joined = jnp.concatenate([halves[0], halves[1]], axis=1)

        @pl.when(jnp.logical_not(last))
        def _():
            v_in[r, me] = joined.astype(BF16)
            for g in range(2):
                for e in (6, 4, 2, 1):
                    g_copy(r, g, e).start()


    def post(r, j):
        halves = v_cur[r].reshape(2, PAIRS, 8, BOND)
        turn(r, jnp.concatenate([halves[0], halves[1]], axis=1))
        for e in (6, 7, 2, 3, 4, 5, 1):
            o_copy(r, j, e).start()
        got[r, lax.rem(j, 2), me] = turned[r, :, own, :]

    def relay(r, g):
        for e in (4, 6, 2):
            g_copy(r, g, e).wait()
            g_pass(r, g, e).start()

    def arrive(r, g):
        g_copy(r, g, 1).wait()
        for e in (4, 6, 2):
            g_pass(r, g, e).wait()

    def assemble(read):
        chunk_of = lax.broadcasted_iota(jnp.int32, (ROWS, BOND), 1) // 16
        pairs = []
        for g in range(2):
            x = [read(p, g) for p in range(DEVS)]
            for bit in (1, 2, 4):
                odd = lax.rem(chunk_of // bit, 2) == 1
                for p in range(DEVS):
                    if p & bit:
                        continue
                    low, high = x[p], x[p + bit]
                    x[p] = jnp.where(odd, pltpu.roll(high, 16 * bit, 1), low)
                    x[p + bit] = jnp.where(odd, high, pltpu.roll(low, BOND - 16 * bit, 1))
            pairs += x
        return pairs

    def collect(r, j):
        for e in range(1, DEVS):
            o_copy(r, j, e).wait()
        for q, x in enumerate(assemble(lambda p, g: got[r, lax.rem(j, 2), p, g])):
            out_ref[r, j + 1, :, q, :] = x


    @pl.loop(0, DEVS)
    def _(d):
        for e in range(1, DEVS):

            @pl.when(d == e)
            def _():
                r_copy(e).wait()
                w_copy(e).wait()

        widen(d)
        form_y(0, d, range(0, PAIRS, 2))

    for d in range(DEVS):
        nxt = d + 1
        if nxt == 1:
            l_copy(1, 0).wait()
            l_copy(1, 1).wait()
        elif nxt == 2:
            for e, x in ((2, 0), (4, 1)):
                l_copy(e, x).wait()
                l_far(x).start()
                l_pass(e, x).start()
            prepare(1)
            for e, x in ((2, 1), (4, 0)):
                l_copy(e, x).wait()
                l_pass(e, x).start()
        elif nxt == 6:
            for x in range(2):
                l_far(x).wait()
                l_pass(6, x).start()
        elif nxt in (3, 5, 7):
            for x in range(2):
                l_pass(nxt - 1, x).wait()
        if nxt < DEVS:
            unpack(nxt)
        form_out(d, (z_buf0, z_buf1)[d % 2], d == 0)

    share(0)

    @pl.loop(1, 2 * STEPS)
    def _(t):
        r, j = lax.rem(t, 2), t // 2
        pr, pj = 1 - r, (t - 1) // 2

        for g in range(2):

            @pl.when(t >= 2)
            def _():
                arrive(r, g)

            for u in range(g * 8, (g + 1) * 8, 2):
                for d in range(DEVS):
                    form_y(r, d, (u,))

        for d in range(DEVS):
            if d == FORM_BEFORE:
                advance(pr, pj, t == 2 * STEPS - 1)

                @pl.when(t == 2 * STEPS - 1)
                def _():
                    post(pr, pj)

            form_out(d, (z_buf0, z_buf1)[d % 2], d == 0)

        share(r)

        @pl.when(t < 2 * STEPS - 1)
        def _():
            relay(pr, 0)
            post(pr, pj)

        @pl.when(t >= 2)
        def _():
            collect(r, j - 1)

        @pl.when(t < 2 * STEPS - 1)
        def _():
            relay(pr, 1)

    halves = sig[1].reshape(2, PAIRS, 8, BOND)
    turn(1, jnp.concatenate([halves[0], halves[1]], axis=1))
    for e in (6, 7, 2, 3, 4, 5, 1):
        e_copy(e).start()
    got_end[me] = turned[1, :, own, :]
    collect(0, STEPS - 1)
    alpha, beta = scalars(1, STEPS - 1)
    shift = jnp.zeros((1, BOND), F32)
    for p in range(DEVS):
        shift = jnp.where(lane[0:1] // 16 == p, alpha - stats[1, p, 2:3, :], shift)
    for e in range(1, DEVS):
        e_copy(e).wait()
    for q, x in enumerate(assemble(lambda p, g: got_end[p, g])):
        v = out_ref[1, STEPS - 1, :, q, :]
        out_ref[1, STEPS, :, q, :] = (x - shift * v) / beta
    number_ref[...] = numbers[...]


def solution(mesh):
    def device_fn(psi, left_loc, phys_loc, right_loc):
        roots = psi.shape[0]
        dma = pltpu.SemaphoreType.DMA
        vecs, both = pl.pallas_call(
            kernel,
            out_shape=(
                jax.ShapeDtypeStruct((roots, STEPS + 1, ROWS, PAIRS, BOND), F32),
                jax.ShapeDtypeStruct((2, 8, BOND), F32),
            ),
            in_specs=[pl.BlockSpec(memory_space=pltpu.HBM)] * 4,
            out_specs=[pl.BlockSpec(memory_space=pltpu.VMEM)] * 2,
            scratch_shapes=[
                pltpu.VMEM((DEVS, TERMS, BOND, BOND), BF16),
                pltpu.VMEM((DEVS, TERMS, ROWS, BOND), BF16),
                pltpu.VMEM((DEVS, TERMS, PAIRS * PAIRS), BF16),
                pltpu.VMEM((DEVS, TERMS, BOND, BOND), BF16),
                pltpu.VMEM((roots, DEVS, PAIRS, ROWS, BOND), BF16),
                pltpu.VMEM((DEVS, TERMS, 2, BOND, BOND), BF16),
                pltpu.VMEM((2 * BOND, TERMS * BOND), BF16),
                pltpu.VMEM((2 * BOND, TERMS * BOND), BF16),
                pltpu.VMEM((2 * BOND, BOND), F32),
                pltpu.VMEM((roots, 2 * BOND, BOND), F32),
                pltpu.VMEM((roots, 2 * BOND, BOND), F32),
                pltpu.VMEM((roots, 2 * BOND, BOND), F32),
                pltpu.VMEM((roots, 8, BOND), F32),
                pltpu.VMEM((roots, DEVS, 8, BOND), F32),
                pltpu.VMEM((roots, 8, BOND), F32),
                pltpu.VMEM((roots, 2, BOND, BOND), F32),
                pltpu.VMEM((roots, 2, DEVS, 2, ROWS, BOND), F32),
                pltpu.VMEM((DEVS, 2, ROWS, BOND), F32),
                pltpu.VMEM((PAIRS, BOND, BOND), F32),
                pltpu.VMEM((2, 8, BOND), F32),
                pltpu.VMEM((TERMS, PAIRS * PAIRS), BF16),
                pltpu.VMEM(psi.shape, F32),
                dma((roots,)),
                pltpu.VMEM((DEVS, PACKED, BOND), BF16),
                pltpu.VMEM((BOND, BOND), F32),
                pltpu.VMEM((TERMS, BOND, BOND), BF16),
                pltpu.VMEM((TERMS, BOND, BOND), BF16),
                pltpu.VMEM((TERMS, PAIRS, PAIRS), BF16),
                dma((3,)),
                dma((DEVS,)), dma((DEVS,)), dma((DEVS,)), dma((DEVS,)), dma((DEVS, 2)), dma((DEVS, 2)),
                dma((roots, DEVS)), dma((roots, DEVS)), dma((roots, 2, DEVS)), dma((roots, 2, DEVS)),
                dma((roots, 2, DEVS)), dma((roots, 2, DEVS)), dma((DEVS,)), dma((DEVS,)),
            ],
            compiler_params=pltpu.CompilerParams(
                collective_id=0, has_side_effects=True, vmem_limit_bytes=50 * 1024 * 1024
            ),
        )(*[pltpu.with_memory_space_constraint(x, pltpu.HBM) for x in (psi, left_loc, right_loc, phys_loc)])
        return vecs.reshape(roots, STEPS + 1, ROWS, *psi.shape[2:]), both[0, :roots, :STEPS], both[1, :roots, :STEPS]

    return jax.shard_map(
        device_fn, mesh=mesh, in_specs=(P(), P("terms"), P("terms"), P("terms")),
        out_specs=(P(None, None, "terms"), P(), P()), check_vma=False,
    )
```
